32 devices in a mesh: expert: 8 (over z, y), tensor: 4 (over x, core).
Axes of the slice: x: 2, y: 2, z: 4, core: 2. Of those that a mesh axis runs over, the one named last changes fastest.
Arguments:
- inputs: bfloat16 [8192, 768], P(('expert', 'tensor')), may hold values from -6 to 6
- attn_gain: float32 [768], replicated, may hold values from 0.5 to 1.5
- w_query: bfloat16 [768, 768], P(None, 'tensor'), may hold values from -0.21875 to 0.21875
- w_key: bfloat16 [768, 768], P(None, 'tensor'), may hold values from -0.21875 to 0.21875
- w_value: bfloat16 [768, 768], P(None, 'tensor'), may hold values from -0.21875 to 0.21875
- w_output: bfloat16 [768, 768], P('tensor'), may hold values from -1.75 to 1.75
- ffn_gain: float32 [768], replicated, may hold values from 0.5 to 1.5
- shared_gate: bfloat16 [768, 2048], P(None, 'tensor'), may hold values from -0.21875 to 0.21875
- shared_up: bfloat16 [768, 2048], P(None, 'tensor'), may hold values from -0.21875 to 0.21875
- shared_down: bfloat16 [2048, 768], P('tensor'), may hold values from -0.125 to 0.125
- expert_gate: bfloat16 [16, 768, 2048], P('expert', None, 'tensor'), may hold values from -0.21875 to 0.21875
- expert_up_slabs: bfloat16 [16, 768, 2048], P('expert', None, 'tensor'), may hold values from -0.21875 to 0.21875
- expert_down: bfloat16 [16, 2048, 768], P('expert', 'tensor'), may hold values from -0.125 to 0.125
- routes: int32 [8192, 2], P('expert'), may hold values from 0 to 15, all different within a row; in each aligned block of 256 rows (0 to 255, 256 to 511, ...) at most 48 rows name the same one
- gate_values: float32 [8192, 2], P('expert'), may hold values from 0.25 to 0.75
- prefix: int32 [8], P('expert'), may hold values from 102 to 512
- cotangent: bfloat16 [8192, 768], P('expert'), may hold values from -6 to 6
Outputs:
- layer_out: float32 [8192, 768], P(('expert', 'tensor'))
- grad_inputs: float32 [8192, 768], P(('expert', 'tensor'))
- grad_attn_gain: float32 [768], replicated
- grad_query: float32 [768, 768], P('expert', 'tensor')
- grad_key: float32 [768, 768], P('expert', 'tensor')
- grad_value: float32 [768, 768], P('expert', 'tensor')
- grad_output: float32 [768, 768], P('tensor', 'expert')
- grad_ffn_gain: float32 [768], replicated
- grad_shared_gate: float32 [768, 2048], P('expert', 'tensor')
- grad_shared_up: float32 [768, 2048], P('expert', 'tensor')
- grad_shared_down: float32 [2048, 768], P('tensor', 'expert')
- grad_expert_gate: float32 [16, 768, 2048], P('expert', None, 'tensor')
- grad_expert_up: float32 [16, 768, 2048], P('expert', None, 'tensor')
- grad_expert_down: float32 [16, 2048, 768], P('expert', 'tensor')
The draws below stay inside these ranges and needn't reach their ends.
Inputs may be any that keep to these rules, and one draw needn't show every extreme that they name: `routes`: within the rows of one device (aligned blocks of 256 tokens) no expert is named by more than 48 of the block's choices; a token's 2 experts differ.
All inputs are finite; a program needn't handle non-finite values.
Results may differ from the reference program's by a relative error of at most 0.015.
Values may be sent and summed in bfloat16 or wider, within the bound.
No kernel may reach another device: no remote copies, remote signals or barrier semaphores. Data moves between devices by JAX's collectives and lax.ppermute only.
A program may use at most 256 MiB of HBM per device.

```python
import math
import jax
import jax.numpy as jnp
import numpy as np
from jax import lax

MODEL_DIM = 768
HEADS = 12
HDIM = 64
FF_E = 2048
FF_S = 2048
TOPK = 2
ROUTED_EXPERTS = 16
TOK_DEV = 256
SEQ = 1024
SEQS = 8
TOKENS = 8192
EXPERT_SLABS = 1
CAP_Q = 48
N_TENSOR = 4


def set_ends(entries, rng, least, top_value):
    spot = [jax.random.randint(jax.random.fold_in(rng, axis), (), 0, length) for axis, length in enumerate(entries.shape)]
    main_axis = entries.shape.index(max(entries.shape))
    neighbour = spot[:main_axis] + [(spot[main_axis] + 1) % entries.shape[main_axis]] + spot[main_axis + 1:]
    return entries.at[tuple(spot)].set(least).at[tuple(neighbour)].set(top_value)


def block_levels(own_key, extent, cuts, low, largest):
    gain, own = 1.0, jax.random.fold_in(own_key, 6)
    for axis_at, blocks in cuts:
        heights = jnp.exp(jax.random.uniform(jax.random.fold_in(own, axis_at), (blocks,), jnp.float32, low / len(cuts), largest / len(cuts)))
        gain = gain * jnp.repeat(heights, extent[axis_at] // blocks).reshape([-1 if axis == axis_at else 1 for axis in range(len(extent))])
    return gain


def assign_block(rng, own, number, rows, amount, top, limit, slope):
    order = jax.random.permutation(rng, amount)
    heavy_load, usual = shares(amount, rows * top, limit, slope, True), shares(amount, rows * top, limit, slope, False)
    places = jnp.arange(amount)

    def named(lengths, turn):
        used = int((lengths > 0).sum())
        fixed = max(1, used // 4)
        shifted = fixed + (places - fixed + turn * (used - fixed)) % max(1, amount - fixed)
        return jnp.zeros((amount,), jnp.int32).at[order[jnp.where(places < fixed, places, shifted)]].set(jnp.asarray(lengths, jnp.int32))

    lengths = jnp.where(number % 4 == 0, named(heavy_load, number // 4), named(usual, number - number // 4 - 1))
    mixed = jax.random.permutation(jax.random.fold_in(own, 3), amount)
    donor, receiver = mixed[0:amount // 2 * 2:2], mixed[1:amount // 2 * 2:2]
    margin = jnp.minimum(lengths[donor] - 1, limit - lengths[receiver]) // 2
    margin = jnp.where((donor == order[0]) | (receiver == order[0]) | (lengths[receiver] == 0), 0, jnp.maximum(margin, 0))
    shifted = jax.random.randint(jax.random.fold_in(own, 4), (amount // 2,), 0, 1 << 20) % (margin + 1)
    lengths = lengths.at[donor].add(-shifted).at[receiver].add(shifted)
    members = jnp.searchsorted(jnp.cumsum(lengths), jnp.arange(rows * top), side="right").astype(jnp.int32)
    grid = members.reshape(top, rows).T
    grid = grid[jax.random.permutation(jax.random.fold_in(own, 1), rows)]
    turn = jax.random.randint(jax.random.fold_in(own, 2), (rows, 1), 0, top)
    return jnp.take_along_axis(grid, (jnp.arange(top)[None, :] + turn) % top, axis=1)


def shares(number_of, total, bound, slope, full):
    loads = [(1 << 20) // math.isqrt(standing ** slope) + 1 for standing in range(1, number_of + 1)]
    largest = bound if full else min(bound, max(-(-total // number_of), total * loads[0] // sum(loads)))
    least = 1 if total - largest >= number_of - 1 else 0
    counts, spare = [largest] + [least] * (number_of - 1), total - largest - least * (number_of - 1)
    while spare > 0:
        candidates = [i for i in range(1, number_of) if counts[i] < largest] or [i for i in range(1, number_of) if counts[i] < bound]
        whole, left = sum([loads[i] for i in candidates]), spare
        for i in candidates:
            more = min(bound - counts[i], max(1, left * loads[i] // whole), spare)
            counts[i] = counts[i] + more
            spare = spare - more
    return np.array(counts)


def gaussian(key, extent, deviation, most, cuts=(), kind=jnp.bfloat16):
    array = jax.random.normal(key, extent, jnp.float32) * deviation
    if len(cuts) > 0:
        array = block_levels(key, extent, cuts, -0.22, 0.18) * array
    return jnp.clip(array, min=-most, max=most).astype(kind)


def setup_inputs(seed: int = 0) -> dict:
    splits = jax.random.split(jax.random.key(seed), 18)
    inputs = gaussian(splits[0], (TOKENS, MODEL_DIM), 1.0, 6.0, ((0, 32),))
    attn_gain = jnp.clip(1.0 + 0.1 * jax.random.normal(splits[1], (MODEL_DIM,), jnp.float32), 0.5, 1.5)
    w_query = gaussian(splits[2], (MODEL_DIM, MODEL_DIM), MODEL_DIM ** -0.5, 0.21875, ((1, 4),))
    w_key = gaussian(splits[3], (MODEL_DIM, MODEL_DIM), MODEL_DIM ** -0.5, 0.21875, ((1, 4),))
    w_value = gaussian(splits[4], (MODEL_DIM, MODEL_DIM), MODEL_DIM ** -0.5, 0.21875, ((1, 4),))
    w_output = gaussian(splits[5], (MODEL_DIM, MODEL_DIM), (max(1, MODEL_DIM // 64)) ** -0.5, 1.75, ((0, 4),))
    ffn_gain = jnp.clip(1.0 + 0.1 * jax.random.normal(splits[6], (MODEL_DIM,), jnp.float32), 0.5, 1.5)
    shared_gate = gaussian(splits[7], (MODEL_DIM, FF_S), MODEL_DIM ** -0.5, 0.21875, ((1, 4),))
    shared_up = gaussian(splits[8], (MODEL_DIM, FF_S), MODEL_DIM ** -0.5, 0.21875, ((1, 4),))
    shared_down = gaussian(splits[9], (FF_S, MODEL_DIM), FF_S ** -0.5, 0.125, ((0, 4),))
    expert_gate = gaussian(splits[10], (ROUTED_EXPERTS * EXPERT_SLABS, MODEL_DIM, FF_E // EXPERT_SLABS), MODEL_DIM ** -0.5, 0.21875, ((0, 8), (2, 4)))
    expert_up_slabs = gaussian(splits[11], (ROUTED_EXPERTS * EXPERT_SLABS, MODEL_DIM, FF_E // EXPERT_SLABS), MODEL_DIM ** -0.5, 0.21875, ((0, 8), (2, 4)))
    expert_down = gaussian(splits[12], (ROUTED_EXPERTS * EXPERT_SLABS, FF_E // EXPERT_SLABS, MODEL_DIM), FF_E ** -0.5, 0.125, ((0, 8), (1, 4)))
    routes_keys = jax.random.split(jax.random.fold_in(splits[13], 1), TOKENS // TOK_DEV)
    routes_turns = jax.random.permutation(jax.random.fold_in(splits[13], 3), TOKENS // TOK_DEV)
    routes = jax.vmap(lambda own, number: assign_block(jax.random.fold_in(splits[13], 2), own, number, TOK_DEV, ROUTED_EXPERTS, TOPK, CAP_Q, 1))(routes_keys, routes_turns).reshape((TOKENS, TOPK))
    gate_values = jnp.clip(0.25 + 0.5 * jax.random.uniform(splits[14], (TOKENS, TOPK), jnp.float32) ** block_levels(splits[14], (TOKENS, TOPK), ((0, 8),), -0.2, 0.2), 0.25, 0.75)
    prefix = set_ends(jax.random.randint(splits[15], (SEQS,), max(1, SEQ // 10), SEQ // 2 + 1), jax.random.fold_in(splits[15], 1), max(1, SEQ // 10), (SEQ // 2 + 1) - 1).astype(jnp.int32)
    cotangent = gaussian(splits[16], (TOKENS, MODEL_DIM), 1.0, 6.0, ((0, 8),))
    return {"inputs": inputs, "attn_gain": attn_gain, "w_query": w_query, "w_key": w_key, "w_value": w_value, "w_output": w_output, "ffn_gain": ffn_gain, "shared_gate": shared_gate, "shared_up": shared_up, "shared_down": shared_down, "expert_gate": expert_gate, "expert_up_slabs": expert_up_slabs, "expert_down": expert_down, "routes": routes, "gate_values": gate_values, "prefix": prefix, "cotangent": cotangent}


@jax.custom_vjp
def low(v):
    return lax.optimization_barrier(v.astype(jnp.bfloat16)).astype(jnp.float32)

@jax.custom_vjp
def low_back(v):
    return v

def low_keep(v):
    return (low(v), None)

def low_pass(kept, grad):
    return (grad,)

def back_keep(v):
    return (v, None)

def back_low(kept, grad):
    return (low(grad),)
low.defvjp(low_keep, low_pass)
low_back.defvjp(back_keep, back_low)
highest = lax.Precision.HIGHEST
epsilon = 1e-05

def matmul(left, right):
    return jnp.dot(left, right, precision=highest)

def normalize(values, gain_vec):
    return values * lax.rsqrt(lax.optimization_barrier(jnp.mean(values * values, axis=-1, keepdims=True)) + epsilon) * gain_vec

def rotary(length, head_width):
    half_width = head_width // 2
    frequency = 10000.0 ** (-jnp.arange(half_width, dtype=jnp.float32) * 2.0 / head_width)
    angles = jnp.arange(length, dtype=jnp.float32)[:, None] * frequency[None, :]
    return (jnp.cos(angles), jnp.sin(angles))

def rotate(values, cosine, sine_table):
    half_width = values.shape[-1] // 2
    first_half = values[..., :half_width]
    second = values[..., half_width:]
    cosine = cosine[:, None, :]
    sine_table = sine_table[:, None, :]
    return jnp.concatenate([first_half * cosine - second * sine_table, second * cosine + first_half * sine_table], axis=-1)

def slot_ranks(routes, block_rows, expert_count):
    expert_ids = routes.reshape(-1).astype(jnp.int32)
    blocks = expert_ids.shape[0] // block_rows
    onehot = (expert_ids[:, None] == jnp.arange(expert_count, dtype=jnp.int32)[None, :]).astype(jnp.int32)
    shaped = onehot.reshape(blocks, block_rows, expert_count)
    before = jnp.cumsum(shaped, axis=1) - shaped
    ranked = lax.optimization_barrier(jnp.sum(before.reshape(-1, expert_count) * onehot, axis=1))
    return (expert_ids, ranked.astype(jnp.int32))

def expert_apply(rows_in, gate_w, up_w, down_w):
    piece_width = gate_w.shape[2] // N_TENSOR
    total = jnp.zeros((rows_in.shape[0], down_w.shape[2]), jnp.float32)
    for slab in range(EXPERT_SLABS):
        for quarter in range(N_TENSOR):
            lower = quarter * piece_width
            upper = lower + piece_width
            entered = low_back(rows_in)
            gate_pre = low_back(matmul(entered, gate_w[slab, :, lower:upper]))
            up_pre = low_back(matmul(entered, up_w[slab, :, lower:upper]))
            hidden_act = low(jax.nn.silu(gate_pre) * up_pre)
            total = total + low(matmul(hidden_act, down_w[slab, lower:upper, :]))
    return total

def reference(inputs, attn_gain, w_query, w_key, w_value, w_output, ffn_gain, shared_gate, shared_up, shared_down, expert_gate, expert_up_slabs, expert_down, routes, gate_values, prefix, cotangent):
    cosine, sine_table = rotary(SEQ, HDIM)
    expert_ids, ranked = slot_ranks(routes, TOK_DEV * TOPK, ROUTED_EXPERTS)
    position = jnp.arange(TOKENS * TOPK, dtype=jnp.int32)
    slot_index = (position // (TOK_DEV * TOPK) * CAP_Q + ranked).astype(jnp.int32)
    buffer_len = TOKENS // TOK_DEV * CAP_Q
    gate_flat = gate_values.astype(jnp.float32).reshape(-1, 1)
    scale = HDIM ** (-0.5)
    row_ids = jnp.arange(SEQ, dtype=jnp.int32)[:, None]
    col_ids = jnp.arange(SEQ, dtype=jnp.int32)[None, :]
    slab_columns = FF_E // EXPERT_SLABS

    def layer_forward(layer_input, first_norm_gain, query_weight, key_weight, value_weight, output_weight, second_norm_gain, shared_gate_weight, shared_up_weight, shared_down_weight, expert_gate_weight, expert_up_weight, expert_down_weight):
        act_a = low(normalize(layer_input, first_norm_gain))

        def one_sequence(pair):
            act_seq, prefix_len = pair
            queries = low(rotate(low_back(matmul(act_seq, query_weight).reshape(SEQ, HEADS, HDIM)), cosine, sine_table))
            keys_rot = low(rotate(low_back(matmul(act_seq, key_weight).reshape(SEQ, HEADS, HDIM)), cosine, sine_table))
            values = low(low_back(matmul(act_seq, value_weight))).reshape(SEQ, HEADS, HDIM)
            scores = low_back(jnp.einsum('qhd,khd->hqk', queries, keys_rot, precision=highest) * scale)
            allowed = (col_ids <= row_ids) | (col_ids < prefix_len)
            probs = low(jax.nn.softmax(jnp.where(allowed[None], scores, -1e+30), axis=-1))
            attended = jnp.einsum('hqk,khd->qhd', probs, values, precision=highest).reshape(SEQ, MODEL_DIM)
            attended = low(low_back(attended))
            return low_back(matmul(attended, output_weight))
        attn_out = lax.map(jax.checkpoint(one_sequence), (act_a.reshape(SEQS, SEQ, MODEL_DIM), prefix))
        hidden = layer_input + attn_out.reshape(TOKENS, MODEL_DIM)
        act_b = low(normalize(hidden, second_norm_gain))
        shared_act = low(jax.nn.silu(low_back(matmul(act_b, shared_gate_weight))) * low_back(matmul(act_b, shared_up_weight)))
        shared_out = matmul(shared_act, shared_down_weight)
        buffers = jnp.zeros((ROUTED_EXPERTS, buffer_len, MODEL_DIM), jnp.float32).at[expert_ids, slot_index].set(jnp.repeat(act_b, TOPK, axis=0))
        gate_four = expert_gate_weight.reshape(ROUTED_EXPERTS, EXPERT_SLABS, MODEL_DIM, slab_columns)
        up_four_way = expert_up_weight.reshape(ROUTED_EXPERTS, EXPERT_SLABS, MODEL_DIM, slab_columns)
        down_four = expert_down_weight.reshape(ROUTED_EXPERTS, EXPERT_SLABS, slab_columns, MODEL_DIM)

        def one_expert(item):
            return expert_apply(item[0], item[1], item[2], item[3])
        results = lax.map(jax.checkpoint(one_expert), (buffers, gate_four, up_four_way, down_four))
        picked = low_back(results[expert_ids, slot_index])
        routed = lax.optimization_barrier(jnp.sum((gate_flat * picked).reshape(TOKENS, TOPK, MODEL_DIM), axis=1))
        return hidden + shared_out + routed
    floats = (inputs.astype(jnp.float32), attn_gain.astype(jnp.float32), w_query.astype(jnp.float32), w_key.astype(jnp.float32), w_value.astype(jnp.float32), w_output.astype(jnp.float32), ffn_gain.astype(jnp.float32), shared_gate.astype(jnp.float32), shared_up.astype(jnp.float32), shared_down.astype(jnp.float32), expert_gate.astype(jnp.float32), expert_up_slabs.astype(jnp.float32), expert_down.astype(jnp.float32))
    layer_out, pullback = jax.vjp(layer_forward, *floats)
    grads = pullback(cotangent.astype(jnp.float32))
    return (layer_out, grads[0], grads[1], grads[2], grads[3], grads[4], grads[5], grads[6], grads[7], grads[8], grads[9], grads[10], grads[11], grads[12])
```

```python
import functools

import jax
import jax.numpy as jnp
import numpy as np
from jax import lax
from jax.experimental import pallas as pl
from jax.experimental.pallas import tpu as pltpu
from jax.sharding import PartitionSpec as P

HDIM = 64
ROUTED_EXPERTS = 16
EPS = 1e-05
F32 = jnp.float32
BF16 = jnp.bfloat16
ROPE_STEP = 32

VMEM = pl.BlockSpec(memory_space=pltpu.VMEM)
SMEM = pl.BlockSpec(memory_space=pltpu.SMEM)
ANY = pl.BlockSpec(memory_space=pl.ANY)


def sds(shape, dtype):
    return jax.ShapeDtypeStruct(tuple(shape), dtype)


def params(n_grid=0):
    if n_grid:
        return pltpu.CompilerParams(
            vmem_limit_bytes=60 * 1024 * 1024, dimension_semantics=("arbitrary",) * n_grid
        )
    return pltpu.CompilerParams(vmem_limit_bytes=60 * 1024 * 1024)


def nn(a, b):
    return jnp.dot(a, b, preferred_element_type=F32)


def nt(a, b):
    return lax.dot_general(a, b, (((1,), (1,)), ((), ())), preferred_element_type=F32)


def tn(a, b):
    return lax.dot_general(a, b, (((0,), (0,)), ((), ())), preferred_element_type=F32)


def swap(x, bit):
    count = lax.axis_size("tensor")
    return lax.ppermute(x, "tensor", [(i, i ^ bit) for i in range(count)])


def rope_parts(seq_len, width):
    half = HDIM // 2
    frequency = 10000.0 ** (-np.arange(half, dtype=np.float64) * 2.0 / HDIM)
    lanes = np.tile(np.concatenate([frequency, frequency]), width // HDIM)
    sign = np.tile(np.concatenate([-np.ones(half), np.ones(half)]), width // HDIM)
    coarse = np.arange(0, seq_len, ROPE_STEP)[:, None] * lanes[None, :]
    fine = np.arange(ROPE_STEP)[:, None] * lanes[None, :]
    return tuple(
        jnp.asarray(a, dtype=F32)
        for a in (np.cos(coarse), np.sin(coarse), np.cos(fine), np.sin(fine), sign[None, :])
    )


def fill_rope(cos_coarse, sin_coarse, cos_fine, sin_fine, sign, cos_out, sin_out):
    cf, sf, sg = cos_fine[...], sin_fine[...], sign[...]

    def step(a, _):
        cc = cos_coarse[pl.ds(a, 1), :]
        sc = sin_coarse[pl.ds(a, 1), :]
        at = pl.ds(pl.multiple_of(a * ROPE_STEP, ROPE_STEP), ROPE_STEP)
        cos_out[at, :] = cc * cf - sc * sf
        sin_out[at, :] = (sc * cf + cc * sf) * sg
        return 0

    lax.fori_loop(0, cos_coarse.shape[0], step, 0)


def half_swap_matrix(width):
    row = lax.broadcasted_iota(jnp.int32, (width, width), 0)
    col = lax.broadcasted_iota(jnp.int32, (width, width), 1)
    half = HDIM // 2
    partner = jnp.where((col & half) == 0, col + half, col - half)
    return jnp.where(row == partner, 1.0, 0.0).astype(BF16)


def rms(values):
    return lax.rsqrt(jnp.mean(values * values, axis=-1, keepdims=True) + EPS)


def slot_pick(codes_k0, codes_k1, slot_code):
    first = codes_k0 == slot_code
    second = codes_k1 == slot_code
    return first, second


def prep_body(cap, tb, where_ref, routes_ref, gates_ref, slot_ref, dy_ref, codes_ref, rows_ref):
    t = where_ref[0]
    blocks = routes_ref.shape[0]
    upper = jnp.where(
        lax.broadcasted_iota(jnp.int32, (tb, tb), 0) < lax.broadcasted_iota(jnp.int32, (tb, tb), 1),
        1.0,
        0.0,
    ).astype(BF16)
    ids = lax.broadcasted_iota(jnp.int32, (ROUTED_EXPERTS, tb), 0)
    for b in range(blocks):
        r0 = routes_ref[b, 0:1, :]
        r1 = routes_ref[b, 1:2, :]
        e0 = ids == r0
        e1 = ids == r1
        named = jnp.where(e0, 1.0, 0.0) + jnp.where(e1, 1.0, 0.0)
        before = nn(named.astype(BF16), upper)
        k0 = jnp.sum(jnp.where(e0, before, 0.0), axis=0, keepdims=True)
        k1 = jnp.sum(jnp.where(e1, before, 0.0), axis=0, keepdims=True)
        codes_ref[b, 0:1, :] = r0 * cap + k0.astype(jnp.int32)
        codes_ref[b, 1:2, :] = r1 * cap + k1.astype(jnp.int32)
    dests, exp_dev, pair = rows_ref.shape[:3]
    slot_code = slot_ref[...]
    for j in range(pair):
        b = t ^ (2 * j)
        first, second = slot_pick(codes_ref[b, 0:1, :], codes_ref[b, 1:2, :], slot_code)
        g0 = gates_ref[b, 0:1, :]
        g1 = gates_ref[b, 1:2, :]
        gate = jnp.sum(
            jnp.where(first, g0, 0.0) + jnp.where(second, g1, 0.0), axis=1, keepdims=True
        )
        pick = jnp.where(first | second, 1.0, 0.0).astype(BF16)
        got = nn(pick, dy_ref[pl.ds(pl.multiple_of(b * tb, tb), tb), :]) * gate
        rows_ref[:, :, j] = got.astype(BF16).reshape(dests, exp_dev, cap, got.shape[1])


def attend_body(
    tb,
    info_ref,
    x0,
    x1,
    x2,
    x3,
    gain_ref,
    wq_ref,
    wk_ref,
    wv_ref,
    wo_ref,
    cos_coarse,
    sin_coarse,
    cos_fine,
    sin_fine,
    sign,
    act_ref,
    q_ref,
    k_ref,
    v_ref,
    att_ref,
    lse_ref,
    out0,
    out1,
    out2,
    out3,
    cos_s,
    sin_s,
):
    t = info_ref[0]
    prefix = info_ref[1]
    seq_len, width = q_ref.shape
    blocks = seq_len // tb
    heads = width // HDIM
    fill_rope(cos_coarse, sin_coarse, cos_fine, sin_fine, sign, cos_s, sin_s)
    gain = gain_ref[...]
    for j, piece in enumerate((x0, x1, x2, x3)):
        x = piece[...].astype(F32)
        at = pl.ds(pl.multiple_of((t ^ j) * tb, tb), tb)
        act_ref[at, :] = (x * rms(x) * gain).astype(BF16)
    flip = half_swap_matrix(width)
    wq = wq_ref[...]
    wk = wk_ref[...]
    wq_flip = nn(wq, flip).astype(BF16)
    wk_flip = nn(wk, flip).astype(BF16)
    scale = HDIM ** (-0.5)

    def project(b, _):
        at = pl.ds(pl.multiple_of(b * tb, tb), tb)
        a = act_ref[at, :]
        cos, sin = cos_s[at, :], sin_s[at, :]
        q_ref[at, :] = (scale * (nn(a, wq) * cos + nn(a, wq_flip) * sin)).astype(BF16)
        k_ref[at, :] = (nn(a, wk) * cos + nn(a, wk_flip) * sin).astype(BF16)
        v_ref[at, :] = nn(a, wv_ref[...]).astype(BF16)
        return 0

    lax.fori_loop(0, blocks, project, 0)
    lane_head = lax.broadcasted_iota(jnp.int32, (tb, width), 1) // HDIM
    lane = lax.broadcasted_iota(jnp.int32, (tb, lse_ref.shape[1]), 1)
    for b in range(blocks):
        extent = max(seq_len // 2, (b + 1) * tb)
        rows = slice(b * tb, (b + 1) * tb)
        qb = q_ref[rows, :]
        limit = jnp.maximum(
            b * tb + lax.broadcasted_iota(jnp.int32, (tb, 1), 0), prefix - 1
        )
        allowed = lax.broadcasted_iota(jnp.int32, (tb, extent), 1) <= limit

        def one_head(h, carried, extent=extent, qb=qb, allowed=allowed):
            att, lse = carried
            mine = lane_head == h
            scores = nt(jnp.where(mine, qb, jnp.zeros_like(qb)), k_ref[:extent, :])
            scores = jnp.where(allowed, scores, -1e30)
            top = jnp.max(scores, axis=-1, keepdims=True)
            weight = jnp.exp(scores - top)
            total = jnp.sum(weight, axis=-1, keepdims=True)
            got = nn(weight.astype(BF16), v_ref[:extent, :]) / total
            att = jnp.where(mine, got, att)
            lse = jnp.where(lane == h, top + jnp.log(total), lse)
            return att, lse

        att, lse = lax.fori_loop(
            0,
            heads,
            one_head,
            (jnp.zeros((tb, width), F32), jnp.zeros((tb, lse_ref.shape[1]), F32)),
        )
        att = att.astype(BF16)
        att_ref[rows, :] = att
        lse_ref[rows, :] = lse
        part = nn(att, wo_ref[...]).astype(BF16)
        for j, out in enumerate((out0, out1, out2, out3)):

            @pl.when((t ^ b) == j)
            def _(out=out, part=part):
                out[...] = part


def dispatch_body(t_blocks, cap, where_ref, x_ref, p0, p1, p2, gain_ref, codes_ref, *rest):
    slots = rest[: t_blocks]
    hidden_ref, act_ref = rest[t_blocks : t_blocks + 2]
    bufs = rest[t_blocks + 2 :]
    t = where_ref[0]
    hidden = (
        x_ref[...].astype(F32)
        + p0[...].astype(F32)
        + p1[...].astype(F32)
        + p2[...].astype(F32)
    )
    hidden_ref[...] = hidden
    act = (hidden * rms(hidden) * gain_ref[...]).astype(BF16)
    act_ref[...] = act
    c0 = codes_ref[t, 0:1, :]
    c1 = codes_ref[t, 1:2, :]
    for slot_ref, buf in zip(slots, bufs, strict=True):
        first, second = slot_pick(c0, c1, slot_ref[...])
        pick = jnp.where(first | second, 1.0, 0.0).astype(BF16)
        got = nn(pick, act).astype(BF16)
        buf[...] = got.reshape(buf.shape)


def shared_body(
    tb,
    where_ref,
    a0,
    a1,
    a2,
    a3,
    dy_ref,
    gate_ref,
    up_ref,
    down_ref,
    f0,
    f1,
    f2,
    f3,
    b0,
    b1,
    b2,
    b3,
    grads_ref,
    act_s,
    dy_s,
    hs_s,
    dg_s,
    du_s,
    f_s,
    b_s,
):
    t = where_ref[0]
    blocks = 4
    for j, piece in enumerate((a0, a1, a2, a3)):
        act_s[j * tb : (j + 1) * tb, :] = piece[...]
        dy_s[j * tb : (j + 1) * tb, :] = dy_ref[pl.ds(pl.multiple_of((t ^ j) * tb, tb), tb), :]

    def block(j, _):
        at = pl.ds(pl.multiple_of(j * tb, tb), tb)
        a = act_s[at, :]
        dy = dy_s[at, :]
        g = nn(a, gate_ref[...])
        u = nn(a, up_ref[...])
        sig = jax.nn.sigmoid(g)
        silu = g * sig
        hs = (silu * u).astype(BF16)
        dhs = nt(dy, down_ref[...])
        dg = (dhs * u * sig * (1.0 + g * (1.0 - sig))).astype(BF16)
        du = (dhs * silu).astype(BF16)
        hs_s[at, :] = hs
        dg_s[at, :] = dg
        du_s[at, :] = du
        f_s[at, :] = nn(hs, down_ref[...]).astype(BF16)
        b_s[at, :] = (nt(dg, gate_ref[...]) + nt(du, up_ref[...])).astype(BF16)
        return 0

    lax.fori_loop(0, blocks, block, 0)
    for j, (f, b) in enumerate(((f0, b0), (f1, b1), (f2, b2), (f3, b3))):
        f[...] = f_s[j * tb : (j + 1) * tb, :]
        b[...] = b_s[j * tb : (j + 1) * tb, :]
    hidden = hs_s.shape[1]

    def columns(c, _):
        at = pl.ds(pl.multiple_of(c * tb, tb), tb)
        a = act_s[:, at]
        dy = dy_s[:, at]
        grads_ref[at, 0:hidden] = tn(a, dg_s[...]).astype(BF16)
        grads_ref[at, hidden : 2 * hidden] = tn(a, du_s[...]).astype(BF16)
        grads_ref[at, 2 * hidden : 3 * hidden] = tn(dy, hs_s[...]).astype(BF16)
        return 0

    lax.fori_loop(0, act_s.shape[1] // tb, columns, 0)


def expert_body(x0, x1, x2, x3, c_ref, cs_ref, gate_ref, up_ref, down_ref, *outs):
    o = outs[:4]
    he_ref, dg_ref, du_ref = outs[4:7]
    n_src, cap, dim = x0.shape
    rows = n_src * cap
    gate = gate_ref[0]
    up = up_ref[0]
    down = down_ref[0]
    cots = {0: (c_ref, 0), 2: (c_ref, 1), 1: (cs_ref, 0), 3: (cs_ref, 1)}
    xs = (x0, x1, x2, x3)
    for j in (3, 1, 2, 0):
        x = xs[j][...].reshape(rows, dim)
        ref, i = cots[j]
        c = ref[:, 0, i].reshape(rows, dim)
        g = nn(x, gate)
        u = nn(x, up)
        sig = jax.nn.sigmoid(g)
        silu = g * sig
        dhe = nt(c, down)
        dg = (dhe * u * sig * (1.0 + g * (1.0 - sig))).astype(BF16)
        du = (dhe * silu).astype(BF16)
        he_ref[j] = (silu * u).astype(BF16)
        dg_ref[j] = dg
        du_ref[j] = du
        o[j][...] = (nt(dg, gate) + nt(du, up)).astype(BF16).reshape(n_src, cap, dim)


def weights_body(aliased, x0, x1, x2, x3, c_ref, cs_ref, he_ref, dg_ref, du_ref, down_ref, *rest):
    if aliased:
        rest = rest[3:]
    o = rest[:4]
    gg_ref, gu_ref, gd_ref, x_s, c_s = rest[4:]
    n_src, cap, dim = x0.shape
    rows = n_src * cap
    step = pl.program_id(0)
    down = down_ref[0]
    cots = {0: (c_ref, 0), 2: (c_ref, 1), 1: (cs_ref, 0), 3: (cs_ref, 1)}
    for j, x in enumerate((x0, x1, x2, x3)):
        ref, i = cots[j]
        x_s[j * rows : (j + 1) * rows, :] = x[...].reshape(rows, dim)
        c_s[j * rows : (j + 1) * rows, :] = ref[:, 0, i].reshape(rows, dim)
        o[j][...] = nn(he_ref[j], down).astype(BF16).reshape(n_src, cap, dim)
    hidden = he_ref.shape[2]
    he = he_ref[...].reshape(4 * rows, hidden)
    dg = dg_ref[...].reshape(4 * rows, hidden)
    du = du_ref[...].reshape(4 * rows, hidden)
    gg = tn(x_s[...], dg)
    gu = tn(x_s[...], du)
    gd = tn(he, c_s[...])

    @pl.when(step == 0)
    def _():
        gg_ref[0] = gg
        gu_ref[0] = gu
        gd_ref[0] = gd

    @pl.when(step > 0)
    def _():
        gg_ref[0] += gg
        gu_ref[0] += gu
        gd_ref[0] += gd


def home_body(n_le, tb, where_ref, *rest):
    backs = rest[:n_le]
    slots = rest[n_le : 2 * n_le]
    s0, s1, s2, hidden_ref, gain_ref, dy_ref, codes_ref = rest[2 * n_le : 2 * n_le + 7]
    gh_ref, dh_ref, gg_ref = rest[2 * n_le + 7 :]
    t = where_ref[0]
    db = s0[...].astype(F32) + s1[...].astype(F32) + s2[...].astype(F32)
    c0 = codes_ref[t, 0:1, :]
    c1 = codes_ref[t, 1:2, :]
    for back, slot_ref in zip(backs, slots, strict=True):
        first, second = slot_pick(c0, c1, slot_ref[...])
        pick = jnp.where(first | second, 1.0, 0.0).astype(BF16)
        db += tn(pick, back[...].reshape(pick.shape[0], db.shape[1]))
    hidden = hidden_ref[...]
    factor = rms(hidden)
    n = hidden * factor
    inner = db * gain_ref[...]
    dy = dy_ref[pl.ds(pl.multiple_of(t * tb, tb), tb), :].astype(F32)
    gh = dy + factor * (inner - n * jnp.mean(inner * n, axis=-1, keepdims=True))
    gh_ref[...] = gh
    dh_ref[...] = gh.astype(BF16)
    gg_ref[...] = jnp.sum(db * n, axis=0, keepdims=True)


def attend_back_body(
    tb,
    info_ref,
    h0,
    h1,
    h2,
    h3,
    gain_ref,
    wq_ref,
    wk_ref,
    wv_ref,
    wo_ref,
    act_ref,
    q_ref,
    k_ref,
    v_ref,
    att_ref,
    lse_ref,
    cos_coarse,
    sin_coarse,
    cos_fine,
    sin_fine,
    sign,
    o0,
    o1,
    o2,
    o3,
    gw_ref,
    gg_ref,
    cos_s,
    sin_s,
    dh_s,
    dat_s,
    qt_s,
    datt_s,
    dq_s,
    dkt_s,
    dvt_s,
    raw_s,
):
    t = info_ref[0]
    prefix = info_ref[1]
    seq_len, width = q_ref.shape
    blocks = seq_len // tb
    heads = width // HDIM
    scale = HDIM ** (-0.5)
    fill_rope(cos_coarse, sin_coarse, cos_fine, sin_fine, sign, cos_s, sin_s)
    for j, piece in enumerate((h0, h1, h2, h3)):
        at = pl.ds(pl.multiple_of((t ^ j) * tb, tb), tb)
        dh = piece[...]
        dh_s[at, :] = dh
        dat_s[at, :] = nt(dh, wo_ref[...]).astype(BF16)
    for b in range(blocks):
        rows = slice(b * tb, (b + 1) * tb)
        qt_s[:, rows] = q_ref[rows, :].T
        datt_s[:, rows] = dat_s[rows, :].T
    dkt_s[...] = jnp.zeros_like(dkt_s)
    dvt_s[...] = jnp.zeros_like(dvt_s)
    lane_head = lax.broadcasted_iota(jnp.int32, (tb, width), 1) // HDIM
    lane = lax.broadcasted_iota(jnp.int32, (tb, lse_ref.shape[1]), 1)
    for b in range(blocks):
        extent = max(seq_len // 2, (b + 1) * tb)
        rows = slice(b * tb, (b + 1) * tb)
        qb = q_ref[rows, :]
        datb = dat_s[rows, :]
        mix = datb.astype(F32) * att_ref[rows, :].astype(F32)
        lse_b = lse_ref[rows, :]
        limit = jnp.maximum(
            b * tb + lax.broadcasted_iota(jnp.int32, (tb, 1), 0), prefix - 1
        )
        allowed = lax.broadcasted_iota(jnp.int32, (tb, extent), 1) <= limit

        def one_head(h, dq, extent=extent, rows=rows, qb=qb, datb=datb, mix=mix, lse_b=lse_b, allowed=allowed):
            mine = lane_head == h
            lse = jnp.sum(jnp.where(lane == h, lse_b, 0.0), axis=-1, keepdims=True)
            delta = jnp.sum(jnp.where(mine, mix, 0.0), axis=-1, keepdims=True)
            scores = nt(jnp.where(mine, qb, jnp.zeros_like(qb)), k_ref[:extent, :])
            prob = jnp.exp(jnp.where(allowed, scores, -1e30) - lse)
            dp = nt(jnp.where(mine, datb, jnp.zeros_like(datb)), v_ref[:extent, :])
            ds = (prob * (dp - delta)).astype(BF16)
            at = pl.ds(pl.multiple_of(h * HDIM, HDIM), HDIM)
            dkt_s[at, :extent] += nn(qt_s[at, rows], ds)
            dvt_s[at, :extent] += nn(datt_s[at, rows], prob.astype(BF16))
            return jnp.where(mine, nn(ds, k_ref[:extent, :]), dq)

        dq_s[rows, :] = lax.fori_loop(0, heads, one_head, jnp.zeros((tb, width), F32))
    flip = half_swap_matrix(width)

    def unrotate(u, at):
        high = u.astype(BF16)
        low = (u - high.astype(F32)).astype(BF16)
        return (u * cos_s[at, :] - (nn(high, flip) + nn(low, flip)) * sin_s[at, :]).astype(BF16)

    gain_sum = jnp.zeros((1, act_ref.shape[1]), F32)
    for b in range(blocks):
        rows = slice(b * tb, (b + 1) * tb)
        dq = unrotate(dq_s[rows, :] * scale, rows)
        dk = unrotate(dkt_s[:, rows].T, rows)
        dv = dvt_s[:, rows].T.astype(BF16)
        raw_s[0, rows, :] = dq
        raw_s[1, rows, :] = dk
        raw_s[2, rows, :] = dv
        da = nt(dq, wq_ref[...]) + nt(dk, wk_ref[...]) + nt(dv, wv_ref[...])
        gain_sum += jnp.sum(da * act_ref[rows, :].astype(F32), axis=0, keepdims=True)
        part = da.astype(BF16)
        for j, out in enumerate((o0, o1, o2, o3)):

            @pl.when((t ^ b) == j)
            def _(out=out, part=part):
                out[...] = part

    gg_ref[...] = gain_sum / gain_ref[...]
    for i in range(3):
        gw_ref[i] = tn(raw_s[i], act_ref[...]).T.astype(BF16)
    gw_ref[3] = tn(att_ref[...], dh_s[...]).T.astype(BF16)


def layer_out_body(n_le, where_ref, *rest):
    backs = rest[:n_le]
    slots = rest[n_le : 2 * n_le]
    hidden_ref, s0, s1, s2, codes_ref, gates_ref, out_ref = rest[2 * n_le :]
    t = where_ref[0]
    out = (
        hidden_ref[...] + s0[...].astype(F32) + s1[...].astype(F32) + s2[...].astype(F32)
    )
    c0 = codes_ref[t, 0:1, :]
    c1 = codes_ref[t, 1:2, :]
    g0 = gates_ref[t, 0:1, :]
    g1 = gates_ref[t, 1:2, :]
    for back, slot_ref in zip(backs, slots, strict=True):
        first, second = slot_pick(c0, c1, slot_ref[...])
        weight = jnp.where(first, g0, 0.0) + jnp.where(second, g1, 0.0)
        high = weight.astype(BF16)
        low = (weight - high.astype(F32)).astype(BF16)
        rows = back[...].reshape(high.shape[0], out.shape[1])
        out += tn(high, rows) + tn(low, rows)
    out_ref[...] = out


def grad_in_body(x_ref, p0, p1, p2, gh_ref, gain_ref, out_ref):
    x = x_ref[...].astype(F32)
    da = p0[...].astype(F32) + p1[...].astype(F32) + p2[...].astype(F32)
    factor = rms(x)
    n = x * factor
    inner = da * gain_ref[...]
    out_ref[...] = gh_ref[...] + factor * (
        inner - n * jnp.mean(inner * n, axis=-1, keepdims=True)
    )


def add2(a, b):
    return (a.astype(F32) + b.astype(F32)).astype(BF16)


def to_owner(pieces):
    r3 = swap(pieces[3], 1)
    r1 = swap(pieces[1], 1)
    rx = swap(add2(pieces[2], r3), 2)
    return pieces[0], r1, rx


def to_all(own):
    across = swap(own, 2)
    beside = swap(own, 1)
    both = swap(across, 1)
    return own, beside, across, both


def over_expert(x, expert_count):
    got = lax.all_to_all(
        x.reshape(expert_count, -1, x.shape[-1]), "expert", split_axis=0, concat_axis=0, tiled=True
    )
    return jnp.sum(got.astype(F32), axis=0)


def per_device(
    inputs,
    attn_gain,
    w_query,
    w_key,
    w_value,
    w_output,
    ffn_gain,
    shared_gate,
    shared_up,
    shared_down,
    expert_gate,
    expert_up,
    expert_down,
    routes,
    gate_values,
    prefix,
    cotangent,
):
    tensor_count = lax.axis_size("tensor")
    expert_count = lax.axis_size("expert")
    assert tensor_count == 4
    t = lax.axis_index("tensor")
    tb, dim = inputs.shape
    seq_len, choices = routes.shape
    width = w_query.shape[1]
    hidden_units = shared_gate.shape[1]
    exp_hidden = expert_gate.shape[2]
    exp_dev = expert_gate.shape[0]
    slabs = max(1, expert_count // ROUTED_EXPERTS)
    cap = max(2, 3 * tb * choices // (2 * ROUTED_EXPERTS))
    where = jnp.reshape(t, (1,)).astype(jnp.int32)
    info = jnp.stack([t.astype(jnp.int32), prefix[0]])
    gain_a = attn_gain.reshape(1, dim)
    gain_b = ffn_gain.reshape(1, dim)

    entries = np.arange(expert_count * exp_dev)
    slot_np = (entries // slabs)[:, None] * cap + np.arange(cap)[None, :]
    slot_np = slot_np.reshape(expert_count, exp_dev, cap).astype(np.int32)
    slot_all = jnp.asarray(slot_np.reshape(-1, 1))
    slot_le = [jnp.asarray(slot_np[:, le].reshape(-1, 1)) for le in range(exp_dev)]

    x0, x1, x2, x3 = to_all(inputs)

    routes_b = routes.reshape(tensor_count, tb, choices).transpose(0, 2, 1)
    gates_b = gate_values.reshape(tensor_count, tb, choices).transpose(0, 2, 1)
    codes, cot_rows = pl.pallas_call(
        functools.partial(prep_body, cap, tb),
        out_shape=(
            sds((tensor_count, choices, tb), jnp.int32),
            sds((expert_count, exp_dev, 2, cap, dim), BF16),
        ),
        in_specs=[SMEM, VMEM, VMEM, VMEM, VMEM],
        out_specs=(VMEM, VMEM),
        compiler_params=params(),
        name="prep",
    )(where, routes_b, gates_b, slot_all, cotangent)
    cot = lax.all_to_all(cot_rows, "expert", split_axis=0, concat_axis=0, tiled=True)
    cot_beside = swap(cot, 1)

    rope = rope_parts(seq_len, width)
    block = sds((tb, dim), BF16)
    att_out = pl.pallas_call(
        functools.partial(attend_body, tb),
        out_shape=(
            sds((seq_len, dim), BF16),
            sds((seq_len, width), BF16),
            sds((seq_len, width), BF16),
            sds((seq_len, width), BF16),
            sds((seq_len, width), BF16),
            sds((seq_len, 128), F32),
            block,
            block,
            block,
            block,
        ),
        in_specs=[SMEM] + [VMEM] * 14,
        out_specs=(VMEM,) * 10,
        scratch_shapes=[pltpu.VMEM((seq_len, width), F32)] * 2,
        compiler_params=params(),
        name="attend",
    )(info, x0, x1, x2, x3, gain_a, w_query, w_key, w_value, w_output, *rope)
    act_a, q, k, v, att, lse = att_out[:6]
    parts = to_owner(att_out[6:])

    got = pl.pallas_call(
        functools.partial(dispatch_body, exp_dev, cap),
        out_shape=(sds((tb, dim), F32), block)
        + (sds((expert_count, cap, dim), BF16),) * exp_dev,
        in_specs=[SMEM] + [VMEM] * (6 + exp_dev),
        out_specs=(VMEM,) * (2 + exp_dev),
        compiler_params=params(),
        name="dispatch",
    )(where, inputs, *parts, gain_b, codes, *slot_le)
    hidden, act_b = got[:2]
    rows_x = []
    for le in range(exp_dev):
        p0 = lax.all_to_all(got[2 + le], "expert", split_axis=0, concat_axis=0, tiled=True)
        rows_x.append(to_all(p0))

    a_all = to_all(act_b)
    sh = pl.pallas_call(
        functools.partial(shared_body, tb),
        out_shape=(block,) * 8 + (sds((dim, 3 * hidden_units), BF16),),
        in_specs=[SMEM] + [VMEM] * 8,
        out_specs=(VMEM,) * 9,
        scratch_shapes=[
            pltpu.VMEM((seq_len, dim), BF16),
            pltpu.VMEM((seq_len, dim), BF16),
            pltpu.VMEM((seq_len, hidden_units), BF16),
            pltpu.VMEM((seq_len, hidden_units), BF16),
            pltpu.VMEM((seq_len, hidden_units), BF16),
            pltpu.VMEM((seq_len, dim), BF16),
            pltpu.VMEM((seq_len, dim), BF16),
        ],
        compiler_params=params(),
        name="shared",
    )(where, *a_all, cotangent, shared_gate, shared_up, shared_down)
    shared_back = to_owner(sh[4:8])
    shared_fwd = to_owner(sh[0:4])
    shared_grads = over_expert(sh[8], expert_count)

    src = min(8, expert_count)
    steps = expert_count // src
    rows_blk = pl.BlockSpec((src, cap, dim), lambda i: (i, 0, 0))
    saved_blk = pl.BlockSpec((4, src * cap, exp_hidden), lambda i: (0, i, 0))

    def weight_blk(le, a, b):
        return pl.BlockSpec((1, a, b), lambda i: (le, 0, 0))

    def cot_blk(le):
        return pl.BlockSpec((src, 1, 2, cap, dim), lambda i: (i, le, 0, 0, 0))

    all_rows = expert_count * cap
    row_out = sds((expert_count, cap, dim), BF16)
    saved_out = sds((4, all_rows, exp_hidden), BF16)
    saved = []
    home_rows = []
    for le in range(exp_dev):
        res = pl.pallas_call(
            expert_body,
            grid=(steps,),
            out_shape=(row_out,) * 4 + (saved_out,) * 3,
            in_specs=[rows_blk] * 4
            + [cot_blk(le)] * 2
            + [
                weight_blk(le, dim, exp_hidden),
                weight_blk(le, dim, exp_hidden),
                weight_blk(le, exp_hidden, dim),
            ],
            out_specs=(rows_blk,) * 4 + (saved_blk,) * 3,
            compiler_params=params(1),
            name="expert",
        )(*rows_x[le], cot, cot_beside, expert_gate, expert_up, expert_down)
        saved.append(res[4:])
        p0, r1, rx = to_owner(res[:4])
        mine = (p0.astype(F32) + r1.astype(F32) + rx.astype(F32)).astype(BF16)
        home_rows.append(
            lax.all_to_all(mine, "expert", split_axis=0, concat_axis=0, tiled=True)
        )

    grads = None
    home_res = []
    for le in range(exp_dev):
        args = (*rows_x[le], cot, cot_beside, *saved[le], expert_down)
        in_specs = (
            [rows_blk] * 4 + [cot_blk(le)] * 2 + [saved_blk] * 3 + [weight_blk(le, exp_hidden, dim)]
        )
        aliases = {}
        if grads is not None:
            aliases = {len(args) + i: 4 + i for i in range(3)}
            args = args + tuple(grads)
            in_specs = in_specs + [ANY] * 3
        res = pl.pallas_call(
            functools.partial(weights_body, grads is not None),
            grid=(steps,),
            out_shape=(row_out,) * 4
            + (
                sds((exp_dev, dim, exp_hidden), F32),
                sds((exp_dev, dim, exp_hidden), F32),
                sds((exp_dev, exp_hidden, dim), F32),
            ),
            in_specs=in_specs,
            out_specs=(rows_blk,) * 4
            + (
                weight_blk(le, dim, exp_hidden),
                weight_blk(le, dim, exp_hidden),
                weight_blk(le, exp_hidden, dim),
            ),
            scratch_shapes=[
                pltpu.VMEM((4 * src * cap, dim), BF16),
                pltpu.VMEM((4 * src * cap, dim), BF16),
            ],
            input_output_aliases=aliases,
            compiler_params=params(1),
            name="weights",
        )(*args)
        grads = res[4:]
        p0, r1, rx = to_owner(res[:4])
        mine = (p0.astype(F32) + r1.astype(F32) + rx.astype(F32)).astype(BF16)
        home_res.append(
            lax.all_to_all(mine, "expert", split_axis=0, concat_axis=0, tiled=True)
        )

    grad_hidden, dh, gain_ffn = pl.pallas_call(
        functools.partial(home_body, exp_dev, tb),
        out_shape=(sds((tb, dim), F32), block, sds((1, dim), F32)),
        in_specs=[SMEM] + [VMEM] * (2 * exp_dev + 7),
        out_specs=(VMEM,) * 3,
        compiler_params=params(),
        name="home",
    )(where, *home_rows, *slot_le, *shared_back, hidden, gain_b, cotangent, codes)

    h_all = to_all(dh)
    back = pl.pallas_call(
        functools.partial(attend_back_body, tb),
        out_shape=(block,) * 4 + (sds((4, dim, width), BF16), sds((1, dim), F32)),
        in_specs=[SMEM] + [VMEM] * 20,
        out_specs=(VMEM,) * 6,
        scratch_shapes=[
            pltpu.VMEM((seq_len, width), F32),
            pltpu.VMEM((seq_len, width), F32),
            pltpu.VMEM((seq_len, dim), BF16),
            pltpu.VMEM((seq_len, width), BF16),
            pltpu.VMEM((width, seq_len), BF16),
            pltpu.VMEM((width, seq_len), BF16),
            pltpu.VMEM((seq_len, width), F32),
            pltpu.VMEM((width, seq_len), F32),
            pltpu.VMEM((width, seq_len), F32),
            pltpu.VMEM((3, seq_len, width), BF16),
        ],
        compiler_params=params(),
        name="attend_back",
    )(
        info,
        *h_all,
        gain_a,
        w_query,
        w_key,
        w_value,
        w_output,
        act_a,
        q,
        k,
        v,
        att,
        lse,
        *rope,
    )
    da_parts = to_owner(back[:4])
    devices = expert_count * tensor_count
    both_gains = jnp.concatenate([back[5], gain_ffn], axis=0)
    gains = jnp.sum(
        lax.all_to_all(
            jnp.broadcast_to(both_gains[None], (devices, 2, dim)),
            ("expert", "tensor"),
            split_axis=0,
            concat_axis=0,
            tiled=True,
        ),
        axis=0,
    )
    gw = lax.all_to_all(
        back[4].reshape(4, expert_count, dim // expert_count, width),
        "expert",
        split_axis=1,
        concat_axis=1,
        tiled=True,
    )
    gw = jnp.sum(gw.astype(F32), axis=1)

    grad_inputs = pl.pallas_call(
        grad_in_body,
        out_shape=sds((tb, dim), F32),
        in_specs=[VMEM] * 6,
        out_specs=VMEM,
        compiler_params=params(),
        name="grad_in",
    )(inputs, *da_parts, grad_hidden, gain_a)
    layer_out = pl.pallas_call(
        functools.partial(layer_out_body, exp_dev),
        out_shape=sds((tb, dim), F32),
        in_specs=[SMEM] + [VMEM] * (2 * exp_dev + 6),
        out_specs=VMEM,
        compiler_params=params(),
        name="layer_out",
    )(where, *home_res, *slot_le, hidden, *shared_fwd, codes, gates_b)
    return (
        layer_out,
        grad_inputs,
        gains[0],
        gw[0],
        gw[1],
        gw[2],
        gw[3].T,
        gains[1],
        shared_grads[:, :hidden_units],
        shared_grads[:, hidden_units : 2 * hidden_units],
        shared_grads[:, 2 * hidden_units :].T,
        grads[0],
        grads[1],
        grads[2],
    )


def solution(mesh):
    return jax.shard_map(
        per_device,
        mesh=mesh,
        in_specs=(
            P(("expert", "tensor"), None),
            P(),
            P(None, "tensor"),
            P(None, "tensor"),
            P(None, "tensor"),
            P("tensor", None),
            P(),
            P(None, "tensor"),
            P(None, "tensor"),
            P("tensor", None),
            P("expert", None, "tensor"),
            P("expert", None, "tensor"),
            P("expert", "tensor", None),
            P("expert", None),
            P("expert", None),
            P("expert"),
            P("expert", None),
        ),
        out_specs=(
            P(("expert", "tensor"), None),
            P(("expert", "tensor"), None),
            P(),
            P("expert", "tensor"),
            P("expert", "tensor"),
            P("expert", "tensor"),
            P("tensor", "expert"),
            P(),
            P("expert", "tensor"),
            P("expert", "tensor"),
            P("tensor", "expert"),
            P("expert", None, "tensor"),
            P("expert", None, "tensor"),
            P("expert", "tensor", None),
        ),
        check_vma=False,
    )
```

```python
import functools

import jax
import jax.numpy as jnp
import numpy as np
from jax import lax
from jax.experimental import pallas as pl
from jax.experimental.pallas import tpu as pltpu
from jax.sharding import PartitionSpec as P

HDIM = 64
ROUTED_EXPERTS = 16
EPS = 1e-05
F32 = jnp.float32
BF16 = jnp.bfloat16
ROPE_STEP = 32

VMEM = pl.BlockSpec(memory_space=pltpu.VMEM)
SMEM = pl.BlockSpec(memory_space=pltpu.SMEM)
ANY = pl.BlockSpec(memory_space=pl.ANY)


def sds(shape, dtype):
    return jax.ShapeDtypeStruct(tuple(shape), dtype)


def params(n_grid=0):
    if n_grid:
        return pltpu.CompilerParams(
            vmem_limit_bytes=60 * 1024 * 1024, dimension_semantics=("arbitrary",) * n_grid
        )
    return pltpu.CompilerParams(vmem_limit_bytes=60 * 1024 * 1024)


def nn(a, b):
    return jnp.dot(a, b, preferred_element_type=F32)


def nt(a, b):
    return lax.dot_general(a, b, (((1,), (1,)), ((), ())), preferred_element_type=F32)


def tn(a, b):
    return lax.dot_general(a, b, (((0,), (0,)), ((), ())), preferred_element_type=F32)


def swap(x, bit):
    count = lax.axis_size("tensor")
    return lax.ppermute(x, "tensor", [(i, i ^ bit) for i in range(count)])


def rope_parts(seq_len, width):
    half = HDIM // 2
    frequency = 10000.0 ** (-np.arange(half, dtype=np.float64) * 2.0 / HDIM)
    lanes = np.tile(np.concatenate([frequency, frequency]), width // HDIM)
    sign = np.tile(np.concatenate([-np.ones(half), np.ones(half)]), width // HDIM)
    coarse = np.arange(0, seq_len, ROPE_STEP)[:, None] * lanes[None, :]
    fine = np.arange(ROPE_STEP)[:, None] * lanes[None, :]
    return tuple(
        jnp.asarray(a, dtype=F32)
        for a in (np.cos(coarse), np.sin(coarse), np.cos(fine), np.sin(fine), sign[None, :])
    )


def fill_rope(cos_coarse, sin_coarse, cos_fine, sin_fine, sign, cos_out, sin_out):
    cf, sf, sg = cos_fine[...], sin_fine[...], sign[...]

    def step(a, _):
        cc = cos_coarse[pl.ds(a, 1), :]
        sc = sin_coarse[pl.ds(a, 1), :]
        at = pl.ds(pl.multiple_of(a * ROPE_STEP, ROPE_STEP), ROPE_STEP)
        cos_out[at, :] = cc * cf - sc * sf
        sin_out[at, :] = (sc * cf + cc * sf) * sg
        return 0

    lax.fori_loop(0, cos_coarse.shape[0], step, 0)


def half_swap_matrix(width):
    row = lax.broadcasted_iota(jnp.int32, (width, width), 0)
    col = lax.broadcasted_iota(jnp.int32, (width, width), 1)
    half = HDIM // 2
    partner = jnp.where((col & half) == 0, col + half, col - half)
    return jnp.where(row == partner, 1.0, 0.0).astype(BF16)


def rms(values):
    return lax.rsqrt(jnp.mean(values * values, axis=-1, keepdims=True) + EPS)


def slot_pick(codes_k0, codes_k1, slot_code):
    first = codes_k0 == slot_code
    second = codes_k1 == slot_code
    return first, second


def prep_body(cap, tb, where_ref, routes_ref, gates_ref, dy_ref, *rest):
    t = where_ref[0]
    blocks = routes_ref.shape[0]
    n_le = (len(rest) - 1) // 2
    slots = rest[:n_le]
    codes_ref = rest[n_le]
    outs = rest[n_le + 1 :]
    upper = jnp.where(
        lax.broadcasted_iota(jnp.int32, (tb, tb), 0) < lax.broadcasted_iota(jnp.int32, (tb, tb), 1),
        1.0,
        0.0,
    ).astype(BF16)
    ids = lax.broadcasted_iota(jnp.int32, (ROUTED_EXPERTS, tb), 0)
    for b in range(blocks):
        r0 = routes_ref[b, 0:1, :]
        r1 = routes_ref[b, 1:2, :]
        e0 = ids == r0
        e1 = ids == r1
        named = jnp.where(e0, 1.0, 0.0) + jnp.where(e1, 1.0, 0.0)
        before = nn(named.astype(BF16), upper)
        k0 = jnp.sum(jnp.where(e0, before, 0.0), axis=0, keepdims=True)
        k1 = jnp.sum(jnp.where(e1, before, 0.0), axis=0, keepdims=True)
        codes_ref[b, 0:1, :] = r0 * cap + k0.astype(jnp.int32)
        codes_ref[b, 1:2, :] = r1 * cap + k1.astype(jnp.int32)
    for slot_ref, rows_ref in zip(slots, outs, strict=True):
        slot_code = slot_ref[...]
        dests, pair = rows_ref.shape[:2]
        for j in range(pair):
            b = t ^ (2 * j)
            first, second = slot_pick(codes_ref[b, 0:1, :], codes_ref[b, 1:2, :], slot_code)
            g0 = gates_ref[b, 0:1, :]
            g1 = gates_ref[b, 1:2, :]
            gate = jnp.sum(
                jnp.where(first, g0, 0.0) + jnp.where(second, g1, 0.0), axis=1, keepdims=True
            )
            pick = jnp.where(first | second, 1.0, 0.0).astype(BF16)
            got = nn(pick, dy_ref[pl.ds(pl.multiple_of(b * tb, tb), tb), :]) * gate
            rows_ref[:, j] = got.astype(BF16).reshape(dests, cap, got.shape[1])


def attend_body(
    tb,
    info_ref,
    x0,
    x1,
    x2,
    x3,
    gain_ref,
    wq_ref,
    wk_ref,
    wv_ref,
    wo_ref,
    cos_coarse,
    sin_coarse,
    cos_fine,
    sin_fine,
    sign,
    act_ref,
    q_ref,
    k_ref,
    v_ref,
    att_ref,
    lse_ref,
    out0,
    out1,
    out2,
    out3,
    cos_s,
    sin_s,
):
    t = info_ref[0]
    prefix = info_ref[1]
    seq_len, width = q_ref.shape
    blocks = seq_len // tb
    heads = width // HDIM
    fill_rope(cos_coarse, sin_coarse, cos_fine, sin_fine, sign, cos_s, sin_s)
    gain = gain_ref[...]
    for j, piece in enumerate((x0, x1, x2, x3)):
        x = piece[...].astype(F32)
        at = pl.ds(pl.multiple_of((t ^ j) * tb, tb), tb)
        act_ref[at, :] = (x * rms(x) * gain).astype(BF16)
    flip = half_swap_matrix(width)
    wq = wq_ref[...]
    wk = wk_ref[...]
    wq_flip = nn(flip, wq).astype(BF16)
    wk_flip = nn(flip, wk).astype(BF16)
    scale = HDIM ** (-0.5)

    def project(b, _):
        at = pl.ds(pl.multiple_of(b * tb, tb), tb)
        a = act_ref[at, :]
        cos, sin = cos_s[at, :], sin_s[at, :]
        q_ref[at, :] = (scale * (nt(a, wq) * cos + nt(a, wq_flip) * sin)).astype(BF16)
        k_ref[at, :] = (nt(a, wk) * cos + nt(a, wk_flip) * sin).astype(BF16)
        v_ref[at, :] = nt(a, wv_ref[...]).astype(BF16)
        return 0

    lax.fori_loop(0, blocks, project, 0)
    lane_head = lax.broadcasted_iota(jnp.int32, (tb, width), 1) // HDIM
    lane = lax.broadcasted_iota(jnp.int32, (tb, lse_ref.shape[1]), 1)
    for b in range(blocks):
        extent = max(seq_len // 2, (b + 1) * tb)
        rows = slice(b * tb, (b + 1) * tb)
        qb = q_ref[rows, :]
        limit = jnp.maximum(
            b * tb + lax.broadcasted_iota(jnp.int32, (tb, 1), 0), prefix - 1
        )
        allowed = lax.broadcasted_iota(jnp.int32, (tb, extent), 1) <= limit

        def one_head(h, carried, extent=extent, qb=qb, allowed=allowed):
            att, lse = carried
            mine = lane_head == h
            scores = nt(jnp.where(mine, qb, jnp.zeros_like(qb)), k_ref[:extent, :])
            scores = jnp.where(allowed, scores, -1e30)
            top = jnp.max(scores, axis=-1, keepdims=True)
            weight = jnp.exp(scores - top)
            total = jnp.sum(weight, axis=-1, keepdims=True)
            got = nn(weight.astype(BF16), v_ref[:extent, :]) / total
            att = jnp.where(mine, got, att)
            lse = jnp.where(lane == h, top + jnp.log(total), lse)
            return att, lse

        att, lse = lax.fori_loop(
            0,
            heads,
            one_head,
            (jnp.zeros((tb, width), F32), jnp.zeros((tb, lse_ref.shape[1]), F32)),
        )
        att = att.astype(BF16)
        att_ref[rows, :] = att
        lse_ref[rows, :] = lse
        part = nn(att, wo_ref[...]).astype(BF16)
        for j, out in enumerate((out0, out1, out2, out3)):

            @pl.when((t ^ b) == j)
            def _(out=out, part=part):
                out[...] = part


def dispatch_body(t_blocks, cap, where_ref, x_ref, p0, p1, p2, gain_ref, codes_ref, *rest):
    slots = rest[: t_blocks]
    hidden_ref, act_ref = rest[t_blocks : t_blocks + 2]
    bufs = rest[t_blocks + 2 :]
    t = where_ref[0]
    hidden = (
        x_ref[...].astype(F32)
        + p0[...].astype(F32)
        + p1[...].astype(F32)
        + p2[...].astype(F32)
    )
    hidden_ref[...] = hidden
    act = (hidden * rms(hidden) * gain_ref[...]).astype(BF16)
    act_ref[...] = act
    c0 = codes_ref[t, 0:1, :]
    c1 = codes_ref[t, 1:2, :]
    for slot_ref, buf in zip(slots, bufs, strict=True):
        first, second = slot_pick(c0, c1, slot_ref[...])
        pick = jnp.where(first | second, 1.0, 0.0).astype(BF16)
        got = nn(pick, act).astype(BF16)
        buf[...] = got.reshape(buf.shape)


def shared_body(
    tb,
    where_ref,
    a0,
    a1,
    a2,
    a3,
    dy_ref,
    gate_ref,
    up_ref,
    down_ref,
    f0,
    f1,
    f2,
    f3,
    b0,
    b1,
    b2,
    b3,
    grads_ref,
    act_s,
    dy_s,
    hs_s,
    dg_s,
    du_s,
    f_s,
    b_s,
):
    t = where_ref[0]
    blocks = 4
    for j, piece in enumerate((a0, a1, a2, a3)):
        act_s[j * tb : (j + 1) * tb, :] = piece[...]
        dy_s[j * tb : (j + 1) * tb, :] = dy_ref[pl.ds(pl.multiple_of((t ^ j) * tb, tb), tb), :]

    def block(j, _):
        at = pl.ds(pl.multiple_of(j * tb, tb), tb)
        a = act_s[at, :]
        dy = dy_s[at, :]
        g = nn(a, gate_ref[...])
        u = nn(a, up_ref[...])
        sig = jax.nn.sigmoid(g)
        silu = g * sig
        hs = (silu * u).astype(BF16)
        dhs = nt(dy, down_ref[...])
        dg = (dhs * u * sig * (1.0 + g * (1.0 - sig))).astype(BF16)
        du = (dhs * silu).astype(BF16)
        hs_s[at, :] = hs
        dg_s[at, :] = dg
        du_s[at, :] = du
        f_s[at, :] = nn(hs, down_ref[...]).astype(BF16)
        b_s[at, :] = (nt(dg, gate_ref[...]) + nt(du, up_ref[...])).astype(BF16)
        return 0

    lax.fori_loop(0, blocks, block, 0)
    for j, (f, b) in enumerate(((f0, b0), (f1, b1), (f2, b2), (f3, b3))):
        f[...] = f_s[j * tb : (j + 1) * tb, :]
        b[...] = b_s[j * tb : (j + 1) * tb, :]
    hidden = hs_s.shape[1]

    def columns(c, _):
        at = pl.ds(pl.multiple_of(c * tb, tb), tb)
        a = act_s[:, at]
        dy = dy_s[:, at]
        grads_ref[at, 0:hidden] = tn(a, dg_s[...]).astype(BF16)
        grads_ref[at, hidden : 2 * hidden] = tn(a, du_s[...]).astype(BF16)
        grads_ref[at, 2 * hidden : 3 * hidden] = tn(dy, hs_s[...]).astype(BF16)
        return 0

    lax.fori_loop(0, act_s.shape[1] // tb, columns, 0)


def expert_body(x0, x1, x2, x3, c0, c1, c2, c3, gate_ref, up_ref, down_ref, *outs):
    o = outs[:4]
    he_ref, dg_ref, du_ref = outs[4:7]
    n_src, cap, dim = x0.shape
    rows = n_src * cap
    gate = gate_ref[0]
    up = up_ref[0]
    down = down_ref[0]
    xs = (x0, x1, x2, x3)
    cs = (c0, c1, c2, c3)
    for j in (3, 1, 2, 0):
        x = xs[j][...].reshape(rows, dim)
        c = cs[j][...].reshape(rows, dim)
        g = nn(x, gate)
        u = nn(x, up)
        sig = jax.nn.sigmoid(g)
        silu = g * sig
        dhe = nt(c, down)
        dg = (dhe * u * sig * (1.0 + g * (1.0 - sig))).astype(BF16)
        du = (dhe * silu).astype(BF16)
        he_ref[j] = (silu * u).astype(BF16)
        dg_ref[j] = dg
        du_ref[j] = du
        o[j][...] = (nt(dg, gate) + nt(du, up)).astype(BF16).reshape(n_src, cap, dim)


def weights_body(aliased, x0, x1, x2, x3, c0, c1, c2, c3, he_ref, dg_ref, du_ref, down_ref, *rest):
    if aliased:
        rest = rest[3:]
    o = rest[:4]
    gg_ref, gu_ref, gd_ref, x_s, c_s = rest[4:]
    n_src, cap, dim = x0.shape
    rows = n_src * cap
    step = pl.program_id(0)
    down = down_ref[0]
    cs = (c0, c1, c2, c3)
    for j, x in enumerate((x0, x1, x2, x3)):
        x_s[j * rows : (j + 1) * rows, :] = x[...].reshape(rows, dim)
        c_s[j * rows : (j + 1) * rows, :] = cs[j][...].reshape(rows, dim)
        o[j][...] = nn(he_ref[j], down).astype(BF16).reshape(n_src, cap, dim)
    hidden = he_ref.shape[2]
    he = he_ref[...].reshape(4 * rows, hidden)
    dg = dg_ref[...].reshape(4 * rows, hidden)
    du = du_ref[...].reshape(4 * rows, hidden)
    gg = tn(x_s[...], dg)
    gu = tn(x_s[...], du)
    gd = tn(he, c_s[...])

    @pl.when(step == 0)
    def _():
        gg_ref[0] = gg
        gu_ref[0] = gu
        gd_ref[0] = gd

    @pl.when(step > 0)
    def _():
        gg_ref[0] += gg
        gu_ref[0] += gu
        gd_ref[0] += gd


def home_body(n_le, tb, where_ref, *rest):
    backs = rest[:n_le]
    slots = rest[n_le : 2 * n_le]
    s0, s1, s2, hidden_ref, gain_ref, dy_ref, codes_ref = rest[2 * n_le : 2 * n_le + 7]
    gh_ref, dh_ref, gg_ref = rest[2 * n_le + 7 :]
    t = where_ref[0]
    db = s0[...].astype(F32) + s1[...].astype(F32) + s2[...].astype(F32)
    c0 = codes_ref[t, 0:1, :]
    c1 = codes_ref[t, 1:2, :]
    for back, slot_ref in zip(backs, slots, strict=True):
        first, second = slot_pick(c0, c1, slot_ref[...])
        pick = jnp.where(first | second, 1.0, 0.0).astype(BF16)
        db += tn(pick, back[...].reshape(pick.shape[0], db.shape[1]))
    hidden = hidden_ref[...]
    factor = rms(hidden)
    n = hidden * factor
    inner = db * gain_ref[...]
    dy = dy_ref[pl.ds(pl.multiple_of(t * tb, tb), tb), :].astype(F32)
    gh = dy + factor * (inner - n * jnp.mean(inner * n, axis=-1, keepdims=True))
    gh_ref[...] = gh
    dh_ref[...] = gh.astype(BF16)
    gg_ref[...] = jnp.sum(db * n, axis=0, keepdims=True)


def attend_back_body(
    tb,
    info_ref,
    h0,
    h1,
    h2,
    h3,
    gain_ref,
    wq_ref,
    wk_ref,
    wv_ref,
    wo_ref,
    act_ref,
    q_ref,
    k_ref,
    v_ref,
    att_ref,
    lse_ref,
    cos_coarse,
    sin_coarse,
    cos_fine,
    sin_fine,
    sign,
    o0,
    o1,
    o2,
    o3,
    gw_ref,
    gg_ref,
    cos_s,
    sin_s,
    dh_s,
    dat_s,
    qt_s,
    datt_s,
    dq_s,
    dkt_s,
    dvt_s,
    raw_s,
):
    t = info_ref[0]
    prefix = info_ref[1]
    seq_len, width = q_ref.shape
    blocks = seq_len // tb
    heads = width // HDIM
    scale = HDIM ** (-0.5)
    fill_rope(cos_coarse, sin_coarse, cos_fine, sin_fine, sign, cos_s, sin_s)
    for j, piece in enumerate((h0, h1, h2, h3)):
        at = pl.ds(pl.multiple_of((t ^ j) * tb, tb), tb)
        dh = piece[...]
        dh_s[at, :] = dh
        dat_s[at, :] = nt(dh, wo_ref[...]).astype(BF16)
    for b in range(blocks):
        rows = slice(b * tb, (b + 1) * tb)
        qt_s[:, rows] = q_ref[rows, :].T
        datt_s[:, rows] = dat_s[rows, :].T
    dkt_s[...] = jnp.zeros_like(dkt_s)
    dvt_s[...] = jnp.zeros_like(dvt_s)
    lane_head = lax.broadcasted_iota(jnp.int32, (tb, width), 1) // HDIM
    lane = lax.broadcasted_iota(jnp.int32, (tb, lse_ref.shape[1]), 1)
    for b in range(blocks):
        extent = max(seq_len // 2, (b + 1) * tb)
        rows = slice(b * tb, (b + 1) * tb)
        qb = q_ref[rows, :]
        datb = dat_s[rows, :]
        mix = datb.astype(F32) * att_ref[rows, :].astype(F32)
        lse_b = lse_ref[rows, :]
        limit = jnp.maximum(
            b * tb + lax.broadcasted_iota(jnp.int32, (tb, 1), 0), prefix - 1
        )
        allowed = lax.broadcasted_iota(jnp.int32, (tb, extent), 1) <= limit

        def one_head(h, dq, extent=extent, rows=rows, qb=qb, datb=datb, mix=mix, lse_b=lse_b, allowed=allowed):
            mine = lane_head == h
            lse = jnp.sum(jnp.where(lane == h, lse_b, 0.0), axis=-1, keepdims=True)
            delta = jnp.sum(jnp.where(mine, mix, 0.0), axis=-1, keepdims=True)
            scores = nt(jnp.where(mine, qb, jnp.zeros_like(qb)), k_ref[:extent, :])
            prob = jnp.exp(jnp.where(allowed, scores, -1e30) - lse)
            dp = nt(jnp.where(mine, datb, jnp.zeros_like(datb)), v_ref[:extent, :])
            ds = (prob * (dp - delta)).astype(BF16)
            at = pl.ds(pl.multiple_of(h * HDIM, HDIM), HDIM)
            dkt_s[at, :extent] += nn(qt_s[at, rows], ds)
            dvt_s[at, :extent] += nn(datt_s[at, rows], prob.astype(BF16))
            return jnp.where(mine, nn(ds, k_ref[:extent, :]), dq)

        dq_s[rows, :] = lax.fori_loop(0, heads, one_head, jnp.zeros((tb, width), F32))
    flip = half_swap_matrix(width)

    def unrotate(u, at):
        high = u.astype(BF16)
        low = (u - high.astype(F32)).astype(BF16)
        return (u * cos_s[at, :] - (nn(high, flip) + nn(low, flip)) * sin_s[at, :]).astype(BF16)

    gain_sum = jnp.zeros((1, act_ref.shape[1]), F32)
    for b in range(blocks):
        rows = slice(b * tb, (b + 1) * tb)
        dq = unrotate(dq_s[rows, :] * scale, rows)
        dk = unrotate(dkt_s[:, rows].T, rows)
        dv = dvt_s[:, rows].T.astype(BF16)
        raw_s[0, rows, :] = dq
        raw_s[1, rows, :] = dk
        raw_s[2, rows, :] = dv
        da = nn(dq, wq_ref[...]) + nn(dk, wk_ref[...]) + nn(dv, wv_ref[...])
        gain_sum += jnp.sum(da * act_ref[rows, :].astype(F32), axis=0, keepdims=True)
        part = da.astype(BF16)
        for j, out in enumerate((o0, o1, o2, o3)):

            @pl.when((t ^ b) == j)
            def _(out=out, part=part):
                out[...] = part

    gg_ref[...] = gain_sum / gain_ref[...]
    for i in range(4):
        if i < 3:
            g = tn(raw_s[i], act_ref[...]).T.astype(BF16)
        else:
            g = tn(att_ref[...], dh_s[...]).T.astype(BF16)
        if gw_ref.shape[0] == 4:
            gw_ref[i] = g
        else:
            gw_ref[:, i] = g.reshape(gw_ref.shape[0], gw_ref.shape[2], width)


def layer_out_body(n_le, where_ref, *rest):
    backs = rest[:n_le]
    slots = rest[n_le : 2 * n_le]
    hidden_ref, s0, s1, s2, codes_ref, gates_ref, out_ref = rest[2 * n_le :]
    t = where_ref[0]
    out = (
        hidden_ref[...] + s0[...].astype(F32) + s1[...].astype(F32) + s2[...].astype(F32)
    )
    c0 = codes_ref[t, 0:1, :]
    c1 = codes_ref[t, 1:2, :]
    g0 = gates_ref[t, 0:1, :]
    g1 = gates_ref[t, 1:2, :]
    for back, slot_ref in zip(backs, slots, strict=True):
        first, second = slot_pick(c0, c1, slot_ref[...])
        weight = jnp.where(first, g0, 0.0) + jnp.where(second, g1, 0.0)
        high = weight.astype(BF16)
        low = (weight - high.astype(F32)).astype(BF16)
        rows = back[...].reshape(high.shape[0], out.shape[1])
        out += tn(high, rows) + tn(low, rows)
    out_ref[...] = out


def grad_in_body(x_ref, p0, p1, p2, gh_ref, gain_ref, out_ref):
    x = x_ref[...].astype(F32)
    da = p0[...].astype(F32) + p1[...].astype(F32) + p2[...].astype(F32)
    factor = rms(x)
    n = x * factor
    inner = da * gain_ref[...]
    out_ref[...] = gh_ref[...] + factor * (
        inner - n * jnp.mean(inner * n, axis=-1, keepdims=True)
    )


def tie(x, *deps):
    return lax.optimization_barrier((x, deps))[0]


def cost(flops, read, transcendentals=0):
    return pl.CostEstimate(
        flops=int(flops), bytes_accessed=int(read), transcendentals=int(transcendentals)
    )


def add2(a, b):
    return (a.astype(F32) + b.astype(F32)).astype(BF16)


def add3(a, b, c):
    return (a.astype(F32) + b.astype(F32) + c.astype(F32)).astype(BF16)


def to_owner(pieces, after=()):
    r3 = swap(pieces[3], 1)
    r1 = swap(pieces[1], 1)
    rx = swap(tie(add2(pieces[2], r3), *after), 2)
    return pieces[0], r1, rx


def to_all(own, after=()):
    own = tie(own, *after)
    across = swap(own, 2)
    beside = swap(own, 1)
    both = swap(across, 1)
    return own, beside, across, both


def exchange(x):
    return lax.all_to_all(x, "expert", split_axis=0, concat_axis=0, tiled=True)


def halving(x, expert_count):
    e = lax.axis_index("expert")
    x = x.reshape(expert_count, -1, x.shape[-1])
    bit = 1
    while bit < expert_count:
        x = x.reshape(-1, 2, *x.shape[1:])
        mine = (e // bit) % 2
        keep = lax.dynamic_index_in_dim(x, mine, 1, keepdims=False)
        send = lax.dynamic_index_in_dim(x, 1 - mine, 1, keepdims=False)
        got = lax.ppermute(send, "expert", [(i, i ^ bit) for i in range(expert_count)])
        bit *= 2
        x = keep.astype(F32) + got.astype(F32)
        if bit < expert_count:
            x = x.astype(BF16)
    return x[0]


def everywhere(x):
    for axis in ("tensor", "expert"):
        count = lax.axis_size(axis)
        bit = 1
        while bit < count:
            x = x + lax.ppermute(x, axis, [(i, i ^ bit) for i in range(count)])
            bit *= 2
    return x


def per_device(
    inputs,
    attn_gain,
    w_query,
    w_key,
    w_value,
    w_output,
    ffn_gain,
    shared_gate,
    shared_up,
    shared_down,
    expert_gate,
    expert_up,
    expert_down,
    routes,
    gate_values,
    prefix,
    cotangent,
):
    tensor_count = lax.axis_size("tensor")
    expert_count = lax.axis_size("expert")
    assert tensor_count == 4
    t = lax.axis_index("tensor")
    tb, dim = inputs.shape
    seq_len, choices = routes.shape
    width = w_query.shape[1]
    hidden_units = shared_gate.shape[1]
    exp_hidden = expert_gate.shape[2]
    exp_dev = expert_gate.shape[0]
    slabs = max(1, expert_count // ROUTED_EXPERTS)
    cap = max(2, 3 * tb * choices // (2 * ROUTED_EXPERTS))
    where = jnp.reshape(t, (1,)).astype(jnp.int32)
    info = jnp.stack([t.astype(jnp.int32), prefix[0]])
    gain_a = attn_gain.reshape(1, dim)
    gain_b = ffn_gain.reshape(1, dim)
    wq_t, wk_t, wv_t = w_query.T, w_key.T, w_value.T

    entries = np.arange(expert_count * exp_dev)
    slot_np = (entries // slabs)[:, None] * cap + np.arange(cap)[None, :]
    slot_np = slot_np.reshape(expert_count, exp_dev, cap).astype(np.int32)
    slot_le = [jnp.asarray(slot_np[:, le].reshape(-1, 1)) for le in range(exp_dev)]
    last = exp_dev - 1

    x0, x1, x2, x3 = to_all(inputs)

    routes_b = routes.reshape(tensor_count, tb, choices).transpose(0, 2, 1)
    gates_b = gate_values.reshape(tensor_count, tb, choices).transpose(0, 2, 1)
    prepared = pl.pallas_call(
        functools.partial(prep_body, cap, tb),
        out_shape=(sds((tensor_count, choices, tb), jnp.int32),)
        + tuple(
            sds((expert_count, 2 if le == 0 else 1, cap, dim), BF16) for le in range(exp_dev)
        ),
        in_specs=[SMEM] + [VMEM] * (3 + exp_dev),
        out_specs=(VMEM,) * (1 + exp_dev),
        compiler_params=params(),
        cost_estimate=cost(2e9, 6e6),
        name="prep",
    )(where, routes_b, gates_b, cotangent, *slot_le)
    codes = prepared[0]
    cots = []
    for le in range(exp_dev):
        cots.append(exchange(tie(prepared[1 + le], *cots)))
    x1 = tie(x1, codes)

    rope = rope_parts(seq_len, width)
    block = sds((tb, dim), BF16)
    att_out = pl.pallas_call(
        functools.partial(attend_body, tb),
        out_shape=(
            sds((seq_len, dim), BF16),
            sds((seq_len, width), BF16),
            sds((seq_len, width), BF16),
            sds((seq_len, width), BF16),
            sds((seq_len, width), BF16),
            sds((seq_len, 128), F32),
            block,
            block,
            block,
            block,
        ),
        in_specs=[SMEM] + [VMEM] * 14,
        out_specs=(VMEM,) * 10,
        scratch_shapes=[pltpu.VMEM((seq_len, width), F32)] * 2,
        compiler_params=params(),
        cost_estimate=cost(12e9, 10e6, 3e6),
        name="attend",
    )(info, x0, x1, x2, x3, gain_a, wq_t, wk_t, wv_t, w_output, *rope)
    act_a, q, k, v, att, lse = att_out[:6]
    parts = to_owner(att_out[6:])

    got = pl.pallas_call(
        functools.partial(dispatch_body, exp_dev, cap),
        out_shape=(sds((tb, dim), F32), block)
        + (sds((expert_count, cap, dim), BF16),) * exp_dev,
        in_specs=[SMEM] + [VMEM] * (6 + exp_dev),
        out_specs=(VMEM,) * (2 + exp_dev),
        compiler_params=params(),
        cost_estimate=cost(1e9, 4e6),
        name="dispatch",
    )(where, inputs, *parts, gain_b, codes, *slot_le)
    hidden, act_b = got[:2]
    a_all = to_all(act_b)
    a_across = a_all[2]
    cot_pieces = [(cots[0], swap(cots[0], 1))]
    crossed = a_across
    for le in range(1, exp_dev):
        c0, c1, c2, c3 = to_all(cots[le], after=(crossed,))
        crossed = c2
        cot_pieces.append((c0, c1, c2, c3))

    sh = pl.pallas_call(
        functools.partial(shared_body, tb),
        out_shape=(block,) * 8 + (sds((dim, 3 * hidden_units), BF16),),
        in_specs=[SMEM] + [VMEM] * 8,
        out_specs=(VMEM,) * 9,
        scratch_shapes=[
            pltpu.VMEM((seq_len, dim), BF16),
            pltpu.VMEM((seq_len, dim), BF16),
            pltpu.VMEM((seq_len, hidden_units), BF16),
            pltpu.VMEM((seq_len, hidden_units), BF16),
            pltpu.VMEM((seq_len, hidden_units), BF16),
            pltpu.VMEM((seq_len, dim), BF16),
            pltpu.VMEM((seq_len, dim), BF16),
        ],
        compiler_params=params(),
        cost_estimate=cost(8e9, 12e6),
        name="shared",
    )(where, *a_all, cotangent, shared_gate, shared_up, shared_down)

    rows_x = []
    sent = cots[last]
    for le in range(exp_dev):
        after = (sent,) if le == 0 else (sent, sh[8])
        p0 = exchange(tie(got[2 + le], *after))
        sent = p0
        pieces = to_all(p0, after=(crossed,))
        crossed = pieces[2]
        rows_x.append(pieces)
    shared_grads = halving(sh[8], expert_count)

    src = min(8, expert_count)
    steps = expert_count // src
    rows_blk = pl.BlockSpec((src, cap, dim), lambda i: (i, 0, 0))
    saved_blk = pl.BlockSpec((4, src * cap, exp_hidden), lambda i: (0, i, 0))

    def weight_blk(le, a, b):
        return pl.BlockSpec((1, a, b), lambda i: (le, 0, 0))

    def cot_blk(j):
        return pl.BlockSpec((src, pl.Squeezed(), cap, dim), lambda i: (i, j, 0, 0))

    cot_args, cot_specs = [], []
    for le in range(exp_dev):
        if le == 0:
            own, beside = cot_pieces[0]
            cot_args.append((own, beside, own, beside))
            cot_specs.append([cot_blk(0), cot_blk(0), cot_blk(1), cot_blk(1)])
        else:
            cot_args.append(cot_pieces[le])
            cot_specs.append([cot_blk(0)] * 4)

    all_rows = expert_count * cap
    row_out = sds((expert_count, cap, dim), BF16)
    saved_out = sds((4, all_rows, exp_hidden), BF16)
    expert_flops = 2 * 4 * all_rows * dim * exp_hidden
    saved = []
    home_rows = []
    for le in range(exp_dev):
        res = pl.pallas_call(
            expert_body,
            grid=(steps,),
            out_shape=(row_out,) * 4 + (saved_out,) * 3,
            in_specs=[rows_blk] * 4
            + cot_specs[le]
            + [
                weight_blk(le, dim, exp_hidden),
                weight_blk(le, dim, exp_hidden),
                weight_blk(le, exp_hidden, dim),
            ],
            out_specs=(rows_blk,) * 4 + (saved_blk,) * 3,
            compiler_params=params(1),
            cost_estimate=cost(5 * expert_flops, 14e6),
            name="expert",
        )(*rows_x[le], *cot_args[le], expert_gate, expert_up, expert_down)
        saved.append(res[4:])
        p0, r1, rx = to_owner(res[:4], after=(crossed,))
        crossed = rx
        home_rows.append(exchange(tie(add3(p0, r1, rx), *home_rows)))
    shared_back = to_owner(sh[4:8], after=(crossed,))
    crossed = shared_back[2]

    grads = None
    home_res = []
    for le in range(exp_dev):
        args = (*tie(rows_x[le], saved[last]), *cot_args[le], *saved[le], expert_down)
        in_specs = (
            [rows_blk] * 4
            + cot_specs[le]
            + [saved_blk] * 3
            + [weight_blk(le, exp_hidden, dim)]
        )
        aliases = {}
        if grads is not None:
            aliases = {len(args) + i: 4 + i for i in range(3)}
            args = args + tuple(grads)
            in_specs = in_specs + [ANY] * 3
        res = pl.pallas_call(
            functools.partial(weights_body, grads is not None),
            grid=(steps,),
            out_shape=(row_out,) * 4
            + (
                sds((exp_dev, dim, exp_hidden), F32),
                sds((exp_dev, dim, exp_hidden), F32),
                sds((exp_dev, exp_hidden, dim), F32),
            ),
            in_specs=in_specs,
            out_specs=(rows_blk,) * 4
            + (
                weight_blk(le, dim, exp_hidden),
                weight_blk(le, dim, exp_hidden),
                weight_blk(le, exp_hidden, dim),
            ),
            scratch_shapes=[
                pltpu.VMEM((4 * src * cap, dim), BF16),
                pltpu.VMEM((4 * src * cap, dim), BF16),
            ],
            input_output_aliases=aliases,
            compiler_params=params(1),
            cost_estimate=cost(4 * expert_flops, 16e6),
            name="weights",
        )(*args)
        grads = res[4:]
        p0, r1, rx = to_owner(res[:4], after=(crossed,))
        crossed = rx
        home_res.append(exchange(tie(add3(p0, r1, rx), home_rows[last], *home_res)))
    shared_fwd = to_owner(sh[0:4], after=(crossed,))

    grad_hidden, dh, gain_ffn = pl.pallas_call(
        functools.partial(home_body, exp_dev, tb),
        out_shape=(sds((tb, dim), F32), block, sds((1, dim), F32)),
        in_specs=[SMEM] + [VMEM] * (2 * exp_dev + 7),
        out_specs=(VMEM,) * 3,
        compiler_params=params(),
        cost_estimate=cost(1e9, 5e6),
        name="home",
    )(
        where,
        *home_rows,
        *slot_le,
        *shared_back,
        tie(hidden, shared_grads),
        gain_b,
        cotangent,
        codes,
    )

    h_all = to_all(dh)
    rows_each = dim // expert_count
    direct = rows_each % 16 == 0
    gw_shape = (expert_count, 4, rows_each, width) if direct else (4, dim, width)
    back = pl.pallas_call(
        functools.partial(attend_back_body, tb),
        out_shape=(block,) * 4 + (sds(gw_shape, BF16), sds((1, dim), F32)),
        in_specs=[SMEM] + [VMEM] * 20,
        out_specs=(VMEM,) * 6,
        scratch_shapes=[
            pltpu.VMEM((seq_len, width), F32),
            pltpu.VMEM((seq_len, width), F32),
            pltpu.VMEM((seq_len, dim), BF16),
            pltpu.VMEM((seq_len, width), BF16),
            pltpu.VMEM((width, seq_len), BF16),
            pltpu.VMEM((width, seq_len), BF16),
            pltpu.VMEM((seq_len, width), F32),
            pltpu.VMEM((width, seq_len), F32),
            pltpu.VMEM((width, seq_len), F32),
            pltpu.VMEM((3, seq_len, width), BF16),
        ],
        compiler_params=params(),
        cost_estimate=cost(20e9, 10e6, 3e6),
        name="attend_back",
    )(
        info,
        *h_all,
        gain_a,
        wq_t,
        wk_t,
        wv_t,
        w_output,
        act_a,
        q,
        k,
        v,
        att,
        lse,
        *rope,
    )
    gw = back[4]
    if not direct:
        gw = gw.reshape(4, expert_count, rows_each, width).transpose(1, 0, 2, 3)
    gw = jnp.sum(exchange(gw).astype(F32), axis=0)
    da_parts = to_owner(back[:4])
    gains = everywhere(jnp.concatenate([back[5], gain_ffn], axis=0))

    grad_inputs = pl.pallas_call(
        grad_in_body,
        out_shape=sds((tb, dim), F32),
        in_specs=[VMEM] * 6,
        out_specs=VMEM,
        compiler_params=params(),
        cost_estimate=cost(1e7, 4e6),
        name="grad_in",
    )(inputs, *da_parts, grad_hidden, gain_a)
    layer_out = pl.pallas_call(
        functools.partial(layer_out_body, exp_dev),
        out_shape=sds((tb, dim), F32),
        in_specs=[SMEM] + [VMEM] * (2 * exp_dev + 6),
        out_specs=VMEM,
        compiler_params=params(),
        cost_estimate=cost(1e9, 4e6),
        name="layer_out",
    )(where, *home_res, *slot_le, hidden, *shared_fwd, codes, gates_b)
    return (
        layer_out,
        grad_inputs,
        gains[0],
        gw[0],
        gw[1],
        gw[2],
        gw[3].T,
        gains[1],
        shared_grads[:, :hidden_units],
        shared_grads[:, hidden_units : 2 * hidden_units],
        shared_grads[:, 2 * hidden_units :].T,
        grads[0],
        grads[1],
        grads[2],
    )


def solution(mesh):
    return jax.shard_map(
        per_device,
        mesh=mesh,
        in_specs=(
            P(("expert", "tensor"), None),
            P(),
            P(None, "tensor"),
            P(None, "tensor"),
            P(None, "tensor"),
            P("tensor", None),
            P(),
            P(None, "tensor"),
            P(None, "tensor"),
            P("tensor", None),
            P("expert", None, "tensor"),
            P("expert", None, "tensor"),
            P("expert", "tensor", None),
            P("expert", None),
            P("expert", None),
            P("expert"),
            P("expert", None),
        ),
        out_specs=(
            P(("expert", "tensor"), None),
            P(("expert", "tensor"), None),
            P(),
            P("expert", "tensor"),
            P("expert", "tensor"),
            P("expert", "tensor"),
            P("tensor", "expert"),
            P(),
            P("expert", "tensor"),
            P("expert", "tensor"),
            P("tensor", "expert"),
            P("expert", None, "tensor"),
            P("expert", None, "tensor"),
            P("expert", "tensor", None),
        ),
        check_vma=False,
    )
```

```python
import functools

import jax
import jax.numpy as jnp
import numpy as np
from jax import lax
from jax.experimental import pallas as pl
from jax.experimental.pallas import tpu as pltpu
from jax.sharding import PartitionSpec as P

HDIM = 64
ROUTED_EXPERTS = 16
EPS = 1e-05
F32 = jnp.float32
BF16 = jnp.bfloat16
ROPE_STEP = 32

VMEM = pl.BlockSpec(memory_space=pltpu.VMEM)
SMEM = pl.BlockSpec(memory_space=pltpu.SMEM)
ANY = pl.BlockSpec(memory_space=pl.ANY)


def sds(shape, dtype):
    return jax.ShapeDtypeStruct(tuple(shape), dtype)


def params(n_grid=0):
    if n_grid:
        return pltpu.CompilerParams(
            vmem_limit_bytes=60 * 1024 * 1024, dimension_semantics=("arbitrary",) * n_grid
        )
    return pltpu.CompilerParams(vmem_limit_bytes=60 * 1024 * 1024)


def nn(a, b):
    return jnp.dot(a, b, preferred_element_type=F32)


def nt(a, b):
    return lax.dot_general(a, b, (((1,), (1,)), ((), ())), preferred_element_type=F32)


def tn(a, b):
    return lax.dot_general(a, b, (((0,), (0,)), ((), ())), preferred_element_type=F32)


def swap(x, bit):
    count = lax.axis_size("tensor")
    return lax.ppermute(x, "tensor", [(i, i ^ bit) for i in range(count)])


def rope_parts(seq_len, width):
    half = HDIM // 2
    frequency = 10000.0 ** (-np.arange(half, dtype=np.float64) * 2.0 / HDIM)
    lanes = np.tile(np.concatenate([frequency, frequency]), width // HDIM)
    sign = np.tile(np.concatenate([-np.ones(half), np.ones(half)]), width // HDIM)
    coarse = np.arange(0, seq_len, ROPE_STEP)[:, None] * lanes[None, :]
    fine = np.arange(ROPE_STEP)[:, None] * lanes[None, :]
    return tuple(
        jnp.asarray(a, dtype=F32)
        for a in (np.cos(coarse), np.sin(coarse), np.cos(fine), np.sin(fine), sign[None, :])
    )


def fill_rope(cos_coarse, sin_coarse, cos_fine, sin_fine, sign, cos_out, sin_out):
    cf, sf, sg = cos_fine[...], sin_fine[...], sign[...]

    def step(a, _):
        cc = cos_coarse[pl.ds(a, 1), :]
        sc = sin_coarse[pl.ds(a, 1), :]
        at = pl.ds(pl.multiple_of(a * ROPE_STEP, ROPE_STEP), ROPE_STEP)
        cos_out[at, :] = cc * cf - sc * sf
        sin_out[at, :] = (sc * cf + cc * sf) * sg
        return 0

    lax.fori_loop(0, cos_coarse.shape[0], step, 0)


def half_swap_matrix(width):
    row = lax.broadcasted_iota(jnp.int32, (width, width), 0)
    col = lax.broadcasted_iota(jnp.int32, (width, width), 1)
    half = HDIM // 2
    partner = jnp.where((col & half) == 0, col + half, col - half)
    return jnp.where(row == partner, 1.0, 0.0).astype(BF16)


def rms(values):
    return lax.rsqrt(jnp.mean(values * values, axis=-1, keepdims=True) + EPS)


def slot_pick(codes_k0, codes_k1, slot_code):
    first = codes_k0 == slot_code
    second = codes_k1 == slot_code
    return first, second


def prep_body(cap, tb, where_ref, routes_ref, gates_ref, dy_ref, *rest):
    t = where_ref[0]
    blocks = routes_ref.shape[0]
    slots = rest[:-2]
    codes_ref, rows_ref = rest[-2:]
    upper = jnp.where(
        lax.broadcasted_iota(jnp.int32, (tb, tb), 0) < lax.broadcasted_iota(jnp.int32, (tb, tb), 1),
        1.0,
        0.0,
    ).astype(BF16)
    ids = lax.broadcasted_iota(jnp.int32, (ROUTED_EXPERTS, tb), 0)
    for b in range(blocks):
        r0 = routes_ref[b, 0:1, :]
        r1 = routes_ref[b, 1:2, :]
        e0 = ids == r0
        e1 = ids == r1
        named = jnp.where(e0, 1.0, 0.0) + jnp.where(e1, 1.0, 0.0)
        before = nn(named.astype(BF16), upper)
        k0 = jnp.sum(jnp.where(e0, before, 0.0), axis=0, keepdims=True)
        k1 = jnp.sum(jnp.where(e1, before, 0.0), axis=0, keepdims=True)
        codes_ref[b, 0:1, :] = r0 * cap + k0.astype(jnp.int32)
        codes_ref[b, 1:2, :] = r1 * cap + k1.astype(jnp.int32)
    c0 = codes_ref[t, 0:1, :]
    c1 = codes_ref[t, 1:2, :]
    g0 = gates_ref[t, 0:1, :]
    g1 = gates_ref[t, 1:2, :]
    dy = dy_ref[pl.ds(pl.multiple_of(t * tb, tb), tb), :]
    for le, slot_ref in enumerate(slots):
        first, second = slot_pick(c0, c1, slot_ref[...])
        gate = jnp.sum(
            jnp.where(first, g0, 0.0) + jnp.where(second, g1, 0.0), axis=1, keepdims=True
        )
        pick = jnp.where(first | second, 1.0, 0.0).astype(BF16)
        got = nn(pick, dy) * gate
        rows_ref[:, le] = got.astype(BF16).reshape(rows_ref.shape[0], cap, got.shape[1])


def attend_body(
    tb,
    info_ref,
    x0,
    x1,
    x2,
    x3,
    gain_ref,
    wq_ref,
    wk_ref,
    wv_ref,
    wo_ref,
    cos_coarse,
    sin_coarse,
    cos_fine,
    sin_fine,
    sign,
    act_ref,
    q_ref,
    k_ref,
    v_ref,
    att_ref,
    lse_ref,
    out0,
    out1,
    out2,
    out3,
    cos_s,
    sin_s,
):
    t = info_ref[0]
    prefix = info_ref[1]
    seq_len, width = q_ref.shape
    blocks = seq_len // tb
    heads = width // HDIM
    fill_rope(cos_coarse, sin_coarse, cos_fine, sin_fine, sign, cos_s, sin_s)
    gain = gain_ref[...]
    for j, piece in enumerate((x0, x1, x2, x3)):
        x = piece[...].astype(F32)
        at = pl.ds(pl.multiple_of((t ^ j) * tb, tb), tb)
        act_ref[at, :] = (x * rms(x) * gain).astype(BF16)
    flip = half_swap_matrix(width)
    wq = wq_ref[...]
    wk = wk_ref[...]
    wq_flip = nn(flip, wq).astype(BF16)
    wk_flip = nn(flip, wk).astype(BF16)
    scale = HDIM ** (-0.5)

    def project(b, _):
        at = pl.ds(pl.multiple_of(b * tb, tb), tb)
        a = act_ref[at, :]
        cos, sin = cos_s[at, :], sin_s[at, :]
        q_ref[at, :] = (scale * (nt(a, wq) * cos + nt(a, wq_flip) * sin)).astype(BF16)
        k_ref[at, :] = (nt(a, wk) * cos + nt(a, wk_flip) * sin).astype(BF16)
        v_ref[at, :] = nt(a, wv_ref[...]).astype(BF16)
        return 0

    lax.fori_loop(0, blocks, project, 0)
    lane_head = lax.broadcasted_iota(jnp.int32, (tb, width), 1) // HDIM
    lane = lax.broadcasted_iota(jnp.int32, (tb, lse_ref.shape[1]), 1)
    for b in range(blocks):
        extent = max(seq_len // 2, (b + 1) * tb)
        rows = slice(b * tb, (b + 1) * tb)
        qb = q_ref[rows, :]
        limit = jnp.maximum(
            b * tb + lax.broadcasted_iota(jnp.int32, (tb, 1), 0), prefix - 1
        )
        allowed = lax.broadcasted_iota(jnp.int32, (tb, extent), 1) <= limit

        def one_head(h, carried, extent=extent, qb=qb, allowed=allowed):
            att, lse = carried
            mine = lane_head == h
            scores = nt(jnp.where(mine, qb, jnp.zeros_like(qb)), k_ref[:extent, :])
            scores = jnp.where(allowed, scores, -1e30)
            top = jnp.max(scores, axis=-1, keepdims=True)
            weight = jnp.exp(scores - top)
            total = jnp.sum(weight, axis=-1, keepdims=True)
            got = nn(weight.astype(BF16), v_ref[:extent, :]) / total
            att = jnp.where(mine, got, att)
            lse = jnp.where(lane == h, top + jnp.log(total), lse)
            return att, lse

        att, lse = lax.fori_loop(
            0,
            heads,
            one_head,
            (jnp.zeros((tb, width), F32), jnp.zeros((tb, lse_ref.shape[1]), F32)),
        )
        att = att.astype(BF16)
        att_ref[rows, :] = att
        lse_ref[rows, :] = lse
        part = nn(att, wo_ref[...]).astype(BF16)
        for j, out in enumerate((out0, out1, out2, out3)):

            @pl.when((t ^ b) == j)
            def _(out=out, part=part):
                out[...] = part


def dispatch_body(t_blocks, cap, where_ref, x_ref, p0, p1, p2, gain_ref, codes_ref, *rest):
    slots = rest[: t_blocks]
    hidden_ref, act_ref = rest[t_blocks : t_blocks + 2]
    bufs = rest[t_blocks + 2 :]
    t = where_ref[0]
    hidden = (
        x_ref[...].astype(F32)
        + p0[...].astype(F32)
        + p1[...].astype(F32)
        + p2[...].astype(F32)
    )
    hidden_ref[...] = hidden
    act = (hidden * rms(hidden) * gain_ref[...]).astype(BF16)
    act_ref[...] = act
    c0 = codes_ref[t, 0:1, :]
    c1 = codes_ref[t, 1:2, :]
    for slot_ref, buf in zip(slots, bufs, strict=True):
        first, second = slot_pick(c0, c1, slot_ref[...])
        pick = jnp.where(first | second, 1.0, 0.0).astype(BF16)
        got = nn(pick, act).astype(BF16)
        buf[...] = got.reshape(buf.shape)


def shared_body(
    tb,
    where_ref,
    a0,
    a1,
    a2,
    a3,
    dy_ref,
    gate_ref,
    up_ref,
    down_ref,
    f0,
    f1,
    f2,
    f3,
    b0,
    b1,
    b2,
    b3,
    grads_ref,
    act_s,
    dy_s,
    hs_s,
    dg_s,
    du_s,
    f_s,
    b_s,
):
    t = where_ref[0]
    blocks = 4
    for j, piece in enumerate((a0, a1, a2, a3)):
        act_s[j * tb : (j + 1) * tb, :] = piece[...]
        dy_s[j * tb : (j + 1) * tb, :] = dy_ref[pl.ds(pl.multiple_of((t ^ j) * tb, tb), tb), :]

    def block(j, _):
        at = pl.ds(pl.multiple_of(j * tb, tb), tb)
        a = act_s[at, :]
        dy = dy_s[at, :]
        g = nn(a, gate_ref[...])
        u = nn(a, up_ref[...])
        sig = jax.nn.sigmoid(g)
        silu = g * sig
        hs = (silu * u).astype(BF16)
        dhs = nt(dy, down_ref[...])
        dg = (dhs * u * sig * (1.0 + g * (1.0 - sig))).astype(BF16)
        du = (dhs * silu).astype(BF16)
        hs_s[at, :] = hs
        dg_s[at, :] = dg
        du_s[at, :] = du
        f_s[at, :] = nn(hs, down_ref[...]).astype(BF16)
        b_s[at, :] = (nt(dg, gate_ref[...]) + nt(du, up_ref[...])).astype(BF16)
        return 0

    lax.fori_loop(0, blocks, block, 0)
    for j, (f, b) in enumerate(((f0, b0), (f1, b1), (f2, b2), (f3, b3))):
        f[...] = f_s[j * tb : (j + 1) * tb, :]
        b[...] = b_s[j * tb : (j + 1) * tb, :]
    hidden = hs_s.shape[1]

    def columns(c, _):
        at = pl.ds(pl.multiple_of(c * tb, tb), tb)
        a = act_s[:, at]
        dy = dy_s[:, at]
        grads_ref[at, 0:hidden] = tn(a, dg_s[...]).astype(BF16)
        grads_ref[at, hidden : 2 * hidden] = tn(a, du_s[...]).astype(BF16)
        grads_ref[at, 2 * hidden : 3 * hidden] = tn(dy, hs_s[...]).astype(BF16)
        return 0

    lax.fori_loop(0, act_s.shape[1] // tb, columns, 0)


def expert_body(x0, x1, x2, x3, c0, c1, c2, c3, gate_ref, up_ref, down_ref, *outs):
    o = outs[:4]
    he_ref, dg_ref, du_ref = outs[4:7]
    n_src, cap, dim = x0.shape
    rows = n_src * cap
    gate = gate_ref[0]
    up = up_ref[0]
    down = down_ref[0]
    xs = (x0, x1, x2, x3)
    cs = (c0, c1, c2, c3)
    for j in (3, 1, 2, 0):
        x = xs[j][...].reshape(rows, dim)
        c = cs[j][...].reshape(rows, dim)
        g = nn(x, gate)
        u = nn(x, up)
        sig = jax.nn.sigmoid(g)
        silu = g * sig
        dhe = nt(c, down)
        dg = (dhe * u * sig * (1.0 + g * (1.0 - sig))).astype(BF16)
        du = (dhe * silu).astype(BF16)
        he_ref[j] = (silu * u).astype(BF16)
        dg_ref[j] = dg
        du_ref[j] = du
        o[j][...] = (nt(dg, gate) + nt(du, up)).astype(BF16).reshape(n_src, cap, dim)


def weights_body(aliased, x0, x1, x2, x3, c0, c1, c2, c3, he_ref, dg_ref, du_ref, down_ref, *rest):
    if aliased:
        rest = rest[3:]
    o = rest[:4]
    gg_ref, gu_ref, gd_ref, x_s, c_s = rest[4:]
    n_src, cap, dim = x0.shape
    rows = n_src * cap
    step = pl.program_id(0)
    down = down_ref[0]
    cs = (c0, c1, c2, c3)
    for j, x in enumerate((x0, x1, x2, x3)):
        x_s[j * rows : (j + 1) * rows, :] = x[...].reshape(rows, dim)
        c_s[j * rows : (j + 1) * rows, :] = cs[j][...].reshape(rows, dim)
        o[j][...] = nn(he_ref[j], down).astype(BF16).reshape(n_src, cap, dim)
    hidden = he_ref.shape[2]
    he = he_ref[...].reshape(4 * rows, hidden)
    dg = dg_ref[...].reshape(4 * rows, hidden)
    du = du_ref[...].reshape(4 * rows, hidden)
    gg = tn(x_s[...], dg)
    gu = tn(x_s[...], du)
    gd = tn(he, c_s[...])

    @pl.when(step == 0)
    def _():
        gg_ref[0] = gg
        gu_ref[0] = gu
        gd_ref[0] = gd

    @pl.when(step > 0)
    def _():
        gg_ref[0] += gg
        gu_ref[0] += gu
        gd_ref[0] += gd


def home_body(n_le, tb, where_ref, *rest):
    backs = rest[:n_le]
    slots = rest[n_le : 2 * n_le]
    s0, s1, s2, hidden_ref, gain_ref, dy_ref, codes_ref = rest[2 * n_le : 2 * n_le + 7]
    gh_ref, dh_ref, gg_ref = rest[2 * n_le + 7 :]
    t = where_ref[0]
    db = s0[...].astype(F32) + s1[...].astype(F32) + s2[...].astype(F32)
    c0 = codes_ref[t, 0:1, :]
    c1 = codes_ref[t, 1:2, :]
    for back, slot_ref in zip(backs, slots, strict=True):
        first, second = slot_pick(c0, c1, slot_ref[...])
        pick = jnp.where(first | second, 1.0, 0.0).astype(BF16)
        db += tn(pick, back[...].reshape(pick.shape[0], db.shape[1]))
    hidden = hidden_ref[...]
    factor = rms(hidden)
    n = hidden * factor
    inner = db * gain_ref[...]
    dy = dy_ref[pl.ds(pl.multiple_of(t * tb, tb), tb), :].astype(F32)
    gh = dy + factor * (inner - n * jnp.mean(inner * n, axis=-1, keepdims=True))
    gh_ref[...] = gh
    dh_ref[...] = gh.astype(BF16)
    gg_ref[...] = jnp.sum(db * n, axis=0, keepdims=True)


def attend_back_body(
    tb,
    info_ref,
    h0,
    h1,
    h2,
    h3,
    gain_ref,
    gb_ref,
    wq_ref,
    wk_ref,
    wv_ref,
    wo_ref,
    act_ref,
    q_ref,
    k_ref,
    v_ref,
    att_ref,
    lse_ref,
    cos_coarse,
    sin_coarse,
    cos_fine,
    sin_fine,
    sign,
    o0,
    o1,
    o2,
    o3,
    gw_ref,
    gg_ref,
    cos_s,
    sin_s,
    dh_s,
    dat_s,
    qt_s,
    datt_s,
    dq_s,
    dkt_s,
    dvt_s,
    raw_s,
):
    t = info_ref[0]
    prefix = info_ref[1]
    seq_len, width = q_ref.shape
    blocks = seq_len // tb
    heads = width // HDIM
    scale = HDIM ** (-0.5)
    fill_rope(cos_coarse, sin_coarse, cos_fine, sin_fine, sign, cos_s, sin_s)
    for j, piece in enumerate((h0, h1, h2, h3)):
        at = pl.ds(pl.multiple_of((t ^ j) * tb, tb), tb)
        dh = piece[...]
        dh_s[at, :] = dh
        dat_s[at, :] = nt(dh, wo_ref[...]).astype(BF16)
    for b in range(blocks):
        rows = slice(b * tb, (b + 1) * tb)
        qt_s[:, rows] = q_ref[rows, :].T
        datt_s[:, rows] = dat_s[rows, :].T
    dkt_s[...] = jnp.zeros_like(dkt_s)
    dvt_s[...] = jnp.zeros_like(dvt_s)
    lane_head = lax.broadcasted_iota(jnp.int32, (tb, width), 1) // HDIM
    lane = lax.broadcasted_iota(jnp.int32, (tb, lse_ref.shape[1]), 1)
    for b in range(blocks):
        extent = max(seq_len // 2, (b + 1) * tb)
        rows = slice(b * tb, (b + 1) * tb)
        qb = q_ref[rows, :]
        datb = dat_s[rows, :]
        mix = datb.astype(F32) * att_ref[rows, :].astype(F32)
        lse_b = lse_ref[rows, :]
        limit = jnp.maximum(
            b * tb + lax.broadcasted_iota(jnp.int32, (tb, 1), 0), prefix - 1
        )
        allowed = lax.broadcasted_iota(jnp.int32, (tb, extent), 1) <= limit

        def one_head(h, dq, extent=extent, rows=rows, qb=qb, datb=datb, mix=mix, lse_b=lse_b, allowed=allowed):
            mine = lane_head == h
            lse = jnp.sum(jnp.where(lane == h, lse_b, 0.0), axis=-1, keepdims=True)
            delta = jnp.sum(jnp.where(mine, mix, 0.0), axis=-1, keepdims=True)
            scores = nt(jnp.where(mine, qb, jnp.zeros_like(qb)), k_ref[:extent, :])
            prob = jnp.exp(jnp.where(allowed, scores, -1e30) - lse)
            dp = nt(jnp.where(mine, datb, jnp.zeros_like(datb)), v_ref[:extent, :])
            ds = (prob * (dp - delta)).astype(BF16)
            at = pl.ds(pl.multiple_of(h * HDIM, HDIM), HDIM)
            dkt_s[at, :extent] += nn(qt_s[at, rows], ds)
            dvt_s[at, :extent] += nn(datt_s[at, rows], prob.astype(BF16))
            return jnp.where(mine, nn(ds, k_ref[:extent, :]), dq)

        dq_s[rows, :] = lax.fori_loop(0, heads, one_head, jnp.zeros((tb, width), F32))
    flip = half_swap_matrix(width)

    def unrotate(u, at):
        high = u.astype(BF16)
        low = (u - high.astype(F32)).astype(BF16)
        return (u * cos_s[at, :] - (nn(high, flip) + nn(low, flip)) * sin_s[at, :]).astype(BF16)

    gain_sum = jnp.zeros((1, act_ref.shape[1]), F32)
    for b in range(blocks):
        rows = slice(b * tb, (b + 1) * tb)
        dq = unrotate(dq_s[rows, :] * scale, rows)
        dk = unrotate(dkt_s[:, rows].T, rows)
        dv = dvt_s[:, rows].T.astype(BF16)
        raw_s[0, rows, :] = dq
        raw_s[1, rows, :] = dk
        raw_s[2, rows, :] = dv
        da = nn(dq, wq_ref[...]) + nn(dk, wk_ref[...]) + nn(dv, wv_ref[...])
        gain_sum += jnp.sum(da * act_ref[rows, :].astype(F32), axis=0, keepdims=True)
        part = da.astype(BF16)
        for j, out in enumerate((o0, o1, o2, o3)):

            @pl.when((t ^ b) == j)
            def _(out=out, part=part):
                out[...] = part

    gain_a = gain_sum / gain_ref[...]
    g = [tn(raw_s[i], act_ref[...]).T for i in range(3)] + [tn(att_ref[...], dh_s[...]).T]
    g = jnp.concatenate(g, axis=1).astype(BF16)
    flat = []
    for gain in (gain_a, gb_ref[...]):
        high = gain.astype(BF16).astype(F32)
        flat += [high, gain - high]
    if len(gw_ref.shape) == 2:
        gw_ref[...] = g
        gg_ref[...] = jnp.concatenate(flat, axis=0)
    else:
        gg_ref[...] = jnp.zeros_like(gg_ref)
        each = g.shape[0] // gw_ref.shape[0]
        gw_ref[:, :each] = g.reshape(gw_ref.shape[0], each, g.shape[1])
        rest = gw_ref.shape[1] - each
        lines = jnp.concatenate(flat + [jnp.zeros((rest - 4, g.shape[1]), F32)], axis=0)
        gw_ref[:, each:] = jnp.broadcast_to(
            lines.astype(BF16)[None], (gw_ref.shape[0], rest, g.shape[1])
        )


def layer_out_body(n_le, where_ref, back_ref, *rest):
    slots = rest[:n_le]
    hidden_ref, s0, s1, s2, codes_ref, gates_ref, out_ref = rest[n_le:]
    t = where_ref[0]
    out = (
        hidden_ref[...] + s0[...].astype(F32) + s1[...].astype(F32) + s2[...].astype(F32)
    )
    c0 = codes_ref[t, 0:1, :]
    c1 = codes_ref[t, 1:2, :]
    g0 = gates_ref[t, 0:1, :]
    g1 = gates_ref[t, 1:2, :]
    for le, slot_ref in enumerate(slots):
        first, second = slot_pick(c0, c1, slot_ref[...])
        weight = jnp.where(first, g0, 0.0) + jnp.where(second, g1, 0.0)
        high = weight.astype(BF16)
        low = (weight - high.astype(F32)).astype(BF16)
        rows = back_ref[:, le].reshape(high.shape[0], out.shape[1])
        out += tn(high, rows) + tn(low, rows)
    out_ref[...] = out


def grad_in_body(x_ref, p0, p1, p2, gh_ref, gain_ref, out_ref):
    x = x_ref[...].astype(F32)
    da = p0[...].astype(F32) + p1[...].astype(F32) + p2[...].astype(F32)
    factor = rms(x)
    n = x * factor
    inner = da * gain_ref[...]
    out_ref[...] = gh_ref[...] + factor * (
        inner - n * jnp.mean(inner * n, axis=-1, keepdims=True)
    )


def tie(x, *deps):
    return lax.optimization_barrier((x, deps))[0]


def cost(flops, read, transcendentals=0):
    return pl.CostEstimate(
        flops=int(flops * 0.3), bytes_accessed=int(read * 0.3), transcendentals=0
    )


def add2(a, b):
    return (a.astype(F32) + b.astype(F32)).astype(BF16)


def add3(a, b, c):
    return (a.astype(F32) + b.astype(F32) + c.astype(F32)).astype(BF16)


def beside_sums(pieces):
    r3 = swap(pieces[3], 1)
    r1 = swap(pieces[1], 1)
    return r1, add2(pieces[2], r3)


def to_owner(pieces, after=()):
    r1, inward = beside_sums(pieces)
    return pieces[0], r1, swap(tie(inward, *after), 2)


def to_all(own, after=(), across=None, during=()):
    if across is None:
        across = swap(tie(own, *after), 2)
    beside = swap(own, 1)
    both = swap(tie(across, *during), 1)
    return own, beside, across, both


def exchange(x):
    return lax.all_to_all(x, "expert", split_axis=0, concat_axis=0, tiled=True)


def halve(x, bit, axis):
    count = lax.axis_size("expert")
    x = x.reshape(*((-1, 2) if axis else (2, -1)), *x.shape[1:])
    mine = (lax.axis_index("expert") // bit) % 2
    keep = lax.dynamic_index_in_dim(x, mine, axis, keepdims=False)
    send = lax.dynamic_index_in_dim(x, 1 - mine, axis, keepdims=False)
    return keep, lax.ppermute(send, "expert", [(i, i ^ bit) for i in range(count)])


def per_device(
    inputs,
    attn_gain,
    w_query,
    w_key,
    w_value,
    w_output,
    ffn_gain,
    shared_gate,
    shared_up,
    shared_down,
    expert_gate,
    expert_up,
    expert_down,
    routes,
    gate_values,
    prefix,
    cotangent,
):
    tensor_count = lax.axis_size("tensor")
    expert_count = lax.axis_size("expert")
    assert tensor_count == 4
    t = lax.axis_index("tensor")
    tb, dim = inputs.shape
    seq_len, choices = routes.shape
    width = w_query.shape[1]
    hidden_units = shared_gate.shape[1]
    exp_hidden = expert_gate.shape[2]
    exp_dev = expert_gate.shape[0]
    slabs = max(1, expert_count // ROUTED_EXPERTS)
    cap = max(2, 3 * tb * choices // (2 * ROUTED_EXPERTS))
    where = jnp.reshape(t, (1,)).astype(jnp.int32)
    info = jnp.stack([t.astype(jnp.int32), prefix[0]])
    gain_a = attn_gain.reshape(1, dim)
    gain_b = ffn_gain.reshape(1, dim)
    wq_t, wk_t, wv_t = w_query.T, w_key.T, w_value.T

    entries = np.arange(expert_count * exp_dev)
    slot_np = (entries // slabs)[:, None] * cap + np.arange(cap)[None, :]
    slot_np = slot_np.reshape(expert_count, exp_dev, cap).astype(np.int32)
    slot_le = [jnp.asarray(slot_np[:, le].reshape(-1, 1)) for le in range(exp_dev)]
    last = exp_dev - 1

    x2 = swap(inputs, 2)

    routes_b = routes.reshape(tensor_count, tb, choices).transpose(0, 2, 1)
    gates_b = gate_values.reshape(tensor_count, tb, choices).transpose(0, 2, 1)
    codes, cot_rows = pl.pallas_call(
        functools.partial(prep_body, cap, tb),
        out_shape=(
            sds((tensor_count, choices, tb), jnp.int32),
            sds((expert_count, exp_dev, cap, dim), BF16),
        ),
        in_specs=[SMEM] + [VMEM] * (3 + exp_dev),
        out_specs=(VMEM, VMEM),
        compiler_params=params(),
        cost_estimate=cost(2e9, 6e6),
        name="prep",
    )(where, routes_b, gates_b, cotangent, *slot_le)
    cot = exchange(cot_rows)
    x1 = swap(inputs, 1)
    x3 = swap(tie(x2, codes), 1)

    rope = rope_parts(seq_len, width)
    block = sds((tb, dim), BF16)
    att_out = pl.pallas_call(
        functools.partial(attend_body, tb),
        out_shape=(
            sds((seq_len, dim), BF16),
            sds((seq_len, width), BF16),
            sds((seq_len, width), BF16),
            sds((seq_len, width), BF16),
            sds((seq_len, width), BF16),
            sds((seq_len, 128), F32),
            block,
            block,
            block,
            block,
        ),
        in_specs=[SMEM] + [VMEM] * 14,
        out_specs=(VMEM,) * 10,
        scratch_shapes=[pltpu.VMEM((seq_len, width), F32)] * 2,
        compiler_params=params(),
        cost_estimate=cost(12e9, 10e6, 3e6),
        name="attend",
    )(info, inputs, x1, x2, x3, gain_a, wq_t, wk_t, wv_t, w_output, *rope)
    act_a, q, k, v, att, lse = att_out[:6]
    r1, inward = beside_sums(att_out[6:])
    crossed = swap(inward, 2)
    parts = (att_out[6], r1, crossed)

    got = pl.pallas_call(
        functools.partial(dispatch_body, exp_dev, cap),
        out_shape=(sds((tb, dim), F32), block)
        + (sds((expert_count, cap, dim), BF16),) * exp_dev,
        in_specs=[SMEM] + [VMEM] * (6 + exp_dev),
        out_specs=(VMEM,) * (2 + exp_dev),
        compiler_params=params(),
        cost_estimate=cost(1e9, 4e6),
        name="dispatch",
    )(where, inputs, *parts, gain_b, codes, *slot_le)
    hidden, act_b = got[:2]
    a_all = to_all(act_b)

    sh = pl.pallas_call(
        functools.partial(shared_body, tb),
        out_shape=(block,) * 8 + (sds((dim, 3 * hidden_units), BF16),),
        in_specs=[SMEM] + [VMEM] * 8,
        out_specs=(VMEM,) * 9,
        scratch_shapes=[
            pltpu.VMEM((seq_len, dim), BF16),
            pltpu.VMEM((seq_len, dim), BF16),
            pltpu.VMEM((seq_len, hidden_units), BF16),
            pltpu.VMEM((seq_len, hidden_units), BF16),
            pltpu.VMEM((seq_len, hidden_units), BF16),
            pltpu.VMEM((seq_len, dim), BF16),
            pltpu.VMEM((seq_len, dim), BF16),
        ],
        compiler_params=params(),
        cost_estimate=cost(8e9, 12e6),
        name="shared",
    )(where, *a_all, cotangent, shared_gate, shared_up, shared_down)

    rows_x = []
    cot_across = swap(tie(cot, a_all[2]), 2)
    cots = to_all(cot, across=cot_across, during=(sh[8],))
    crossed = cot_across
    sent = cot
    for le in range(exp_dev):
        sent = exchange(tie(got[2 + le], sent))
        crossed = swap(tie(sent, crossed), 2)
        rows_x.append((sent, crossed))

    src = min(8, expert_count)
    steps = expert_count // src
    rows_blk = pl.BlockSpec((src, cap, dim), lambda i: (i, 0, 0))
    saved_blk = pl.BlockSpec((4, src * cap, exp_hidden), lambda i: (0, i, 0))

    def cot_blk(le):
        return pl.BlockSpec((src, pl.Squeezed(), cap, dim), lambda i: (i, le, 0, 0))

    def weight_blk(le, a, b):
        return pl.BlockSpec((1, a, b), lambda i: (le, 0, 0))

    all_rows = expert_count * cap
    row_out = sds((expert_count, cap, dim), BF16)
    saved_out = sds((4, all_rows, exp_hidden), BF16)
    expert_flops = 2 * 4 * all_rows * dim * exp_hidden
    bits = [1 << i for i in range(1, expert_count.bit_length() - 1)][::-1]
    halves = halve(tie(sh[8], sent).reshape(expert_count, -1, sh[8].shape[1]), 1, 1)
    saved = []
    home_in = []
    for le in range(exp_dev):
        rows_x[le] = to_all(
            rows_x[le][0], across=rows_x[le][1], during=saved[le - 1] if le else (sh[8],)
        )
        res = pl.pallas_call(
            expert_body,
            grid=(steps,),
            out_shape=(row_out,) * 4 + (saved_out,) * 3,
            in_specs=[rows_blk] * 4
            + [cot_blk(le)] * 4
            + [
                weight_blk(le, dim, exp_hidden),
                weight_blk(le, dim, exp_hidden),
                weight_blk(le, exp_hidden, dim),
            ],
            out_specs=(rows_blk,) * 4 + (saved_blk,) * 3,
            compiler_params=params(1),
            cost_estimate=cost(5 * expert_flops, 14e6),
            name="expert",
        )(*rows_x[le], *cots, expert_gate, expert_up, expert_down)
        if le == 0:
            res = tie(res, halves[1])
            halves = halve(add2(*halves), bits[0], 0)
        else:
            res = tie(res, crossed)
        saved.append(res[4:])
        r1, inward = beside_sums(res[:4])
        crossed = swap(tie(inward, crossed), 2)
        home_in.append((res[0], r1, crossed))
    home_rows = []
    for le in range(last):
        home_rows.append(exchange(tie(add3(*home_in[le]), *home_rows)))
    before_weights = (inward, *[add3(*home_in[le]) for le in range(last)])
    across_last = crossed
    shared_back = to_owner(sh[4:8], after=(crossed,))
    crossed = shared_back[2]

    grads = ()
    res_in = []
    for le in range(exp_dev):
        args = (*tie(rows_x[le], *before_weights), *cots, *saved[le], expert_down)
        specs = [rows_blk] * 4 + [cot_blk(le)] * 4 + [saved_blk] * 3 + [weight_blk(le, exp_hidden, dim)]
        aliases = {len(args) + i: 4 + i for i in range(len(grads))}
        done = pl.pallas_call(
            functools.partial(weights_body, le > 0),
            grid=(steps,),
            out_shape=(row_out,) * 4
            + (
                sds((exp_dev, dim, exp_hidden), F32),
                sds((exp_dev, dim, exp_hidden), F32),
                sds((exp_dev, exp_hidden, dim), F32),
            ),
            in_specs=specs + [ANY] * len(grads),
            out_specs=(rows_blk,) * 4
            + (
                weight_blk(le, dim, exp_hidden),
                weight_blk(le, dim, exp_hidden),
                weight_blk(le, exp_hidden, dim),
            ),
            scratch_shapes=[
                pltpu.VMEM((4 * src * cap, dim), BF16),
                pltpu.VMEM((4 * src * cap, dim), BF16),
            ],
            input_output_aliases=aliases,
            compiler_params=params(1),
            cost_estimate=cost(4 * expert_flops, 16e6),
            name="weights",
        )(*args, *grads)
        done = tie(done, across_last) if le == 0 else tie(done, home_rows[0], crossed)
        grads = done[4:]
        res_in.append(done[:4])
    p0, r1, rx = home_in[last]
    home_rows.append(exchange(tie(add3(p0, r1, tie(rx, grads)), *home_rows)))
    for le in range(exp_dev):
        res_in[le] = to_owner(res_in[le], after=(crossed,))
        crossed = res_in[le][2]

    both_res = jnp.stack([add3(*terms) for terms in res_in], axis=1)
    for bit in bits[1:]:
        halves = halve(tie(add2(*halves), home_rows[0]), bit, 0)

    grad_hidden, dh, gain_ffn = pl.pallas_call(
        functools.partial(home_body, exp_dev, tb),
        out_shape=(sds((tb, dim), F32), block, sds((1, dim), F32)),
        in_specs=[SMEM] + [VMEM] * (2 * exp_dev + 7),
        out_specs=(VMEM,) * 3,
        compiler_params=params(),
        cost_estimate=cost(1e9, 5e6),
        name="home",
    )(
        where,
        *home_rows,
        *slot_le,
        *shared_back,
        tie(hidden, *grads, both_res),
        gain_b,
        cotangent,
        codes,
    )

    h_all = to_all(dh)
    home_res = exchange(tie(both_res, home_rows[last]))
    shared_fwd = to_owner(sh[0:4], after=(h_all[2],))
    rows_each = dim // expert_count
    direct = rows_each % 16 == 0
    gw_shape = (expert_count, rows_each + 16, dim) if direct else (dim, dim)
    back = pl.pallas_call(
        functools.partial(attend_back_body, tb),
        out_shape=(block,) * 4 + (sds(gw_shape, BF16), sds((4, dim), F32)),
        in_specs=[SMEM] + [VMEM] * 21,
        out_specs=(VMEM,) * 6,
        scratch_shapes=[
            pltpu.VMEM((seq_len, width), F32),
            pltpu.VMEM((seq_len, width), F32),
            pltpu.VMEM((seq_len, dim), BF16),
            pltpu.VMEM((seq_len, width), BF16),
            pltpu.VMEM((width, seq_len), BF16),
            pltpu.VMEM((width, seq_len), BF16),
            pltpu.VMEM((seq_len, width), F32),
            pltpu.VMEM((width, seq_len), F32),
            pltpu.VMEM((width, seq_len), F32),
            pltpu.VMEM((3, seq_len, width), BF16),
        ],
        compiler_params=params(),
        cost_estimate=cost(20e9, 10e6, 3e6),
        name="attend_back",
    )(
        info,
        *h_all,
        gain_a,
        gain_ffn,
        wq_t,
        wk_t,
        wv_t,
        w_output,
        act_a,
        q,
        k,
        v,
        att,
        lse,
        *rope,
    )
    back = tie(back, halves[1])
    gw = back[4]
    if not direct:
        gain_part = jnp.broadcast_to(back[5].astype(BF16)[None], (expert_count, 4, dim))
        gw = jnp.concatenate([gw.reshape(expert_count, rows_each, dim), gain_part], axis=1)
    r1, inward = beside_sums(back[:4])
    gw = exchange(tie(gw, home_res, inward))
    da_parts = (back[0], r1, swap(inward, 2))
    kept, got = halves
    shared_grads = (kept.astype(F32) + tie(got, da_parts).astype(F32))[0]
    grad_inputs = pl.pallas_call(
        grad_in_body,
        out_shape=sds((tb, dim), F32),
        in_specs=[VMEM] * 6,
        out_specs=VMEM,
        compiler_params=params(),
        cost_estimate=cost(1e7, 4e6),
        name="grad_in",
    )(inputs, *da_parts, grad_hidden, gain_a)
    layer_out = pl.pallas_call(
        functools.partial(layer_out_body, exp_dev),
        out_shape=sds((tb, dim), F32),
        in_specs=[SMEM] + [VMEM] * (exp_dev + 7),
        out_specs=VMEM,
        compiler_params=params(),
        cost_estimate=cost(1e9, 4e6),
        name="layer_out",
    )(where, tie(home_res, back), *slot_le, hidden, *shared_fwd, codes, gates_b)
    gw = jnp.sum(tie(gw, layer_out, grad_inputs).astype(F32), axis=0)
    gains = jnp.sum(gw[rows_each : rows_each + 4].reshape(2, 2, dim), axis=1)
    gains = gains + swap(gains, 1)
    gains = gains + swap(gains, 2)
    gw = [gw[:rows_each, i * width : (i + 1) * width] for i in range(4)]
    return (
        layer_out,
        grad_inputs,
        gains[0],
        gw[0],
        gw[1],
        gw[2],
        gw[3].T,
        gains[1],
        shared_grads[:, :hidden_units],
        shared_grads[:, hidden_units : 2 * hidden_units],
        shared_grads[:, 2 * hidden_units :].T,
        grads[0],
        grads[1],
        grads[2],
    )


def solution(mesh):
    return jax.shard_map(
        per_device,
        mesh=mesh,
        in_specs=(
            P(("expert", "tensor"), None),
            P(),
            P(None, "tensor"),
            P(None, "tensor"),
            P(None, "tensor"),
            P("tensor", None),
            P(),
            P(None, "tensor"),
            P(None, "tensor"),
            P("tensor", None),
            P("expert", None, "tensor"),
            P("expert", None, "tensor"),
            P("expert", "tensor", None),
            P("expert", None),
            P("expert", None),
            P("expert"),
            P("expert", None),
        ),
        out_specs=(
            P(("expert", "tensor"), None),
            P(("expert", "tensor"), None),
            P(),
            P("expert", "tensor"),
            P("expert", "tensor"),
            P("expert", "tensor"),
            P("tensor", "expert"),
            P(),
            P("expert", "tensor"),
            P("expert", "tensor"),
            P("tensor", "expert"),
            P("expert", None, "tensor"),
            P("expert", None, "tensor"),
            P("expert", "tensor", None),
        ),
        check_vma=False,
    )
```

```python
import functools

import jax
import jax.numpy as jnp
import numpy as np
from jax import lax
from jax.experimental import pallas as pl
from jax.experimental.pallas import tpu as pltpu
from jax.sharding import PartitionSpec as P

HDIM = 64
ROUTED_EXPERTS = 16
EPS = 1e-05
F32 = jnp.float32
BF16 = jnp.bfloat16
ROPE_STEP = 32

VMEM = pl.BlockSpec(memory_space=pltpu.VMEM)
SMEM = pl.BlockSpec(memory_space=pltpu.SMEM)
ANY = pl.BlockSpec(memory_space=pl.ANY)


def sds(shape, dtype):
    return jax.ShapeDtypeStruct(tuple(shape), dtype)


def params(n_grid=0):
    if n_grid:
        return pltpu.CompilerParams(
            vmem_limit_bytes=60 * 1024 * 1024, dimension_semantics=("arbitrary",) * n_grid
        )
    return pltpu.CompilerParams(vmem_limit_bytes=60 * 1024 * 1024)


def nn(a, b):
    return jnp.dot(a, b, preferred_element_type=F32)


def nt(a, b):
    return lax.dot_general(a, b, (((1,), (1,)), ((), ())), preferred_element_type=F32)


def tn(a, b):
    return lax.dot_general(a, b, (((0,), (0,)), ((), ())), preferred_element_type=F32)


def swap(x, bit):
    count = lax.axis_size("tensor")
    return lax.ppermute(x, "tensor", [(i, i ^ bit) for i in range(count)])


def rope_parts(seq_len, width):
    half = HDIM // 2
    frequency = 10000.0 ** (-np.arange(half, dtype=np.float64) * 2.0 / HDIM)
    lanes = np.tile(np.concatenate([frequency, frequency]), width // HDIM)
    sign = np.tile(np.concatenate([-np.ones(half), np.ones(half)]), width // HDIM)
    coarse = np.arange(0, seq_len, ROPE_STEP)[:, None] * lanes[None, :]
    fine = np.arange(ROPE_STEP)[:, None] * lanes[None, :]
    return tuple(
        jnp.asarray(a, dtype=F32)
        for a in (np.cos(coarse), np.sin(coarse), np.cos(fine), np.sin(fine), sign[None, :])
    )


def fill_rope(cos_coarse, sin_coarse, cos_fine, sin_fine, sign, cos_out, sin_out):
    cf, sf, sg = cos_fine[...], sin_fine[...], sign[...]

    def step(a, _):
        cc = cos_coarse[pl.ds(a, 1), :]
        sc = sin_coarse[pl.ds(a, 1), :]
        at = pl.ds(pl.multiple_of(a * ROPE_STEP, ROPE_STEP), ROPE_STEP)
        cos_out[at, :] = cc * cf - sc * sf
        sin_out[at, :] = (sc * cf + cc * sf) * sg
        return 0

    lax.fori_loop(0, cos_coarse.shape[0], step, 0)


def half_swap_matrix(width):
    row = lax.broadcasted_iota(jnp.int32, (width, width), 0)
    col = lax.broadcasted_iota(jnp.int32, (width, width), 1)
    half = HDIM // 2
    partner = jnp.where((col & half) == 0, col + half, col - half)
    return jnp.where(row == partner, 1.0, 0.0).astype(BF16)


def rms(values):
    return lax.rsqrt(jnp.mean(values * values, axis=-1, keepdims=True) + EPS)


def slot_pick(codes_k0, codes_k1, slot_code):
    first = codes_k0 == slot_code
    second = codes_k1 == slot_code
    return first, second


def prep_body(cap, tb, where_ref, routes_ref, gates_ref, dy_ref, *rest):
    t = where_ref[0]
    blocks = routes_ref.shape[0]
    slots = rest[:-2]
    codes_ref, rows_ref = rest[-2:]
    upper = jnp.where(
        lax.broadcasted_iota(jnp.int32, (tb, tb), 0) < lax.broadcasted_iota(jnp.int32, (tb, tb), 1),
        1.0,
        0.0,
    ).astype(BF16)
    ids = lax.broadcasted_iota(jnp.int32, (ROUTED_EXPERTS, tb), 0)
    for b in range(blocks):
        r0 = routes_ref[b, 0:1, :]
        r1 = routes_ref[b, 1:2, :]
        e0 = ids == r0
        e1 = ids == r1
        named = jnp.where(e0, 1.0, 0.0) + jnp.where(e1, 1.0, 0.0)
        before = nn(named.astype(BF16), upper)
        k0 = jnp.sum(jnp.where(e0, before, 0.0), axis=0, keepdims=True)
        k1 = jnp.sum(jnp.where(e1, before, 0.0), axis=0, keepdims=True)
        codes_ref[b, 0:1, :] = r0 * cap + k0.astype(jnp.int32)
        codes_ref[b, 1:2, :] = r1 * cap + k1.astype(jnp.int32)
    c0 = codes_ref[t, 0:1, :]
    c1 = codes_ref[t, 1:2, :]
    g0 = gates_ref[t, 0:1, :]
    g1 = gates_ref[t, 1:2, :]
    dy = dy_ref[pl.ds(pl.multiple_of(t * tb, tb), tb), :]
    for le, slot_ref in enumerate(slots):
        first, second = slot_pick(c0, c1, slot_ref[...])
        gate = jnp.sum(
            jnp.where(first, g0, 0.0) + jnp.where(second, g1, 0.0), axis=1, keepdims=True
        )
        pick = jnp.where(first | second, 1.0, 0.0).astype(BF16)
        got = nn(pick, dy) * gate
        rows_ref[:, le] = got.astype(BF16).reshape(rows_ref.shape[0], cap, got.shape[1])


def attend_body(
    tb,
    info_ref,
    x0,
    x1,
    x2,
    x3,
    gain_ref,
    wq_ref,
    wk_ref,
    wv_ref,
    wo_ref,
    cos_coarse,
    sin_coarse,
    cos_fine,
    sin_fine,
    sign,
    act_ref,
    q_ref,
    k_ref,
    v_ref,
    att_ref,
    lse_ref,
    out0,
    out1,
    out2,
    out3,
    cos_s,
    sin_s,
):
    t = info_ref[0]
    prefix = info_ref[1]
    seq_len, width = q_ref.shape
    blocks = seq_len // tb
    heads = width // HDIM
    fill_rope(cos_coarse, sin_coarse, cos_fine, sin_fine, sign, cos_s, sin_s)
    gain = gain_ref[...]
    for j, piece in enumerate((x0, x1, x2, x3)):
        x = piece[...].astype(F32)
        at = pl.ds(pl.multiple_of((t ^ j) * tb, tb), tb)
        act_ref[at, :] = (x * rms(x) * gain).astype(BF16)
    flip = half_swap_matrix(width)
    wq = wq_ref[...]
    wk = wk_ref[...]
    wq_flip = nn(flip, wq).astype(BF16)
    wk_flip = nn(flip, wk).astype(BF16)
    scale = HDIM ** (-0.5)

    def project(b, _):
        at = pl.ds(pl.multiple_of(b * tb, tb), tb)
        a = act_ref[at, :]
        cos, sin = cos_s[at, :], sin_s[at, :]
        q_ref[at, :] = (scale * (nt(a, wq) * cos + nt(a, wq_flip) * sin)).astype(BF16)
        k_ref[at, :] = (nt(a, wk) * cos + nt(a, wk_flip) * sin).astype(BF16)
        v_ref[at, :] = nt(a, wv_ref[...]).astype(BF16)
        return 0

    lax.fori_loop(0, blocks, project, 0)
    lane_head = lax.broadcasted_iota(jnp.int32, (tb, width), 1) // HDIM
    lane = lax.broadcasted_iota(jnp.int32, (tb, lse_ref.shape[1]), 1)
    for b in range(blocks):
        extent = max(seq_len // 2, (b + 1) * tb)
        rows = slice(b * tb, (b + 1) * tb)
        qb = q_ref[rows, :]
        limit = jnp.maximum(
            b * tb + lax.broadcasted_iota(jnp.int32, (tb, 1), 0), prefix - 1
        )
        allowed = lax.broadcasted_iota(jnp.int32, (tb, extent), 1) <= limit

        def one_head(h, carried, extent=extent, qb=qb, allowed=allowed):
            att, lse = carried
            mine = lane_head == h
            scores = nt(jnp.where(mine, qb, jnp.zeros_like(qb)), k_ref[:extent, :])
            scores = jnp.where(allowed, scores, -1e30)
            top = jnp.max(scores, axis=-1, keepdims=True)
            weight = jnp.exp(scores - top)
            total = jnp.sum(weight, axis=-1, keepdims=True)
            got = nn(weight.astype(BF16), v_ref[:extent, :]) / total
            att = jnp.where(mine, got, att)
            lse = jnp.where(lane == h, top + jnp.log(total), lse)
            return att, lse

        att, lse = lax.fori_loop(
            0,
            heads,
            one_head,
            (jnp.zeros((tb, width), F32), jnp.zeros((tb, lse_ref.shape[1]), F32)),
        )
        att = att.astype(BF16)
        att_ref[rows, :] = att
        lse_ref[rows, :] = lse
        part = nn(att, wo_ref[...]).astype(BF16)
        for j, out in enumerate((out0, out1, out2, out3)):

            @pl.when((t ^ b) == j)
            def _(out=out, part=part):
                out[...] = part


def dispatch_body(t_blocks, cap, where_ref, x_ref, p0, p1, p2, gain_ref, codes_ref, *rest):
    slots = rest[: t_blocks]
    hidden_ref, act_ref = rest[t_blocks : t_blocks + 2]
    bufs = rest[t_blocks + 2 :]
    t = where_ref[0]
    hidden = (
        x_ref[...].astype(F32)
        + p0[...].astype(F32)
        + p1[...].astype(F32)
        + p2[...].astype(F32)
    )
    hidden_ref[...] = hidden
    act = (hidden * rms(hidden) * gain_ref[...]).astype(BF16)
    act_ref[...] = act
    c0 = codes_ref[t, 0:1, :]
    c1 = codes_ref[t, 1:2, :]
    for slot_ref, buf in zip(slots, bufs, strict=True):
        first, second = slot_pick(c0, c1, slot_ref[...])
        pick = jnp.where(first | second, 1.0, 0.0).astype(BF16)
        got = nn(pick, act).astype(BF16)
        buf[...] = got.reshape(buf.shape)


def shared_body(
    tb,
    where_ref,
    a0,
    a1,
    a2,
    a3,
    dy_ref,
    gate_ref,
    up_ref,
    down_ref,
    f0,
    f1,
    f2,
    f3,
    b0,
    b1,
    b2,
    b3,
    grads_ref,
    act_s,
    dy_s,
    hs_s,
    dg_s,
    du_s,
    f_s,
    b_s,
):
    t = where_ref[0]
    blocks = 4
    for j, piece in enumerate((a0, a1, a2, a3)):
        act_s[j * tb : (j + 1) * tb, :] = piece[...]
        dy_s[j * tb : (j + 1) * tb, :] = dy_ref[pl.ds(pl.multiple_of((t ^ j) * tb, tb), tb), :]

    def block(j, _):
        at = pl.ds(pl.multiple_of(j * tb, tb), tb)
        a = act_s[at, :]
        dy = dy_s[at, :]
        g = nn(a, gate_ref[...])
        u = nn(a, up_ref[...])
        sig = jax.nn.sigmoid(g)
        silu = g * sig
        hs = (silu * u).astype(BF16)
        dhs = nt(dy, down_ref[...])
        dg = (dhs * u * sig * (1.0 + g * (1.0 - sig))).astype(BF16)
        du = (dhs * silu).astype(BF16)
        hs_s[at, :] = hs
        dg_s[at, :] = dg
        du_s[at, :] = du
        f_s[at, :] = nn(hs, down_ref[...]).astype(BF16)
        b_s[at, :] = (nt(dg, gate_ref[...]) + nt(du, up_ref[...])).astype(BF16)
        return 0

    lax.fori_loop(0, blocks, block, 0)
    for j, (f, b) in enumerate(((f0, b0), (f1, b1), (f2, b2), (f3, b3))):
        f[...] = f_s[j * tb : (j + 1) * tb, :]
        b[...] = b_s[j * tb : (j + 1) * tb, :]
    hidden = hs_s.shape[1]

    def columns(c, _):
        at = pl.ds(pl.multiple_of(c * tb, tb), tb)
        a = act_s[:, at]
        dy = dy_s[:, at]
        grads_ref[at, 0:hidden] = tn(a, dg_s[...]).astype(BF16)
        grads_ref[at, hidden : 2 * hidden] = tn(a, du_s[...]).astype(BF16)
        grads_ref[at, 2 * hidden : 3 * hidden] = tn(dy, hs_s[...]).astype(BF16)
        return 0

    lax.fori_loop(0, act_s.shape[1] // tb, columns, 0)


def expert_body(x0, x1, x2, x3, c0, c1, c2, c3, gate_ref, up_ref, down_ref, *outs):
    o = outs[:4]
    he_ref, dg_ref, du_ref = outs[4:7]
    n_src, cap, dim = x0.shape
    rows = n_src * cap
    gate = gate_ref[0]
    up = up_ref[0]
    down = down_ref[0]
    xs = (x0, x1, x2, x3)
    cs = (c0, c1, c2, c3)
    for j in (3, 1, 2, 0):
        x = xs[j][...].reshape(rows, dim)
        c = cs[j][...].reshape(rows, dim)
        g = nn(x, gate)
        u = nn(x, up)
        sig = jax.nn.sigmoid(g)
        silu = g * sig
        dhe = nt(c, down)
        dg = (dhe * u * sig * (1.0 + g * (1.0 - sig))).astype(BF16)
        du = (dhe * silu).astype(BF16)
        he_ref[j] = (silu * u).astype(BF16)
        dg_ref[j] = dg
        du_ref[j] = du
        o[j][...] = (nt(dg, gate) + nt(du, up)).astype(BF16).reshape(n_src, cap, dim)


def weights_body(aliased, x0, x1, x2, x3, c0, c1, c2, c3, he_ref, dg_ref, du_ref, down_ref, *rest):
    if aliased:
        rest = rest[3:]
    o = rest[:4]
    gg_ref, gu_ref, gd_ref, x_s, c_s = rest[4:]
    n_src, cap, dim = x0.shape
    rows = n_src * cap
    step = pl.program_id(0)
    down = down_ref[0]
    cs = (c0, c1, c2, c3)
    for j, x in enumerate((x0, x1, x2, x3)):
        x_s[j * rows : (j + 1) * rows, :] = x[...].reshape(rows, dim)
        c_s[j * rows : (j + 1) * rows, :] = cs[j][...].reshape(rows, dim)
        o[j][...] = nn(he_ref[j], down).astype(BF16).reshape(n_src, cap, dim)
    hidden = he_ref.shape[2]
    he = he_ref[...].reshape(4 * rows, hidden)
    dg = dg_ref[...].reshape(4 * rows, hidden)
    du = du_ref[...].reshape(4 * rows, hidden)
    gg = tn(x_s[...], dg)
    gu = tn(x_s[...], du)
    gd = tn(he, c_s[...])

    @pl.when(step == 0)
    def _():
        gg_ref[0] = gg
        gu_ref[0] = gu
        gd_ref[0] = gd

    @pl.when(step > 0)
    def _():
        gg_ref[0] += gg
        gu_ref[0] += gu
        gd_ref[0] += gd


def home_body(n_le, tb, where_ref, *rest):
    backs = rest[:n_le]
    slots = rest[n_le : 2 * n_le]
    s0, s1, s2, hidden_ref, gain_ref, dy_ref, codes_ref = rest[2 * n_le : 2 * n_le + 7]
    gh_ref, dh_ref, gg_ref = rest[2 * n_le + 7 :]
    t = where_ref[0]
    db = s0[...].astype(F32) + s1[...].astype(F32) + s2[...].astype(F32)
    c0 = codes_ref[t, 0:1, :]
    c1 = codes_ref[t, 1:2, :]
    for back, slot_ref in zip(backs, slots, strict=True):
        first, second = slot_pick(c0, c1, slot_ref[...])
        pick = jnp.where(first | second, 1.0, 0.0).astype(BF16)
        db += tn(pick, back[...].reshape(pick.shape[0], db.shape[1]))
    hidden = hidden_ref[...]
    factor = rms(hidden)
    n = hidden * factor
    inner = db * gain_ref[...]
    dy = dy_ref[pl.ds(pl.multiple_of(t * tb, tb), tb), :].astype(F32)
    gh = dy + factor * (inner - n * jnp.mean(inner * n, axis=-1, keepdims=True))
    gh_ref[...] = gh
    dh_ref[...] = gh.astype(BF16)
    gg_ref[...] = jnp.sum(db * n, axis=0, keepdims=True)


def attend_back_body(
    tb,
    info_ref,
    h0,
    h1,
    h2,
    h3,
    gain_ref,
    gb_ref,
    wq_ref,
    wk_ref,
    wv_ref,
    wo_ref,
    act_ref,
    q_ref,
    k_ref,
    v_ref,
    att_ref,
    lse_ref,
    cos_coarse,
    sin_coarse,
    cos_fine,
    sin_fine,
    sign,
    o0,
    o1,
    o2,
    o3,
    gw_ref,
    gg_ref,
    cos_s,
    sin_s,
    dh_s,
    dat_s,
    qt_s,
    datt_s,
    dq_s,
    dkt_s,
    dvt_s,
    raw_s,
):
    t = info_ref[0]
    prefix = info_ref[1]
    seq_len, width = q_ref.shape
    blocks = seq_len // tb
    heads = width // HDIM
    scale = HDIM ** (-0.5)
    fill_rope(cos_coarse, sin_coarse, cos_fine, sin_fine, sign, cos_s, sin_s)
    for j, piece in enumerate((h0, h1, h2, h3)):
        at = pl.ds(pl.multiple_of((t ^ j) * tb, tb), tb)
        dh = piece[...]
        dh_s[at, :] = dh
        dat_s[at, :] = nt(dh, wo_ref[...]).astype(BF16)
    for b in range(blocks):
        rows = slice(b * tb, (b + 1) * tb)
        qt_s[:, rows] = q_ref[rows, :].T
        datt_s[:, rows] = dat_s[rows, :].T
    dkt_s[...] = jnp.zeros_like(dkt_s)
    dvt_s[...] = jnp.zeros_like(dvt_s)
    lane_head = lax.broadcasted_iota(jnp.int32, (tb, width), 1) // HDIM
    lane = lax.broadcasted_iota(jnp.int32, (tb, lse_ref.shape[1]), 1)
    for b in range(blocks):
        extent = max(seq_len // 2, (b + 1) * tb)
        rows = slice(b * tb, (b + 1) * tb)
        qb = q_ref[rows, :]
        datb = dat_s[rows, :]
        mix = datb.astype(F32) * att_ref[rows, :].astype(F32)
        lse_b = lse_ref[rows, :]
        limit = jnp.maximum(
            b * tb + lax.broadcasted_iota(jnp.int32, (tb, 1), 0), prefix - 1
        )
        allowed = lax.broadcasted_iota(jnp.int32, (tb, extent), 1) <= limit

        def one_head(h, dq, extent=extent, rows=rows, qb=qb, datb=datb, mix=mix, lse_b=lse_b, allowed=allowed):
            mine = lane_head == h
            lse = jnp.sum(jnp.where(lane == h, lse_b, 0.0), axis=-1, keepdims=True)
            delta = jnp.sum(jnp.where(mine, mix, 0.0), axis=-1, keepdims=True)
            scores = nt(jnp.where(mine, qb, jnp.zeros_like(qb)), k_ref[:extent, :])
            prob = jnp.exp(jnp.where(allowed, scores, -1e30) - lse)
            dp = nt(jnp.where(mine, datb, jnp.zeros_like(datb)), v_ref[:extent, :])
            ds = (prob * (dp - delta)).astype(BF16)
            at = pl.ds(pl.multiple_of(h * HDIM, HDIM), HDIM)
            dkt_s[at, :extent] += nn(qt_s[at, rows], ds)
            dvt_s[at, :extent] += nn(datt_s[at, rows], prob.astype(BF16))
            return jnp.where(mine, nn(ds, k_ref[:extent, :]), dq)

        dq_s[rows, :] = lax.fori_loop(0, heads, one_head, jnp.zeros((tb, width), F32))
    flip = half_swap_matrix(width)

    def unrotate(u, at):
        high = u.astype(BF16)
        low = (u - high.astype(F32)).astype(BF16)
        return (u * cos_s[at, :] - (nn(high, flip) + nn(low, flip)) * sin_s[at, :]).astype(BF16)

    gain_sum = jnp.zeros((1, act_ref.shape[1]), F32)
    for b in range(blocks):
        rows = slice(b * tb, (b + 1) * tb)
        dq = unrotate(dq_s[rows, :] * scale, rows)
        dk = unrotate(dkt_s[:, rows].T, rows)
        dv = dvt_s[:, rows].T.astype(BF16)
        raw_s[0, rows, :] = dq
        raw_s[1, rows, :] = dk
        raw_s[2, rows, :] = dv
        da = nn(dq, wq_ref[...]) + nn(dk, wk_ref[...]) + nn(dv, wv_ref[...])
        gain_sum += jnp.sum(da * act_ref[rows, :].astype(F32), axis=0, keepdims=True)
        part = da.astype(BF16)
        for j, out in enumerate((o0, o1, o2, o3)):

            @pl.when((t ^ b) == j)
            def _(out=out, part=part):
                out[...] = part

    gain_a = gain_sum / gain_ref[...]
    g = [tn(raw_s[i], act_ref[...]).T for i in range(3)] + [tn(att_ref[...], dh_s[...]).T]
    g = jnp.concatenate(g, axis=1).astype(BF16)
    flat = []
    for gain in (gain_a, gb_ref[...]):
        high = gain.astype(BF16).astype(F32)
        flat += [high, gain - high]
    if len(gw_ref.shape) == 2:
        gw_ref[...] = g
        gg_ref[...] = jnp.concatenate(flat, axis=0)
    else:
        gg_ref[...] = jnp.zeros_like(gg_ref)
        each = g.shape[0] // gw_ref.shape[0]
        gw_ref[:, :each] = g.reshape(gw_ref.shape[0], each, g.shape[1])
        rest = gw_ref.shape[1] - each
        lines = jnp.concatenate(flat + [jnp.zeros((rest - 4, g.shape[1]), F32)], axis=0)
        gw_ref[:, each:] = jnp.broadcast_to(
            lines.astype(BF16)[None], (gw_ref.shape[0], rest, g.shape[1])
        )


def layer_out_body(n_le, where_ref, back_ref, *rest):
    slots = rest[:n_le]
    hidden_ref, s0, s1, s2, codes_ref, gates_ref, out_ref = rest[n_le:]
    t = where_ref[0]
    out = (
        hidden_ref[...] + s0[...].astype(F32) + s1[...].astype(F32) + s2[...].astype(F32)
    )
    c0 = codes_ref[t, 0:1, :]
    c1 = codes_ref[t, 1:2, :]
    g0 = gates_ref[t, 0:1, :]
    g1 = gates_ref[t, 1:2, :]
    for le, slot_ref in enumerate(slots):
        first, second = slot_pick(c0, c1, slot_ref[...])
        weight = jnp.where(first, g0, 0.0) + jnp.where(second, g1, 0.0)
        high = weight.astype(BF16)
        low = (weight - high.astype(F32)).astype(BF16)
        rows = back_ref[:, le].reshape(high.shape[0], out.shape[1])
        out += tn(high, rows) + tn(low, rows)
    out_ref[...] = out


def grad_in_body(x_ref, p0, p1, p2, gh_ref, gain_ref, out_ref):
    x = x_ref[...].astype(F32)
    da = p0[...].astype(F32) + p1[...].astype(F32) + p2[...].astype(F32)
    factor = rms(x)
    n = x * factor
    inner = da * gain_ref[...]
    out_ref[...] = gh_ref[...] + factor * (
        inner - n * jnp.mean(inner * n, axis=-1, keepdims=True)
    )


def tie(x, *deps):
    return lax.optimization_barrier((x, deps))[0]


def cost(flops, read, transcendentals=0):
    return pl.CostEstimate(
        flops=int(flops * 0.4), bytes_accessed=int(read * 0.4), transcendentals=0
    )


def add2(a, b):
    return (a.astype(F32) + b.astype(F32)).astype(BF16)


def add3(a, b, c):
    return (a.astype(F32) + b.astype(F32) + c.astype(F32)).astype(BF16)


def beside_sums(pieces):
    r3 = swap(pieces[3], 1)
    r1 = swap(pieces[1], 1)
    return r1, add2(pieces[2], r3)


def to_owner(pieces, after=()):
    r1, inward = beside_sums(pieces)
    return pieces[0], r1, swap(tie(inward, *after), 2)


def to_all(own, after=(), across=None, during=()):
    if across is None:
        across = swap(tie(own, *after), 2)
    beside = swap(own, 1)
    both = swap(tie(across, *during), 1)
    return own, beside, across, both


def exchange(x):
    return lax.all_to_all(x, "expert", split_axis=0, concat_axis=0, tiled=True)


def halve(x, bit, axis):
    count = lax.axis_size("expert")
    x = x.reshape(*((-1, 2) if axis else (2, -1)), *x.shape[1:])
    mine = (lax.axis_index("expert") // bit) % 2
    keep = lax.dynamic_index_in_dim(x, mine, axis, keepdims=False)
    send = lax.dynamic_index_in_dim(x, 1 - mine, axis, keepdims=False)
    return keep, lax.ppermute(send, "expert", [(i, i ^ bit) for i in range(count)])


def per_device(
    inputs,
    attn_gain,
    w_query,
    w_key,
    w_value,
    w_output,
    ffn_gain,
    shared_gate,
    shared_up,
    shared_down,
    expert_gate,
    expert_up,
    expert_down,
    routes,
    gate_values,
    prefix,
    cotangent,
):
    tensor_count = lax.axis_size("tensor")
    expert_count = lax.axis_size("expert")
    assert tensor_count == 4
    t = lax.axis_index("tensor")
    tb, dim = inputs.shape
    seq_len, choices = routes.shape
    width = w_query.shape[1]
    hidden_units = shared_gate.shape[1]
    exp_hidden = expert_gate.shape[2]
    exp_dev = expert_gate.shape[0]
    slabs = max(1, expert_count // ROUTED_EXPERTS)
    cap = max(2, 3 * tb * choices // (2 * ROUTED_EXPERTS))
    where = jnp.reshape(t, (1,)).astype(jnp.int32)
    info = jnp.stack([t.astype(jnp.int32), prefix[0]])
    gain_a = attn_gain.reshape(1, dim)
    gain_b = ffn_gain.reshape(1, dim)
    wq_t, wk_t, wv_t = w_query.T, w_key.T, w_value.T

    entries = np.arange(expert_count * exp_dev)
    slot_np = (entries // slabs)[:, None] * cap + np.arange(cap)[None, :]
    slot_np = slot_np.reshape(expert_count, exp_dev, cap).astype(np.int32)
    slot_le = [jnp.asarray(slot_np[:, le].reshape(-1, 1)) for le in range(exp_dev)]
    last = exp_dev - 1

    x2 = swap(inputs, 2)

    routes_b = routes.reshape(tensor_count, tb, choices).transpose(0, 2, 1)
    gates_b = gate_values.reshape(tensor_count, tb, choices).transpose(0, 2, 1)
    codes, cot_rows = pl.pallas_call(
        functools.partial(prep_body, cap, tb),
        out_shape=(
            sds((tensor_count, choices, tb), jnp.int32),
            sds((expert_count, exp_dev, cap, dim), BF16),
        ),
        in_specs=[SMEM] + [VMEM] * (3 + exp_dev),
        out_specs=(VMEM, VMEM),
        compiler_params=params(),
        cost_estimate=cost(2e9, 6e6),
        name="prep",
    )(where, routes_b, gates_b, cotangent, *slot_le)
    cot = exchange(cot_rows)
    x1 = swap(inputs, 1)
    x3 = swap(tie(x2, codes), 1)

    rope = rope_parts(seq_len, width)
    block = sds((tb, dim), BF16)
    att_out = pl.pallas_call(
        functools.partial(attend_body, tb),
        out_shape=(
            sds((seq_len, dim), BF16),
            sds((seq_len, width), BF16),
            sds((seq_len, width), BF16),
            sds((seq_len, width), BF16),
            sds((seq_len, width), BF16),
            sds((seq_len, 128), F32),
            block,
            block,
            block,
            block,
        ),
        in_specs=[SMEM] + [VMEM] * 14,
        out_specs=(VMEM,) * 10,
        scratch_shapes=[pltpu.VMEM((seq_len, width), F32)] * 2,
        compiler_params=params(),
        cost_estimate=cost(3e9, 3e6, 3e6),
        name="attend",
    )(info, inputs, x1, x2, x3, gain_a, wq_t, wk_t, wv_t, w_output, *rope)
    act_a, q, k, v, att, lse = att_out[:6]
    r1, inward = beside_sums(att_out[6:])
    crossed = swap(inward, 2)
    parts = (att_out[6], r1, crossed)

    got = pl.pallas_call(
        functools.partial(dispatch_body, exp_dev, cap),
        out_shape=(sds((tb, dim), F32), block)
        + (sds((expert_count, cap, dim), BF16),) * exp_dev,
        in_specs=[SMEM] + [VMEM] * (6 + exp_dev),
        out_specs=(VMEM,) * (2 + exp_dev),
        compiler_params=params(),
        cost_estimate=cost(1e9, 4e6),
        name="dispatch",
    )(where, inputs, *parts, gain_b, codes, *slot_le)
    hidden, act_b = got[:2]
    a_all = to_all(act_b)

    sh = pl.pallas_call(
        functools.partial(shared_body, tb),
        out_shape=(block,) * 8 + (sds((dim, 3 * hidden_units), BF16),),
        in_specs=[SMEM] + [VMEM] * 8,
        out_specs=(VMEM,) * 9,
        scratch_shapes=[
            pltpu.VMEM((seq_len, dim), BF16),
            pltpu.VMEM((seq_len, dim), BF16),
            pltpu.VMEM((seq_len, hidden_units), BF16),
            pltpu.VMEM((seq_len, hidden_units), BF16),
            pltpu.VMEM((seq_len, hidden_units), BF16),
            pltpu.VMEM((seq_len, dim), BF16),
            pltpu.VMEM((seq_len, dim), BF16),
        ],
        compiler_params=params(),
        cost_estimate=cost(8e9, 12e6),
        name="shared",
    )(where, *a_all, cotangent, shared_gate, shared_up, shared_down)

    rows_x = []
    cot_across = swap(tie(cot, a_all[2]), 2)
    cots = to_all(cot, across=cot_across, during=(sh[8],))
    crossed = cot_across
    sent = cot
    for le in range(exp_dev):
        sent = exchange(tie(got[2 + le], sent, sh[8] if le else sent))
        crossed = swap(tie(sent, crossed), 2)
        rows_x.append((sent, crossed))

    src = min(8, expert_count)
    steps = expert_count // src
    rows_blk = pl.BlockSpec((src, cap, dim), lambda i: (i, 0, 0))
    saved_blk = pl.BlockSpec((4, src * cap, exp_hidden), lambda i: (0, i, 0))

    def cot_blk(le):
        return pl.BlockSpec((src, pl.Squeezed(), cap, dim), lambda i: (i, le, 0, 0))

    def weight_blk(le, a, b):
        return pl.BlockSpec((1, a, b), lambda i: (le, 0, 0))

    all_rows = expert_count * cap
    row_out = sds((expert_count, cap, dim), BF16)
    saved_out = sds((4, all_rows, exp_hidden), BF16)
    expert_flops = 2 * 4 * all_rows * dim * exp_hidden
    bits = [1 << i for i in range(1, expert_count.bit_length() - 1)][::-1]
    halves = halve(tie(sh[8], cot_across).reshape(expert_count, -1, sh[8].shape[1]), 1, 1)
    saved = []
    home_in = []
    for le in range(exp_dev):
        rows_x[le] = to_all(
            rows_x[le][0], across=rows_x[le][1], during=saved[le - 1] if le else (sh[8],)
        )
        res = pl.pallas_call(
            expert_body,
            grid=(steps,),
            out_shape=(row_out,) * 4 + (saved_out,) * 3,
            in_specs=[rows_blk] * 4
            + [cot_blk(le)] * 4
            + [
                weight_blk(le, dim, exp_hidden),
                weight_blk(le, dim, exp_hidden),
                weight_blk(le, exp_hidden, dim),
            ],
            out_specs=(rows_blk,) * 4 + (saved_blk,) * 3,
            compiler_params=params(1),
            cost_estimate=cost(5 * expert_flops, 14e6),
            name="expert",
        )(*rows_x[le], *cots, expert_gate, expert_up, expert_down)
        if le == 0:
            res = tie(res, halves[1])
            halves = halve(add2(*halves), bits[0], 0)
        else:
            res = tie(res, crossed)
        saved.append(res[4:])
        r1, inward = beside_sums(res[:4])
        crossed = swap(tie(inward, crossed), 2)
        home_in.append((res[0], r1, crossed))
    home_rows = []
    for le in range(last):
        home_rows.append(exchange(tie(add3(*home_in[le]), *home_rows)))
    before_weights = (inward, *[add3(*home_in[le]) for le in range(last)])
    across_last = crossed
    shared_back = to_owner(sh[4:8], after=(crossed,))
    crossed = shared_back[2]

    grads = ()
    res_in = []
    for le in range(exp_dev):
        args = (*tie(rows_x[le], *before_weights), *cots, *saved[le], expert_down)
        specs = [rows_blk] * 4 + [cot_blk(le)] * 4 + [saved_blk] * 3 + [weight_blk(le, exp_hidden, dim)]
        aliases = {len(args) + i: 4 + i for i in range(len(grads))}
        done = pl.pallas_call(
            functools.partial(weights_body, le > 0),
            grid=(steps,),
            out_shape=(row_out,) * 4
            + (
                sds((exp_dev, dim, exp_hidden), F32),
                sds((exp_dev, dim, exp_hidden), F32),
                sds((exp_dev, exp_hidden, dim), F32),
            ),
            in_specs=specs + [ANY] * len(grads),
            out_specs=(rows_blk,) * 4
            + (
                weight_blk(le, dim, exp_hidden),
                weight_blk(le, dim, exp_hidden),
                weight_blk(le, exp_hidden, dim),
            ),
            scratch_shapes=[
                pltpu.VMEM((4 * src * cap, dim), BF16),
                pltpu.VMEM((4 * src * cap, dim), BF16),
            ],
            input_output_aliases=aliases,
            compiler_params=params(1),
            cost_estimate=cost(4 * expert_flops, 16e6),
            name="weights",
        )(*args, *grads)
        done = tie(done, across_last) if le == 0 else tie(done, home_rows[0], crossed)
        grads = done[4:]
        res_in.append(done[:4])
    p0, r1, rx = home_in[last]
    home_rows.append(exchange(tie(add3(p0, r1, tie(rx, grads)), *home_rows)))
    for le in range(exp_dev):
        res_in[le] = to_owner(res_in[le], after=(crossed,))
        crossed = res_in[le][2]

    both_res = jnp.stack([add3(*terms) for terms in res_in], axis=1)
    for bit in bits[1:]:
        halves = halve(tie(add2(*halves), home_rows[0]), bit, 0)

    grad_hidden, dh, gain_ffn = pl.pallas_call(
        functools.partial(home_body, exp_dev, tb),
        out_shape=(sds((tb, dim), F32), block, sds((1, dim), F32)),
        in_specs=[SMEM] + [VMEM] * (2 * exp_dev + 7),
        out_specs=(VMEM,) * 3,
        compiler_params=params(),
        cost_estimate=cost(1e9, 5e6),
        name="home",
    )(
        where,
        *home_rows,
        *slot_le,
        *shared_back,
        tie(hidden, *grads, both_res),
        gain_b,
        cotangent,
        codes,
    )

    h_all = to_all(dh)
    home_res = exchange(tie(both_res, home_rows[last]))
    shared_fwd = to_owner(sh[0:4], after=(h_all[2],))
    rows_each = dim // expert_count
    direct = rows_each % 16 == 0
    gw_shape = (expert_count, rows_each + 16, dim) if direct else (dim, dim)
    back = pl.pallas_call(
        functools.partial(attend_back_body, tb),
        out_shape=(block,) * 4 + (sds(gw_shape, BF16), sds((4, dim), F32)),
        in_specs=[SMEM] + [VMEM] * 21,
        out_specs=(VMEM,) * 6,
        scratch_shapes=[
            pltpu.VMEM((seq_len, width), F32),
            pltpu.VMEM((seq_len, width), F32),
            pltpu.VMEM((seq_len, dim), BF16),
            pltpu.VMEM((seq_len, width), BF16),
            pltpu.VMEM((width, seq_len), BF16),
            pltpu.VMEM((width, seq_len), BF16),
            pltpu.VMEM((seq_len, width), F32),
            pltpu.VMEM((width, seq_len), F32),
            pltpu.VMEM((width, seq_len), F32),
            pltpu.VMEM((3, seq_len, width), BF16),
        ],
        compiler_params=params(),
        cost_estimate=cost(30e9, 15e6, 3e6),
        name="attend_back",
    )(
        info,
        *h_all,
        gain_a,
        gain_ffn,
        wq_t,
        wk_t,
        wv_t,
        w_output,
        act_a,
        q,
        k,
        v,
        att,
        lse,
        *rope,
    )
    back = tie(back, halves[1])
    gw = back[4]
    if not direct:
        gain_part = jnp.broadcast_to(back[5].astype(BF16)[None], (expert_count, 4, dim))
        gw = jnp.concatenate([gw.reshape(expert_count, rows_each, dim), gain_part], axis=1)
    r1, inward = beside_sums(back[:4])
    gw = exchange(tie(gw, home_res))
    da_parts = (back[0], r1, swap(inward, 2))
    kept, got = halves
    shared_grads = (kept.astype(F32) + tie(got, da_parts).astype(F32))[0]
    grad_inputs = pl.pallas_call(
        grad_in_body,
        out_shape=sds((tb, dim), F32),
        in_specs=[VMEM] * 6,
        out_specs=VMEM,
        compiler_params=params(),
        cost_estimate=cost(1e7, 4e6),
        name="grad_in",
    )(inputs, *da_parts, grad_hidden, gain_a)
    layer_out = pl.pallas_call(
        functools.partial(layer_out_body, exp_dev),
        out_shape=sds((tb, dim), F32),
        in_specs=[SMEM] + [VMEM] * (exp_dev + 7),
        out_specs=VMEM,
        compiler_params=params(),
        cost_estimate=cost(1e9, 4e6),
        name="layer_out",
    )(where, tie(home_res, back), *slot_le, hidden, *shared_fwd, codes, gates_b)
    gw = jnp.sum(tie(gw, layer_out, grad_inputs).astype(F32), axis=0)
    gains = jnp.sum(gw[rows_each : rows_each + 4].reshape(2, 2, dim), axis=1)
    gains = gains + swap(gains, 1)
    gains = gains + swap(gains, 2)
    gw = [gw[:rows_each, i * width : (i + 1) * width] for i in range(4)]
    return (
        layer_out,
        grad_inputs,
        gains[0],
        gw[0],
        gw[1],
        gw[2],
        gw[3].T,
        gains[1],
        shared_grads[:, :hidden_units],
        shared_grads[:, hidden_units : 2 * hidden_units],
        shared_grads[:, 2 * hidden_units :].T,
        grads[0],
        grads[1],
        grads[2],
    )


def solution(mesh):
    return jax.shard_map(
        per_device,
        mesh=mesh,
        in_specs=(
            P(("expert", "tensor"), None),
            P(),
            P(None, "tensor"),
            P(None, "tensor"),
            P(None, "tensor"),
            P("tensor", None),
            P(),
            P(None, "tensor"),
            P(None, "tensor"),
            P("tensor", None),
            P("expert", None, "tensor"),
            P("expert", None, "tensor"),
            P("expert", "tensor", None),
            P("expert", None),
            P("expert", None),
            P("expert"),
            P("expert", None),
        ),
        out_specs=(
            P(("expert", "tensor"), None),
            P(("expert", "tensor"), None),
            P(),
            P("expert", "tensor"),
            P("expert", "tensor"),
            P("expert", "tensor"),
            P("tensor", "expert"),
            P(),
            P("expert", "tensor"),
            P("expert", "tensor"),
            P("tensor", "expert"),
            P("expert", None, "tensor"),
            P("expert", None, "tensor"),
            P("expert", "tensor", None),
        ),
        check_vma=False,
    )
```

```python
import functools

import jax
import jax.numpy as jnp
import numpy as np
from jax import lax
from jax.experimental import pallas as pl
from jax.experimental.pallas import tpu as pltpu
from jax.sharding import PartitionSpec as P

HDIM = 64
ROUTED_EXPERTS = 16
EPS = 1e-05
F32 = jnp.float32
BF16 = jnp.bfloat16
ROPE_STEP = 32

VMEM = pl.BlockSpec(memory_space=pltpu.VMEM)
SMEM = pl.BlockSpec(memory_space=pltpu.SMEM)
ANY = pl.BlockSpec(memory_space=pl.ANY)


def sds(shape, dtype):
    return jax.ShapeDtypeStruct(tuple(shape), dtype)


def params(n_grid=0):
    if n_grid:
        return pltpu.CompilerParams(
            vmem_limit_bytes=60 * 1024 * 1024, dimension_semantics=("arbitrary",) * n_grid
        )
    return pltpu.CompilerParams(vmem_limit_bytes=60 * 1024 * 1024)


def nn(a, b):
    return jnp.dot(a, b, preferred_element_type=F32)


def nt(a, b):
    return lax.dot_general(a, b, (((1,), (1,)), ((), ())), preferred_element_type=F32)


def tn(a, b):
    return lax.dot_general(a, b, (((0,), (0,)), ((), ())), preferred_element_type=F32)


def swap(x, bit):
    count = lax.axis_size("tensor")
    return lax.ppermute(x, "tensor", [(i, i ^ bit) for i in range(count)])


def rope_parts(seq_len, width):
    half = HDIM // 2
    frequency = 10000.0 ** (-np.arange(half, dtype=np.float64) * 2.0 / HDIM)
    lanes = np.tile(np.concatenate([frequency, frequency]), width // HDIM)
    sign = np.tile(np.concatenate([-np.ones(half), np.ones(half)]), width // HDIM)
    coarse = np.arange(0, seq_len, ROPE_STEP)[:, None] * lanes[None, :]
    fine = np.arange(ROPE_STEP)[:, None] * lanes[None, :]
    return tuple(
        jnp.asarray(a, dtype=F32)
        for a in (np.cos(coarse), np.sin(coarse), np.cos(fine), np.sin(fine), sign[None, :])
    )


def fill_rope(cos_coarse, sin_coarse, cos_fine, sin_fine, sign, cos_out, sin_out):
    cf, sf, sg = cos_fine[...], sin_fine[...], sign[...]

    def step(a, _):
        cc = cos_coarse[pl.ds(a, 1), :]
        sc = sin_coarse[pl.ds(a, 1), :]
        at = pl.ds(pl.multiple_of(a * ROPE_STEP, ROPE_STEP), ROPE_STEP)
        cos_out[at, :] = cc * cf - sc * sf
        sin_out[at, :] = (sc * cf + cc * sf) * sg
        return 0

    lax.fori_loop(0, cos_coarse.shape[0], step, 0)


def half_swap_matrix(width):
    row = lax.broadcasted_iota(jnp.int32, (width, width), 0)
    col = lax.broadcasted_iota(jnp.int32, (width, width), 1)
    half = HDIM // 2
    partner = jnp.where((col & half) == 0, col + half, col - half)
    return jnp.where(row == partner, 1.0, 0.0).astype(BF16)


def rms(values):
    return lax.rsqrt(jnp.mean(values * values, axis=-1, keepdims=True) + EPS)


def slot_pick(codes_k0, codes_k1, slot_code):
    first = codes_k0 == slot_code
    second = codes_k1 == slot_code
    return first, second


def prep_body(cap, tb, where_ref, routes_ref, gates_ref, dy_ref, *rest):
    t = where_ref[0]
    blocks = routes_ref.shape[0]
    slots = rest[:-2]
    codes_ref, rows_ref = rest[-2:]
    upper = jnp.where(
        lax.broadcasted_iota(jnp.int32, (tb, tb), 0) < lax.broadcasted_iota(jnp.int32, (tb, tb), 1),
        1.0,
        0.0,
    ).astype(BF16)
    ids = lax.broadcasted_iota(jnp.int32, (ROUTED_EXPERTS, tb), 0)
    for b in range(blocks):
        r0 = routes_ref[b, 0:1, :]
        r1 = routes_ref[b, 1:2, :]
        e0 = ids == r0
        e1 = ids == r1
        named = jnp.where(e0, 1.0, 0.0) + jnp.where(e1, 1.0, 0.0)
        before = nn(named.astype(BF16), upper)
        k0 = jnp.sum(jnp.where(e0, before, 0.0), axis=0, keepdims=True)
        k1 = jnp.sum(jnp.where(e1, before, 0.0), axis=0, keepdims=True)
        codes_ref[b, 0:1, :] = r0 * cap + k0.astype(jnp.int32)
        codes_ref[b, 1:2, :] = r1 * cap + k1.astype(jnp.int32)
    c0 = codes_ref[t, 0:1, :]
    c1 = codes_ref[t, 1:2, :]
    g0 = gates_ref[t, 0:1, :]
    g1 = gates_ref[t, 1:2, :]
    dy = dy_ref[pl.ds(pl.multiple_of(t * tb, tb), tb), :]
    for le, slot_ref in enumerate(slots):
        first, second = slot_pick(c0, c1, slot_ref[...])
        gate = jnp.sum(
            jnp.where(first, g0, 0.0) + jnp.where(second, g1, 0.0), axis=1, keepdims=True
        )
        pick = jnp.where(first | second, 1.0, 0.0).astype(BF16)
        got = nn(pick, dy) * gate
        rows_ref[:, le] = got.astype(BF16).reshape(rows_ref.shape[0], cap, got.shape[1])


def attend_body(
    tb,
    info_ref,
    x0,
    x1,
    x2,
    x3,
    gain_ref,
    wq_ref,
    wk_ref,
    wv_ref,
    wo_ref,
    cos_coarse,
    sin_coarse,
    cos_fine,
    sin_fine,
    sign,
    act_ref,
    q_ref,
    k_ref,
    v_ref,
    att_ref,
    lse_ref,
    out0,
    out1,
    out2,
    out3,
    cos_s,
    sin_s,
):
    t = info_ref[0]
    prefix = info_ref[1]
    seq_len, width = q_ref.shape
    blocks = seq_len // tb
    heads = width // HDIM
    fill_rope(cos_coarse, sin_coarse, cos_fine, sin_fine, sign, cos_s, sin_s)
    gain = gain_ref[...]
    for j, piece in enumerate((x0, x1, x2, x3)):
        x = piece[...].astype(F32)
        at = pl.ds(pl.multiple_of((t ^ j) * tb, tb), tb)
        act_ref[at, :] = (x * rms(x) * gain).astype(BF16)
    flip = half_swap_matrix(width)
    wq = wq_ref[...]
    wk = wk_ref[...]
    wq_flip = nn(flip, wq).astype(BF16)
    wk_flip = nn(flip, wk).astype(BF16)
    scale = HDIM ** (-0.5)

    def project(b, _):
        at = pl.ds(pl.multiple_of(b * tb, tb), tb)
        a = act_ref[at, :]
        cos, sin = cos_s[at, :], sin_s[at, :]
        q_ref[at, :] = (scale * (nt(a, wq) * cos + nt(a, wq_flip) * sin)).astype(BF16)
        k_ref[at, :] = (nt(a, wk) * cos + nt(a, wk_flip) * sin).astype(BF16)
        v_ref[at, :] = nt(a, wv_ref[...]).astype(BF16)
        return 0

    lax.fori_loop(0, blocks, project, 0)
    lane_head = lax.broadcasted_iota(jnp.int32, (tb, width), 1) // HDIM
    lane = lax.broadcasted_iota(jnp.int32, (tb, lse_ref.shape[1]), 1)
    for b in range(blocks):
        extent = max(seq_len // 2, (b + 1) * tb)
        rows = slice(b * tb, (b + 1) * tb)
        qb = q_ref[rows, :]
        limit = jnp.maximum(
            b * tb + lax.broadcasted_iota(jnp.int32, (tb, 1), 0), prefix - 1
        )
        allowed = lax.broadcasted_iota(jnp.int32, (tb, extent), 1) <= limit

        def one_head(h, carried, extent=extent, qb=qb, allowed=allowed):
            att, lse = carried
            mine = lane_head == h
            scores = nt(jnp.where(mine, qb, jnp.zeros_like(qb)), k_ref[:extent, :])
            scores = jnp.where(allowed, scores, -1e30)
            top = jnp.max(scores, axis=-1, keepdims=True)
            weight = jnp.exp(scores - top)
            total = jnp.sum(weight, axis=-1, keepdims=True)
            got = nn(weight.astype(BF16), v_ref[:extent, :]) / total
            att = jnp.where(mine, got, att)
            lse = jnp.where(lane == h, top + jnp.log(total), lse)
            return att, lse

        att, lse = lax.fori_loop(
            0,
            heads,
            one_head,
            (jnp.zeros((tb, width), F32), jnp.zeros((tb, lse_ref.shape[1]), F32)),
        )
        att = att.astype(BF16)
        att_ref[rows, :] = att
        lse_ref[rows, :] = lse
        part = nn(att, wo_ref[...]).astype(BF16)
        for j, out in enumerate((out0, out1, out2, out3)):

            @pl.when((t ^ b) == j)
            def _(out=out, part=part):
                out[...] = part


def dispatch_body(t_blocks, cap, where_ref, x_ref, p0, p1, p2, gain_ref, codes_ref, *rest):
    slots = rest[: t_blocks]
    hidden_ref, act_ref = rest[t_blocks : t_blocks + 2]
    bufs = rest[t_blocks + 2 :]
    t = where_ref[0]
    hidden = (
        x_ref[...].astype(F32)
        + p0[...].astype(F32)
        + p1[...].astype(F32)
        + p2[...].astype(F32)
    )
    hidden_ref[...] = hidden
    act = (hidden * rms(hidden) * gain_ref[...]).astype(BF16)
    act_ref[...] = act
    c0 = codes_ref[t, 0:1, :]
    c1 = codes_ref[t, 1:2, :]
    for slot_ref, buf in zip(slots, bufs, strict=True):
        first, second = slot_pick(c0, c1, slot_ref[...])
        pick = jnp.where(first | second, 1.0, 0.0).astype(BF16)
        got = nn(pick, act).astype(BF16)
        buf[...] = got.reshape(buf.shape)


def shared_body(
    tb,
    where_ref,
    a0,
    a1,
    a2,
    a3,
    dy_ref,
    gate_ref,
    up_ref,
    down_ref,
    f0,
    f1,
    f2,
    f3,
    b0,
    b1,
    b2,
    b3,
    grads_ref,
    act_s,
    dy_s,
    hs_s,
    dg_s,
    du_s,
    f_s,
    b_s,
):
    t = where_ref[0]
    blocks = 4
    for j, piece in enumerate((a0, a1, a2, a3)):
        act_s[j * tb : (j + 1) * tb, :] = piece[...]
        dy_s[j * tb : (j + 1) * tb, :] = dy_ref[pl.ds(pl.multiple_of((t ^ j) * tb, tb), tb), :]

    def block(j, _):
        at = pl.ds(pl.multiple_of(j * tb, tb), tb)
        a = act_s[at, :]
        dy = dy_s[at, :]
        g = nn(a, gate_ref[...])
        u = nn(a, up_ref[...])
        sig = jax.nn.sigmoid(g)
        silu = g * sig
        hs = (silu * u).astype(BF16)
        dhs = nt(dy, down_ref[...])
        dg = (dhs * u * sig * (1.0 + g * (1.0 - sig))).astype(BF16)
        du = (dhs * silu).astype(BF16)
        hs_s[at, :] = hs
        dg_s[at, :] = dg
        du_s[at, :] = du
        f_s[at, :] = nn(hs, down_ref[...]).astype(BF16)
        b_s[at, :] = (nt(dg, gate_ref[...]) + nt(du, up_ref[...])).astype(BF16)
        return 0

    lax.fori_loop(0, blocks, block, 0)
    for j, (f, b) in enumerate(((f0, b0), (f1, b1), (f2, b2), (f3, b3))):
        f[...] = f_s[j * tb : (j + 1) * tb, :]
        b[...] = b_s[j * tb : (j + 1) * tb, :]
    hidden = hs_s.shape[1]

    def columns(c, _):
        at = pl.ds(pl.multiple_of(c * tb, tb), tb)
        a = act_s[:, at]
        dy = dy_s[:, at]
        grads_ref[at, 0:hidden] = tn(a, dg_s[...]).astype(BF16)
        grads_ref[at, hidden : 2 * hidden] = tn(a, du_s[...]).astype(BF16)
        grads_ref[at, 2 * hidden : 3 * hidden] = tn(dy, hs_s[...]).astype(BF16)
        return 0

    lax.fori_loop(0, act_s.shape[1] // tb, columns, 0)


def expert_body(x0, x1, x2, x3, c0, c1, c2, c3, gate_ref, up_ref, down_ref, *outs):
    o = outs[:4]
    he_ref, dg_ref, du_ref = outs[4:7]
    n_src, cap, dim = x0.shape
    rows = n_src * cap
    gate = gate_ref[0]
    up = up_ref[0]
    down = down_ref[0]
    xs = (x0, x1, x2, x3)
    cs = (c0, c1, c2, c3)
    for j in (3, 1, 2, 0):
        x = xs[j][...].reshape(rows, dim)
        c = cs[j][...].reshape(rows, dim)
        g = nn(x, gate)
        u = nn(x, up)
        sig = jax.nn.sigmoid(g)
        silu = g * sig
        dhe = nt(c, down)
        dg = (dhe * u * sig * (1.0 + g * (1.0 - sig))).astype(BF16)
        du = (dhe * silu).astype(BF16)
        he_ref[j] = (silu * u).astype(BF16)
        dg_ref[j] = dg
        du_ref[j] = du
        o[j][...] = (nt(dg, gate) + nt(du, up)).astype(BF16).reshape(n_src, cap, dim)


def weights_body(aliased, x0, x1, x2, x3, c0, c1, c2, c3, he_ref, dg_ref, du_ref, down_ref, *rest):
    if aliased:
        rest = rest[3:]
    o = rest[:4]
    gg_ref, gu_ref, gd_ref, x_s, c_s = rest[4:]
    n_src, cap, dim = x0.shape
    rows = n_src * cap
    step = pl.program_id(0)
    down = down_ref[0]
    cs = (c0, c1, c2, c3)
    for j, x in enumerate((x0, x1, x2, x3)):
        x_s[j * rows : (j + 1) * rows, :] = x[...].reshape(rows, dim)
        c_s[j * rows : (j + 1) * rows, :] = cs[j][...].reshape(rows, dim)
        o[j][...] = nn(he_ref[j], down).astype(BF16).reshape(n_src, cap, dim)
    hidden = he_ref.shape[2]
    he = he_ref[...].reshape(4 * rows, hidden)
    dg = dg_ref[...].reshape(4 * rows, hidden)
    du = du_ref[...].reshape(4 * rows, hidden)
    gg = tn(x_s[...], dg)
    gu = tn(x_s[...], du)
    gd = tn(he, c_s[...])

    @pl.when(step == 0)
    def _():
        gg_ref[0] = gg
        gu_ref[0] = gu
        gd_ref[0] = gd

    @pl.when(step > 0)
    def _():
        gg_ref[0] += gg
        gu_ref[0] += gu
        gd_ref[0] += gd


def home_body(n_le, tb, where_ref, *rest):
    backs = rest[:n_le]
    slots = rest[n_le : 2 * n_le]
    s0, s1, s2, hidden_ref, gain_ref, dy_ref, codes_ref = rest[2 * n_le : 2 * n_le + 7]
    gh_ref, dh_ref, gg_ref = rest[2 * n_le + 7 :]
    t = where_ref[0]
    db = s0[...].astype(F32) + s1[...].astype(F32) + s2[...].astype(F32)
    c0 = codes_ref[t, 0:1, :]
    c1 = codes_ref[t, 1:2, :]
    for back, slot_ref in zip(backs, slots, strict=True):
        first, second = slot_pick(c0, c1, slot_ref[...])
        pick = jnp.where(first | second, 1.0, 0.0).astype(BF16)
        db += tn(pick, back[...].reshape(pick.shape[0], db.shape[1]))
    hidden = hidden_ref[...]
    factor = rms(hidden)
    n = hidden * factor
    inner = db * gain_ref[...]
    dy = dy_ref[pl.ds(pl.multiple_of(t * tb, tb), tb), :].astype(F32)
    gh = dy + factor * (inner - n * jnp.mean(inner * n, axis=-1, keepdims=True))
    gh_ref[...] = gh
    dh_ref[...] = gh.astype(BF16)
    gg_ref[...] = jnp.sum(db * n, axis=0, keepdims=True)


def attend_back_body(
    tb,
    info_ref,
    h0,
    h1,
    h2,
    h3,
    gain_ref,
    gb_ref,
    wq_ref,
    wk_ref,
    wv_ref,
    wo_ref,
    act_ref,
    q_ref,
    k_ref,
    v_ref,
    att_ref,
    lse_ref,
    cos_coarse,
    sin_coarse,
    cos_fine,
    sin_fine,
    sign,
    o0,
    o1,
    o2,
    o3,
    gw_ref,
    gg_ref,
    cos_s,
    sin_s,
    dh_s,
    dat_s,
    qt_s,
    datt_s,
    dq_s,
    dkt_s,
    dvt_s,
    raw_s,
):
    t = info_ref[0]
    prefix = info_ref[1]
    seq_len, width = q_ref.shape
    blocks = seq_len // tb
    heads = width // HDIM
    scale = HDIM ** (-0.5)
    fill_rope(cos_coarse, sin_coarse, cos_fine, sin_fine, sign, cos_s, sin_s)
    for j, piece in enumerate((h0, h1, h2, h3)):
        at = pl.ds(pl.multiple_of((t ^ j) * tb, tb), tb)
        dh = piece[...]
        dh_s[at, :] = dh
        dat_s[at, :] = nt(dh, wo_ref[...]).astype(BF16)
    for b in range(blocks):
        rows = slice(b * tb, (b + 1) * tb)
        qt_s[:, rows] = q_ref[rows, :].T
        datt_s[:, rows] = dat_s[rows, :].T
    dkt_s[...] = jnp.zeros_like(dkt_s)
    dvt_s[...] = jnp.zeros_like(dvt_s)
    lane_head = lax.broadcasted_iota(jnp.int32, (tb, width), 1) // HDIM
    lane = lax.broadcasted_iota(jnp.int32, (tb, lse_ref.shape[1]), 1)
    for b in range(blocks):
        extent = max(seq_len // 2, (b + 1) * tb)
        rows = slice(b * tb, (b + 1) * tb)
        qb = q_ref[rows, :]
        datb = dat_s[rows, :]
        mix = datb.astype(F32) * att_ref[rows, :].astype(F32)
        lse_b = lse_ref[rows, :]
        limit = jnp.maximum(
            b * tb + lax.broadcasted_iota(jnp.int32, (tb, 1), 0), prefix - 1
        )
        allowed = lax.broadcasted_iota(jnp.int32, (tb, extent), 1) <= limit

        def one_head(h, dq, extent=extent, rows=rows, qb=qb, datb=datb, mix=mix, lse_b=lse_b, allowed=allowed):
            mine = lane_head == h
            lse = jnp.sum(jnp.where(lane == h, lse_b, 0.0), axis=-1, keepdims=True)
            delta = jnp.sum(jnp.where(mine, mix, 0.0), axis=-1, keepdims=True)
            scores = nt(jnp.where(mine, qb, jnp.zeros_like(qb)), k_ref[:extent, :])
            prob = jnp.exp(jnp.where(allowed, scores, -1e30) - lse)
            dp = nt(jnp.where(mine, datb, jnp.zeros_like(datb)), v_ref[:extent, :])
            ds = (prob * (dp - delta)).astype(BF16)
            at = pl.ds(pl.multiple_of(h * HDIM, HDIM), HDIM)
            dkt_s[at, :extent] += nn(qt_s[at, rows], ds)
            dvt_s[at, :extent] += nn(datt_s[at, rows], prob.astype(BF16))
            return jnp.where(mine, nn(ds, k_ref[:extent, :]), dq)

        dq_s[rows, :] = lax.fori_loop(0, heads, one_head, jnp.zeros((tb, width), F32))
    flip = half_swap_matrix(width)

    def unrotate(u, at):
        high = u.astype(BF16)
        low = (u - high.astype(F32)).astype(BF16)
        return (u * cos_s[at, :] - (nn(high, flip) + nn(low, flip)) * sin_s[at, :]).astype(BF16)

    gain_sum = jnp.zeros((1, act_ref.shape[1]), F32)
    for b in range(blocks):
        rows = slice(b * tb, (b + 1) * tb)
        dq = unrotate(dq_s[rows, :] * scale, rows)
        dk = unrotate(dkt_s[:, rows].T, rows)
        dv = dvt_s[:, rows].T.astype(BF16)
        raw_s[0, rows, :] = dq
        raw_s[1, rows, :] = dk
        raw_s[2, rows, :] = dv
        da = nn(dq, wq_ref[...]) + nn(dk, wk_ref[...]) + nn(dv, wv_ref[...])
        gain_sum += jnp.sum(da * act_ref[rows, :].astype(F32), axis=0, keepdims=True)
        part = da.astype(BF16)
        for j, out in enumerate((o0, o1, o2, o3)):

            @pl.when((t ^ b) == j)
            def _(out=out, part=part):
                out[...] = part

    gain_a = gain_sum / gain_ref[...]
    g = [tn(raw_s[i], act_ref[...]).T for i in range(3)] + [tn(att_ref[...], dh_s[...]).T]
    g = jnp.concatenate(g, axis=1).astype(BF16)
    flat = []
    for gain in (gain_a, gb_ref[...]):
        high = gain.astype(BF16).astype(F32)
        flat += [high, gain - high]
    if len(gw_ref.shape) == 2:
        gw_ref[...] = g
        gg_ref[...] = jnp.concatenate(flat, axis=0)
    else:
        gg_ref[...] = jnp.zeros_like(gg_ref)
        each = g.shape[0] // gw_ref.shape[0]
        gw_ref[:, :each] = g.reshape(gw_ref.shape[0], each, g.shape[1])
        rest = gw_ref.shape[1] - each
        lines = jnp.concatenate(flat + [jnp.zeros((rest - 4, g.shape[1]), F32)], axis=0)
        gw_ref[:, each:] = jnp.broadcast_to(
            lines.astype(BF16)[None], (gw_ref.shape[0], rest, g.shape[1])
        )


def layer_out_body(n_le, where_ref, back_ref, *rest):
    slots = rest[:n_le]
    hidden_ref, s0, s1, s2, codes_ref, gates_ref, out_ref = rest[n_le:]
    t = where_ref[0]
    out = (
        hidden_ref[...] + s0[...].astype(F32) + s1[...].astype(F32) + s2[...].astype(F32)
    )
    c0 = codes_ref[t, 0:1, :]
    c1 = codes_ref[t, 1:2, :]
    g0 = gates_ref[t, 0:1, :]
    g1 = gates_ref[t, 1:2, :]
    for le, slot_ref in enumerate(slots):
        first, second = slot_pick(c0, c1, slot_ref[...])
        weight = jnp.where(first, g0, 0.0) + jnp.where(second, g1, 0.0)
        high = weight.astype(BF16)
        low = (weight - high.astype(F32)).astype(BF16)
        rows = back_ref[:, le].reshape(high.shape[0], out.shape[1])
        out += tn(high, rows) + tn(low, rows)
    out_ref[...] = out


def grad_in_body(x_ref, p0, p1, p2, gh_ref, gain_ref, out_ref):
    x = x_ref[...].astype(F32)
    da = p0[...].astype(F32) + p1[...].astype(F32) + p2[...].astype(F32)
    factor = rms(x)
    n = x * factor
    inner = da * gain_ref[...]
    out_ref[...] = gh_ref[...] + factor * (
        inner - n * jnp.mean(inner * n, axis=-1, keepdims=True)
    )


def tie(x, *deps):
    return lax.optimization_barrier((x, deps))[0]


def cost(flops, read, transcendentals=0):
    return pl.CostEstimate(
        flops=int(flops * 0.4), bytes_accessed=int(read * 0.4), transcendentals=0
    )


def add2(a, b):
    return (a.astype(F32) + b.astype(F32)).astype(BF16)


def add3(a, b, c):
    return (a.astype(F32) + b.astype(F32) + c.astype(F32)).astype(BF16)


def beside_sums(pieces):
    r3 = swap(pieces[3], 1)
    r1 = swap(pieces[1], 1)
    return r1, add2(pieces[2], r3)


def to_owner(pieces, after=()):
    r1, inward = beside_sums(pieces)
    return pieces[0], r1, swap(tie(inward, *after), 2)


def to_all(own, after=(), across=None, during=()):
    if across is None:
        across = swap(tie(own, *after), 2)
    beside = swap(own, 1)
    both = swap(tie(across, *during), 1)
    return own, beside, across, both


def exchange(x):
    return lax.all_to_all(x, "expert", split_axis=0, concat_axis=0, tiled=True)


def halve(x, bit, axis):
    count = lax.axis_size("expert")
    x = x.reshape(*((-1, 2) if axis else (2, -1)), *x.shape[1:])
    mine = (lax.axis_index("expert") // bit) % 2
    keep = lax.dynamic_index_in_dim(x, mine, axis, keepdims=False)
    send = lax.dynamic_index_in_dim(x, 1 - mine, axis, keepdims=False)
    return keep, lax.ppermute(send, "expert", [(i, i ^ bit) for i in range(count)])


def per_device(
    inputs,
    attn_gain,
    w_query,
    w_key,
    w_value,
    w_output,
    ffn_gain,
    shared_gate,
    shared_up,
    shared_down,
    expert_gate,
    expert_up,
    expert_down,
    routes,
    gate_values,
    prefix,
    cotangent,
):
    tensor_count = lax.axis_size("tensor")
    expert_count = lax.axis_size("expert")
    assert tensor_count == 4
    t = lax.axis_index("tensor")
    tb, dim = inputs.shape
    seq_len, choices = routes.shape
    width = w_query.shape[1]
    hidden_units = shared_gate.shape[1]
    exp_hidden = expert_gate.shape[2]
    exp_dev = expert_gate.shape[0]
    slabs = max(1, expert_count // ROUTED_EXPERTS)
    cap = max(2, 3 * tb * choices // (2 * ROUTED_EXPERTS))
    where = jnp.reshape(t, (1,)).astype(jnp.int32)
    info = jnp.stack([t.astype(jnp.int32), prefix[0]])
    gain_a = attn_gain.reshape(1, dim)
    gain_b = ffn_gain.reshape(1, dim)
    wq_t, wk_t, wv_t = w_query.T, w_key.T, w_value.T

    entries = np.arange(expert_count * exp_dev)
    slot_np = (entries // slabs)[:, None] * cap + np.arange(cap)[None, :]
    slot_np = slot_np.reshape(expert_count, exp_dev, cap).astype(np.int32)
    slot_le = [jnp.asarray(slot_np[:, le].reshape(-1, 1)) for le in range(exp_dev)]
    last = exp_dev - 1

    x2 = swap(inputs, 2)

    routes_b = routes.reshape(tensor_count, tb, choices).transpose(0, 2, 1)
    gates_b = gate_values.reshape(tensor_count, tb, choices).transpose(0, 2, 1)
    codes, cot_rows = pl.pallas_call(
        functools.partial(prep_body, cap, tb),
        out_shape=(
            sds((tensor_count, choices, tb), jnp.int32),
            sds((expert_count, exp_dev, cap, dim), BF16),
        ),
        in_specs=[SMEM] + [VMEM] * (3 + exp_dev),
        out_specs=(VMEM, VMEM),
        compiler_params=params(),
        cost_estimate=cost(2e9, 6e6),
        name="prep",
    )(where, routes_b, gates_b, cotangent, *slot_le)
    cot = exchange(cot_rows)
    x1 = swap(inputs, 1)
    x3 = swap(tie(x2, codes), 1)

    rope = rope_parts(seq_len, width)
    block = sds((tb, dim), BF16)
    att_out = pl.pallas_call(
        functools.partial(attend_body, tb),
        out_shape=(
            sds((seq_len, dim), BF16),
            sds((seq_len, width), BF16),
            sds((seq_len, width), BF16),
            sds((seq_len, width), BF16),
            sds((seq_len, width), BF16),
            sds((seq_len, 128), F32),
            block,
            block,
            block,
            block,
        ),
        in_specs=[SMEM] + [VMEM] * 14,
        out_specs=(VMEM,) * 10,
        scratch_shapes=[pltpu.VMEM((seq_len, width), F32)] * 2,
        compiler_params=params(),
        cost_estimate=cost(3e9, 3e6, 3e6),
        name="attend",
    )(info, inputs, x1, x2, x3, gain_a, wq_t, wk_t, wv_t, w_output, *rope)
    act_a, q, k, v, att, lse = att_out[:6]
    r1, inward = beside_sums(att_out[6:])
    crossed = swap(inward, 2)
    parts = (att_out[6], r1, crossed)

    got = pl.pallas_call(
        functools.partial(dispatch_body, exp_dev, cap),
        out_shape=(sds((tb, dim), F32), block)
        + (sds((expert_count, cap, dim), BF16),) * exp_dev,
        in_specs=[SMEM] + [VMEM] * (6 + exp_dev),
        out_specs=(VMEM,) * (2 + exp_dev),
        compiler_params=params(),
        cost_estimate=cost(1e9, 4e6),
        name="dispatch",
    )(where, inputs, *parts, gain_b, codes, *slot_le)
    hidden, act_b = got[:2]
    a_all = to_all(act_b)

    sh = pl.pallas_call(
        functools.partial(shared_body, tb),
        out_shape=(block,) * 8 + (sds((dim, 3 * hidden_units), BF16),),
        in_specs=[SMEM] + [VMEM] * 8,
        out_specs=(VMEM,) * 9,
        scratch_shapes=[
            pltpu.VMEM((seq_len, dim), BF16),
            pltpu.VMEM((seq_len, dim), BF16),
            pltpu.VMEM((seq_len, hidden_units), BF16),
            pltpu.VMEM((seq_len, hidden_units), BF16),
            pltpu.VMEM((seq_len, hidden_units), BF16),
            pltpu.VMEM((seq_len, dim), BF16),
            pltpu.VMEM((seq_len, dim), BF16),
        ],
        compiler_params=params(),
        cost_estimate=cost(8e9, 12e6),
        name="shared",
    )(where, *a_all, cotangent, shared_gate, shared_up, shared_down)

    rows_x = []
    cot_across = swap(tie(cot, a_all[2]), 2)
    cots = to_all(cot, across=cot_across, during=(sh[8],))
    crossed = cot_across
    sent = cot
    for le in range(exp_dev):
        sent = exchange(tie(got[2 + le], sent, sh[8] if le else sent))
        crossed = swap(tie(sent, crossed), 2)
        rows_x.append((sent, crossed))

    src = min(8, expert_count)
    steps = expert_count // src
    rows_blk = pl.BlockSpec((src, cap, dim), lambda i: (i, 0, 0))
    saved_blk = pl.BlockSpec((4, src * cap, exp_hidden), lambda i: (0, i, 0))

    def cot_blk(le):
        return pl.BlockSpec((src, pl.Squeezed(), cap, dim), lambda i: (i, le, 0, 0))

    def weight_blk(le, a, b):
        return pl.BlockSpec((1, a, b), lambda i: (le, 0, 0))

    all_rows = expert_count * cap
    row_out = sds((expert_count, cap, dim), BF16)
    saved_out = sds((4, all_rows, exp_hidden), BF16)
    expert_flops = 2 * 4 * all_rows * dim * exp_hidden
    bits = [1 << i for i in range(1, expert_count.bit_length() - 1)][::-1]
    halves = halve(tie(sh[8], cot_across).reshape(expert_count, -1, sh[8].shape[1]), 1, 1)
    saved = []
    home_in = []
    for le in range(exp_dev):
        rows_x[le] = to_all(
            rows_x[le][0], across=rows_x[le][1], during=saved[le - 1] if le else (sh[8],)
        )
        res = pl.pallas_call(
            expert_body,
            grid=(steps,),
            out_shape=(row_out,) * 4 + (saved_out,) * 3,
            in_specs=[rows_blk] * 4
            + [cot_blk(le)] * 4
            + [
                weight_blk(le, dim, exp_hidden),
                weight_blk(le, dim, exp_hidden),
                weight_blk(le, exp_hidden, dim),
            ],
            out_specs=(rows_blk,) * 4 + (saved_blk,) * 3,
            compiler_params=params(1),
            cost_estimate=cost(5 * expert_flops, 14e6),
            name="expert",
        )(*rows_x[le], *cots, expert_gate, expert_up, expert_down)
        if le == 0:
            res = tie(res, halves[1])
            halves = halve(add2(*halves), bits[0], 0)
        else:
            res = tie(res, crossed)
        saved.append(res[4:])
        r1, inward = beside_sums(res[:4])
        crossed = swap(tie(inward, crossed), 2)
        home_in.append((res[0], r1, crossed))
    home_rows = []
    for le in range(last):
        home_rows.append(exchange(tie(add3(*home_in[le]), *home_rows)))
    before_weights = (inward, *[add3(*home_in[le]) for le in range(last)])
    across_last = crossed
    shared_back = to_owner(sh[4:8], after=(crossed,))
    crossed = shared_back[2]

    grads = ()
    res_in = []
    for le in range(exp_dev):
        args = (*tie(rows_x[le], *before_weights), *cots, *saved[le], expert_down)
        specs = [rows_blk] * 4 + [cot_blk(le)] * 4 + [saved_blk] * 3 + [weight_blk(le, exp_hidden, dim)]
        aliases = {len(args) + i: 4 + i for i in range(len(grads))}
        done = pl.pallas_call(
            functools.partial(weights_body, le > 0),
            grid=(steps,),
            out_shape=(row_out,) * 4
            + (
                sds((exp_dev, dim, exp_hidden), F32),
                sds((exp_dev, dim, exp_hidden), F32),
                sds((exp_dev, exp_hidden, dim), F32),
            ),
            in_specs=specs + [ANY] * len(grads),
            out_specs=(rows_blk,) * 4
            + (
                weight_blk(le, dim, exp_hidden),
                weight_blk(le, dim, exp_hidden),
                weight_blk(le, exp_hidden, dim),
            ),
            scratch_shapes=[
                pltpu.VMEM((4 * src * cap, dim), BF16),
                pltpu.VMEM((4 * src * cap, dim), BF16),
            ],
            input_output_aliases=aliases,
            compiler_params=params(1),
            cost_estimate=cost(4 * expert_flops, 16e6),
            name="weights",
        )(*args, *grads)
        done = tie(done, across_last) if le == 0 else tie(done, home_rows[0], crossed)
        grads = done[4:]
        res_in.append(done[:4])
    p0, r1, rx = home_in[last]
    home_rows.append(exchange(tie(add3(p0, r1, tie(rx, grads)), *home_rows)))
    for le in range(exp_dev):
        res_in[le] = to_owner(res_in[le], after=(crossed,))
        crossed = res_in[le][2]

    both_res = jnp.stack([add3(*terms) for terms in res_in], axis=1)
    for bit in bits[1:]:
        halves = halve(tie(add2(*halves), home_rows[0]), bit, 0)

    grad_hidden, dh, gain_ffn = pl.pallas_call(
        functools.partial(home_body, exp_dev, tb),
        out_shape=(sds((tb, dim), F32), block, sds((1, dim), F32)),
        in_specs=[SMEM] + [VMEM] * (2 * exp_dev + 7),
        out_specs=(VMEM,) * 3,
        compiler_params=params(),
        cost_estimate=cost(1e9, 5e6),
        name="home",
    )(
        where,
        *home_rows,
        *slot_le,
        *shared_back,
        tie(hidden, *grads, both_res),
        gain_b,
        cotangent,
        codes,
    )

    h_all = to_all(dh)
    home_res = exchange(tie(both_res, home_rows[last]))
    shared_fwd = to_owner(sh[0:4], after=(h_all[2],))
    rows_each = dim // expert_count
    direct = rows_each % 16 == 0
    gw_shape = (expert_count, rows_each + 16, dim) if direct else (dim, dim)
    back = pl.pallas_call(
        functools.partial(attend_back_body, tb),
        out_shape=(block,) * 4 + (sds(gw_shape, BF16), sds((4, dim), F32)),
        in_specs=[SMEM] + [VMEM] * 21,
        out_specs=(VMEM,) * 6,
        scratch_shapes=[
            pltpu.VMEM((seq_len, width), F32),
            pltpu.VMEM((seq_len, width), F32),
            pltpu.VMEM((seq_len, dim), BF16),
            pltpu.VMEM((seq_len, width), BF16),
            pltpu.VMEM((width, seq_len), BF16),
            pltpu.VMEM((width, seq_len), BF16),
            pltpu.VMEM((seq_len, width), F32),
            pltpu.VMEM((width, seq_len), F32),
            pltpu.VMEM((width, seq_len), F32),
            pltpu.VMEM((3, seq_len, width), BF16),
        ],
        compiler_params=params(),
        cost_estimate=cost(30e9, 15e6, 3e6),
        name="attend_back",
    )(
        info,
        *h_all,
        gain_a,
        gain_ffn,
        wq_t,
        wk_t,
        wv_t,
        w_output,
        act_a,
        q,
        k,
        v,
        att,
        lse,
        *rope,
    )
    back = tie(back, halves[1])
    gw = back[4]
    if not direct:
        gain_part = jnp.broadcast_to(back[5].astype(BF16)[None], (expert_count, 4, dim))
        gw = jnp.concatenate([gw.reshape(expert_count, rows_each, dim), gain_part], axis=1)
    r1, inward = beside_sums(back[:4])
    gw = exchange(tie(gw, home_res))
    da_parts = (back[0], r1, swap(inward, 2))
    kept, got = halves
    shared_grads = (kept.astype(F32) + tie(got, da_parts).astype(F32))[0]
    grad_inputs = pl.pallas_call(
        grad_in_body,
        out_shape=sds((tb, dim), F32),
        in_specs=[VMEM] * 6,
        out_specs=VMEM,
        compiler_params=params(),
        cost_estimate=cost(1e7, 4e6),
        name="grad_in",
    )(inputs, *da_parts, grad_hidden, gain_a)
    layer_out = pl.pallas_call(
        functools.partial(layer_out_body, exp_dev),
        out_shape=sds((tb, dim), F32),
        in_specs=[SMEM] + [VMEM] * (exp_dev + 7),
        out_specs=VMEM,
        compiler_params=params(),
        cost_estimate=cost(1e9, 4e6),
        name="layer_out",
    )(where, tie(home_res, back), *slot_le, hidden, *shared_fwd, codes, gates_b)
    gw = jnp.sum(tie(gw, layer_out, grad_inputs).astype(F32), axis=0)
    gains = jnp.sum(gw[rows_each : rows_each + 4].reshape(2, 2, dim), axis=1)
    gains = (gains + swap(gains, 1)) + (swap(gains, 2) + swap(gains, 3))
    gw = [gw[:rows_each, i * width : (i + 1) * width] for i in range(4)]
    return (
        layer_out,
        grad_inputs,
        gains[0],
        gw[0],
        gw[1],
        gw[2],
        gw[3].T,
        gains[1],
        shared_grads[:, :hidden_units],
        shared_grads[:, hidden_units : 2 * hidden_units],
        shared_grads[:, 2 * hidden_units :].T,
        grads[0],
        grads[1],
        grads[2],
    )


def solution(mesh):
    return jax.shard_map(
        per_device,
        mesh=mesh,
        in_specs=(
            P(("expert", "tensor"), None),
            P(),
            P(None, "tensor"),
            P(None, "tensor"),
            P(None, "tensor"),
            P("tensor", None),
            P(),
            P(None, "tensor"),
            P(None, "tensor"),
            P("tensor", None),
            P("expert", None, "tensor"),
            P("expert", None, "tensor"),
            P("expert", "tensor", None),
            P("expert", None),
            P("expert", None),
            P("expert"),
            P("expert", None),
        ),
        out_specs=(
            P(("expert", "tensor"), None),
            P(("expert", "tensor"), None),
            P(),
            P("expert", "tensor"),
            P("expert", "tensor"),
            P("expert", "tensor"),
            P("tensor", "expert"),
            P(),
            P("expert", "tensor"),
            P("expert", "tensor"),
            P("tensor", "expert"),
            P("expert", None, "tensor"),
            P("expert", None, "tensor"),
            P("expert", "tensor", None),
        ),
        check_vma=False,
    )
```
